8 devices in a mesh: sys: 1 (over z), aux: 2 (over y), orb: 4 (over x, core).
Axes of the slice: x: 2, y: 2, z: 1, core: 2. Of those that a mesh axis runs over, the one named last changes fastest.
Arguments:
- aux_ints: float32 [928, 464, 464], P(('sys', 'aux'), 'orb')
- metric: float32 [928, 928], P(('sys', 'aux'))
- orbitals: float32 [1, 464, 40], P('sys')
Outputs:
- output: float32 [1, 464, 464], P('sys', 'orb', 'aux')
All inputs are finite; a program needn't handle non-finite values.
Results may differ from the reference program's by a relative error of at most 0.001.
Values are sent between devices in bfloat16 or wider.
A program may use at most 1 GiB of HBM per device.

```python
import jax
import jax.numpy as jnp
from jax import lax

N_AUX = 928
N_BASIS = 464
N_OCC = 40
DENS = 1

PRECISE = lax.Precision.HIGHEST


def setup_inputs(seed: int = 0, part: int = 0) -> dict:
    base_key = jax.random.fold_in(jax.random.key(seed), part)
    sub_keys = jax.random.split(base_key, 6)
    rank_b = 4
    rank_m = 4
    coh_scale = (2.0 * N_AUX * N_OCC) ** -0.5 * rank_b ** -0.25
    noise_scale = 2.0 * coh_scale
    coeffs = jax.random.normal(sub_keys[0], (N_AUX, rank_b), jnp.float32)
    patterns = jax.random.normal(sub_keys[1], (rank_b, N_BASIS), jnp.float32)
    row_keys = jax.random.split(sub_keys[2], N_AUX)

    def one_row(row_args):
        row_key, coeff_row = row_args
        noise_mat = jax.random.normal(row_key, (N_BASIS, N_BASIS), jnp.float32)
        sym_noise = (noise_mat + noise_mat.T) * (0.5 ** 0.5)
        low_rank = jnp.einsum('k,km,kl->ml', coeff_row, patterns, patterns)
        return noise_scale * sym_noise + coh_scale * low_rank

    aux_ints = lax.map(one_row, (row_keys, coeffs))
    spread = jax.random.normal(sub_keys[3], (N_AUX, N_AUX), jnp.float32)
    sym_spread = (spread + spread.T) * (0.125 / N_AUX) ** 0.5
    directions = jax.random.normal(sub_keys[4], (rank_m, N_AUX), jnp.float32) * N_AUX ** -0.5
    boost_scale = (N_AUX / rank_m) ** 0.5
    metric = jnp.eye(N_AUX, dtype=jnp.float32) + sym_spread + boost_scale * jnp.dot(directions.T, directions)
    orbitals = jax.random.normal(sub_keys[5], (DENS, N_BASIS, N_OCC), jnp.float32) * N_BASIS ** -0.5
    return {'aux_ints': aux_ints, 'metric': metric, 'orbitals': orbitals}


def reference(aux_ints, metric, orbitals):
    def one_density(coeff_mat):
        half_tr = jnp.einsum('qml,li->qmi', aux_ints, coeff_mat, precision=PRECISE)
        fitted = jnp.einsum('pq,qmi->pmi', metric, half_tr, precision=PRECISE)
        exchange = jnp.einsum('pmi,pni->mn', fitted, fitted, precision=PRECISE)
        gamma_raw = jnp.einsum('qmi,mi->q', half_tr, coeff_mat, precision=PRECISE)
        gamma_fit = jnp.dot(metric, gamma_raw, precision=PRECISE)
        weights = jnp.dot(gamma_fit, metric, precision=PRECISE)
        coulomb = jnp.einsum('q,qmn->mn', weights, aux_ints, precision=PRECISE)
        return 2.0 * coulomb - exchange

    return lax.map(one_density, orbitals)
```

```python
import jax
import jax.numpy as jnp
from jax import lax
from jax.experimental import pallas as pl
from jax.experimental.pallas import tpu as pltpu

P = jax.sharding.PartitionSpec
F32, BF16 = jnp.float32, jnp.bfloat16
MESH = pl.DeviceIdType.MESH
NT = (((1,), (1,)), ((), ()))

NAUX, NORB, NDEV = 2, 4, 8
QB, MB, NB, NI = 464, 116, 464, 40
IV = NI // NDEV
QP, MP = 512, 120
MC = 8
NCH = MP // MC
TAIL = MB - MC * (NCH - 1)
SP = 48
NBUF = 12
NSP = 4


def split3(x):
    a = x.astype(BF16)
    r = x - a.astype(F32)
    b = r.astype(BF16)
    c = (r - b.astype(F32)).astype(BF16)
    return a, b, c


def half_kernel(b_hbm, ct_ref, co_ref, md_hbm, arecv, grecv, mrecv,
                bbuf, bs, cw, abuf, sbuf, gbuf, gsend,
                bsem, ssem, rsem, osem, gs_sem, gr_sem, ms_sem, mr_sem):
    aux, orb = lax.axis_index('aux'), lax.axis_index('orb')
    me = aux * NORB + orb

    def at(d):
        return {'aux': d // NORB, 'orb': lax.rem(d, NORB)}

    def peer(t):
        return lax.rem(me + t, NDEV)

    def fetch(m, slot):
        return pltpu.make_async_copy(b_hbm.at[m], bbuf.at[slot], bsem.at[slot])

    for m in range(NBUF):
        fetch(m, m).start()

    barrier = pltpu.get_barrier_semaphore()
    for t in range(1, NDEV):
        pl.semaphore_signal(barrier, inc=1, device_id=at(peer(t)), device_id_type=MESH)

    abuf[...] = jnp.zeros_like(abuf)
    gbuf[...] = jnp.zeros_like(gbuf)
    c1, c2, c3 = split3(ct_ref[...])
    cw[...] = jnp.concatenate(
        [c1.astype(F32), c2.astype(F32), c3.astype(F32), jnp.zeros((8, NB), F32)], axis=0).astype(BF16)

    pl.semaphore_wait(barrier, NDEV - 1)
    mcopy = pltpu.make_async_remote_copy(md_hbm, mrecv, ms_sem, mr_sem,
                                         device_id={'aux': 1 - aux, 'orb': orb}, device_id_type=MESH)
    mcopy.start()

    def place(c):
        return arecv.at[aux, :, pl.ds(pl.multiple_of(orb * MP + c * MC, 8), MC), :]

    def send(c, slot, t):
        d = peer(t)
        return pltpu.make_async_remote_copy(sbuf.at[slot, d], place(c), ssem.at[slot, t], rsem.at[t],
                                            device_id=at(d), device_id_type=MESH)

    def own(c, slot):
        return pltpu.make_async_copy(sbuf.at[slot, me], place(c), osem.at[slot])

    def chunk(c, rows, more):
        two = lax.rem(c, 2)
        for k in range(rows):
            m = c * MC + k
            slot = lax.rem(m, NBUF)
            fetch(m, slot).wait()
            parts = split3(bbuf[slot])
            r = None
            for j in range(3):
                bs[k % NSP, j] = parts[j]
            for j in range(3):
                x = lax.dot_general(cw[...], bs[k % NSP, j], NT, preferred_element_type=F32)
                r = x if r is None else r + x
            a2 = r[0:NI] + r[NI:2 * NI] + r[2 * NI:3 * NI]
            for v in range(IV):
                for lt in range(4):
                    l0, l1 = lt * 128, min(lt * 128 + 128, QB)
                    abuf[lt, pl.ds(v * MC + k, NDEV, stride=SP), 0:l1 - l0] = a2[8 * v:8 * v + 8, l0:l1]

            def refill():
                fetch(m + NBUF, slot).start()
            if more is None:
                pass
            else:
                pl.when(m + NBUF < MB)(refill)

        @pl.when(c >= 2)
        def _():
            for t in range(1, NDEV):
                send(c - 2, two, t).wait_send()
            own(c - 2, two).wait()

        g = gbuf[...]
        for s in range(NDEV):
            for v in range(IV):
                r0 = s * SP + v * MC
                col = co_ref[pl.ds(pl.multiple_of(c * MC, MC), MC), 8 * v + s:8 * v + s + 1]
                x = jnp.concatenate([abuf[lt, r0:r0 + MC, :] for lt in range(4)], axis=1)
                g = g + x * col
                sbuf[two, s, v] = x.astype(BF16)
        gbuf[...] = g
        for t in range(1, NDEV):
            send(c, two, t).start()
        own(c, two).start()

    @pl.loop(0, NCH - 1)
    def _(c):
        chunk(c, MC, True)
    abuf[...] = jnp.zeros_like(abuf)
    chunk(jnp.int32(NCH - 1), TAIL, None)

    gsend[...] = jnp.broadcast_to(jnp.sum(gbuf[...], axis=0, keepdims=True), (8, QP))

    def gcopy(t):
        return pltpu.make_async_remote_copy(gsend, grecv.at[me], gs_sem.at[t], gr_sem.at[t],
                                            device_id=at(peer(t)), device_id_type=MESH)

    for t in range(1, NDEV):
        gcopy(t).start()
    gown = pltpu.make_async_copy(gsend, grecv.at[me], gs_sem.at[0])
    gown.start()

    for c in (NCH - 2, NCH - 1):
        for t in range(1, NDEV):
            send(c, c % 2, t).wait_send()
        own(c, c % 2).wait()
    for t in range(1, NDEV):
        src = lax.rem(me + NDEV - t, NDEV)
        whole = arecv.at[src // NORB, :, pl.ds(pl.multiple_of(lax.rem(src, NORB) * MP, 8), MP), :]
        pltpu.make_async_remote_copy(whole, whole, rsem.at[t], rsem.at[t],
                                     device_id=at(src), device_id_type=MESH).wait_recv()
        pltpu.make_async_remote_copy(gsend, grecv.at[src], gs_sem.at[t], gr_sem.at[t],
                                     device_id=at(src), device_id_type=MESH).wait()
    gown.wait()
    mcopy.wait()


def half_transform(ints, ct, co, mdiag):
    vmem, hbm = pl.BlockSpec(memory_space=pltpu.VMEM), pl.BlockSpec(memory_space=pl.ANY)
    return pl.pallas_call(
        half_kernel,
        name='half',
        out_shape=(jax.ShapeDtypeStruct((NAUX, IV, NORB * MP, QP), BF16),
                   jax.ShapeDtypeStruct((NDEV, 8, QP), F32),
                   jax.ShapeDtypeStruct((QB, QB), F32)),
        in_specs=[hbm, vmem, vmem, hbm],
        out_specs=(hbm, hbm, hbm),
        scratch_shapes=[
            pltpu.VMEM((NBUF, QB, NB), F32),
            pltpu.VMEM((NSP, 3, QB, NB), BF16),
            pltpu.VMEM((128, NB), BF16),
            pltpu.VMEM((4, NDEV * SP, 128), F32),
            pltpu.VMEM((2, NDEV, IV, MC, QP), BF16),
            pltpu.VMEM((MC, QP), F32),
            pltpu.VMEM((8, QP), F32),
            pltpu.SemaphoreType.DMA((NBUF,)),
            pltpu.SemaphoreType.DMA((2, NDEV)),
            pltpu.SemaphoreType.DMA((NDEV,)),
            pltpu.SemaphoreType.DMA((2,)),
            pltpu.SemaphoreType.DMA((NDEV,)),
            pltpu.SemaphoreType.DMA((NDEV,)),
            pltpu.SemaphoreType.DMA,
            pltpu.SemaphoreType.DMA,
        ],
        compiler_params=pltpu.CompilerParams(collective_id=0, has_side_effects=True, vmem_limit_bytes=60 * 2 ** 20),
    )(ints, ct, co, mdiag)


JBUF = 24


def fock_kernel(b_hbm, a_ref, md_ref, mo_ref, mx_ref, g_ref, k_ref, j_ref,
                ms, ts, jbuf, wb, jp, jsem):
    def fetch(c, slot):
        return pltpu.make_async_copy(b_hbm.at[c], jbuf.at[slot], jsem.at[slot])

    for c in range(JBUF):
        fetch(c, c).start()

    off = mo_ref[...]
    blocks = ((md_ref[...], off), (off.T, mx_ref[...]))

    gam = [jnp.sum(g_ref[r][:, 0:1, 0:QB], axis=0) for r in range(2)]
    fit = [sum(jnp.sum(blocks[r][s] * gam[s], axis=1, keepdims=True) for s in range(2)) for r in range(2)]
    wrow = sum(jnp.sum(blocks[r][0] * fit[r], axis=0, keepdims=True) for r in range(2))
    wb[...] = jnp.broadcast_to(wrow, (128, QB)).T

    ms[...] = jnp.zeros_like(ms)
    for r in range(2):
        for s in range(2):
            parts = split3(blocks[r][s])
            for j in range(3):
                ms[j, r * QP:r * QP + QB, s * QP:s * QP + QB] = parts[j]
    k_ref[...] = jnp.zeros_like(k_ref)

    def coulomb(lo, n):
        @pl.loop(0, n)
        def _(x):
            m = lo + x

            @pl.when(m < MB)
            def _():
                slot = lax.rem(m, JBUF)
                fetch(m, slot).wait()
                acc = [None] * 4
                for g in range(QB // 8):
                    w = wb[8 * g:8 * g + 8, :]
                    for lt in range(4):
                        l0, l1 = lt * 128, min(lt * 128 + 128, NB)
                        y = jbuf[slot, 8 * g:8 * g + 8, l0:l1] * w[:, 0:l1 - l0]
                        acc[lt] = y if acc[lt] is None else acc[lt] + y
                for lt in range(4):
                    l0, l1 = lt * 128, min(lt * 128 + 128, NB)
                    jp[m, :, l0:l1] = acc[lt]

                @pl.when(m + JBUF < MB)
                def _():
                    fetch(m + JBUF, slot).start()

    @pl.loop(0, IV)
    def _(v):
        t = None
        for s in range(2):
            a = a_ref[s, v]
            for j in range(3):
                x = jnp.dot(a, ms[j, s * QP:(s + 1) * QP, :], preferred_element_type=F32)
                t = x if t is None else t + x
        t1, t2, t3 = split3(t)
        ts[0], ts[1], ts[2] = t1, t2, t3
        coulomb(v * 24, 12)
        half = jnp.asarray(0.5, BF16)
        t1, t2, t3 = ts[0], ts[1], ts[2]
        s1 = lax.dot_general(t1, t1 * half, NT, preferred_element_type=F32)
        s1 = s1 + lax.dot_general(t1, t2, NT, preferred_element_type=F32)
        s1 = s1 + lax.dot_general(t1, t3, NT, preferred_element_type=F32)
        s1 = s1 + lax.dot_general(t2, t2 * half, NT, preferred_element_type=F32)
        k_ref[...] += s1
        coulomb(v * 24 + 12, 12)

    j_ref[...] = jnp.sum(jp[...], axis=1)
    k = k_ref[...]
    k_ref[...] = k + k.T


def fock_parts(ints, arecv, md, mo, mx, g):
    vmem, hbm = pl.BlockSpec(memory_space=pltpu.VMEM), pl.BlockSpec(memory_space=pl.ANY)
    return pl.pallas_call(
        fock_kernel,
        name='fock',
        out_shape=(jax.ShapeDtypeStruct((NORB * MP, NORB * MP), F32), jax.ShapeDtypeStruct((MB, NB), F32)),
        in_specs=[hbm] + [vmem] * 5,
        out_specs=(vmem, vmem),
        scratch_shapes=[
            pltpu.VMEM((3, 2 * QP, 2 * QP), BF16),
            pltpu.VMEM((3, NORB * MP, 2 * QP), BF16),
            pltpu.VMEM((JBUF, QB, NB), F32),
            pltpu.VMEM((QB, 128), F32),
            pltpu.VMEM((MB, 8, NB), F32),
            pltpu.SemaphoreType.DMA((JBUF,)),
        ],
        compiler_params=pltpu.CompilerParams(vmem_limit_bytes=63 * 2 ** 20),
    )(ints, arecv, md, mo, mx, g)


def solution(mesh):
    def local_fock(ints, metric, orbitals):
        aux, orb = lax.axis_index('aux'), lax.axis_index('orb')
        c = orbitals[0]
        ints = jnp.transpose(ints, (1, 0, 2))
        co = jnp.pad(lax.dynamic_slice_in_dim(c, orb * MB, MB, 0), ((0, MP - MB), (0, 128 - NI)))
        md = lax.dynamic_slice_in_dim(metric, aux * QB, QB, 1)
        mo = lax.dynamic_slice_in_dim(metric, (1 - aux) * QB, QB, 1)
        arecv, grecv, mx = half_transform(ints, c.T, co, md)
        arecv = jnp.where(aux == 0, arecv, arecv[::-1])
        g = grecv.reshape(NAUX, NORB, 8, QP)
        g = jnp.where(aux == 0, g, g[::-1])
        k, j = fock_parts(ints, arecv, md, mo, mx, g)
        k = k.reshape(NORB, MP, NORB, MP)[:, :MB, :, :MB].reshape(NB, NB)
        krow = lax.psum_scatter(k, 'orb', scatter_dimension=0, tiled=True)
        fock = 2.0 * j - krow
        return lax.psum_scatter(fock, 'aux', scatter_dimension=1, tiled=True)[None]

    return jax.shard_map(local_fock, mesh=mesh,
                         in_specs=(P(('sys', 'aux'), 'orb', None), P(('sys', 'aux'), None), P('sys', None, None)),
                         out_specs=P('sys', 'orb', 'aux'), check_vma=False)
```

```python
import jax
import jax.numpy as jnp
from jax import lax
from jax.experimental import pallas as pl
from jax.experimental.pallas import tpu as pltpu

P = jax.sharding.PartitionSpec
F32, BF16 = jnp.float32, jnp.bfloat16
MESH = pl.DeviceIdType.MESH
NT = (((1,), (1,)), ((), ()))

NAUX, NORB, NDEV = 2, 4, 8
QB, MB, NB, NI = 464, 116, 464, 40
IV = NI // NDEV
QP, MP = 512, 120
MC = 8
NCH = MP // MC
TAIL = MB - MC * (NCH - 1)
SP = 48
GR = 4
NG = MB // GR
NBUF = 4


def split3(x):
    a = x.astype(BF16)
    r = x - a.astype(F32)
    b = r.astype(BF16)
    c = (r - b.astype(F32)).astype(BF16)
    return a, b, c


def half_kernel(b_hbm, ct_ref, co_ref, md_hbm, arecv, grecv, mrecv,
                bbuf, bs, cw, abuf, sbuf, gbuf, gsend,
                bsem, ssem, rsem, osem, gs_sem, gr_sem, ms_sem, mr_sem):
    aux, orb = lax.axis_index('aux'), lax.axis_index('orb')
    me = aux * NORB + orb

    def at(d):
        return {'aux': d // NORB, 'orb': lax.rem(d, NORB)}

    def peer(t):
        return lax.rem(me + t, NDEV)

    def fetch(g):
        slot = g % NBUF if isinstance(g, int) else lax.rem(g, NBUF)
        return pltpu.make_async_copy(b_hbm.at[pl.ds(g * GR, GR)], bbuf.at[slot], bsem.at[slot])

    for g in range(NBUF - 1):
        fetch(g).start()

    barrier = pltpu.get_barrier_semaphore()
    for t in range(1, NDEV):
        pl.semaphore_signal(barrier, inc=1, device_id=at(peer(t)), device_id_type=MESH)

    abuf[...] = jnp.zeros_like(abuf)
    gbuf[...] = jnp.zeros_like(gbuf)
    c1, c2, c3 = split3(ct_ref[...])
    cw[...] = jnp.concatenate(
        [c1.astype(F32), c2.astype(F32), c3.astype(F32), jnp.zeros((8, NB), F32)], axis=0).astype(BF16)

    pl.semaphore_wait(barrier, NDEV - 1)
    mcopy = pltpu.make_async_remote_copy(md_hbm, mrecv, ms_sem, mr_sem,
                                         device_id={'aux': 1 - aux, 'orb': orb}, device_id_type=MESH)
    mcopy.start()

    def place(c):
        return arecv.at[aux, :, pl.ds(pl.multiple_of(orb * MP + c * MC, 8), MC), :]

    def send(c, slot, t):
        d = peer(t)
        return pltpu.make_async_remote_copy(sbuf.at[slot, d], place(c), ssem.at[slot, t], rsem.at[t],
                                            device_id=at(d), device_id_type=MESH)

    def own(c, slot):
        return pltpu.make_async_copy(sbuf.at[slot, me], place(c), osem.at[slot])

    def cut(g, half):
        slot = lax.rem(g, NBUF)
        for k in range(GR):
            for r in range(0, QB, 16):
                parts = split3(bbuf[slot, k, r:r + 16, :])
                for j in range(3):
                    bs[half * GR + k, j, r:r + 16, :] = parts[j]

    def dots(half):
        for k in range(half * GR, (half + 1) * GR):
            r = None
            for j in range(3):
                x = lax.dot_general(cw[...], bs[k, j], NT, preferred_element_type=F32)
                r = x if r is None else r + x
            a2 = r[0:NI] + r[NI:2 * NI] + r[2 * NI:3 * NI]
            for v in range(IV):
                for lt in range(4):
                    l0, l1 = lt * 128, min(lt * 128 + 128, QB)
                    abuf[lt, pl.ds(v * MC + k, NDEV, stride=SP), 0:l1 - l0] = a2[8 * v:8 * v + 8, l0:l1]

    def deliver(c):
        two = lax.rem(c, 2)
        g = gbuf[...]
        for s in range(NDEV):
            for v in range(IV):
                r0 = s * SP + v * MC
                col = co_ref[pl.ds(pl.multiple_of(c * MC, MC), MC), 8 * v + s:8 * v + s + 1]
                x = jnp.concatenate([abuf[lt, r0:r0 + MC, :] for lt in range(4)], axis=1)
                g = g + x * col
                sbuf[two, s, v] = x.astype(BF16)
        gbuf[...] = g
        for t in range(1, NDEV):
            send(c, two, t).start()
        own(c, two).start()

    def reuse(c):
        two = lax.rem(c, 2)

        @pl.when(c >= 2)
        def _():
            for t in range(1, NDEV):
                send(c - 2, two, t).wait_send()
            own(c - 2, two).wait()

    fetch(0).wait()
    cut(jnp.int32(0), 0)

    @pl.loop(0, NCH - 1)
    def _(c):
        fetch(2 * c + 1).wait()
        fetch(2 * c + 2).wait()

        @pl.when(2 * c + 3 < NG)
        def _():
            fetch(2 * c + 3).start()

        @pl.when(2 * c + 4 < NG)
        def _():
            fetch(2 * c + 4).start()

        reuse(c)
        cut(2 * c + 1, 1)
        dots(0)
        cut(2 * c + 2, 0)
        dots(1)
        deliver(c)

    reuse(jnp.int32(NCH - 1))
    abuf[...] = jnp.zeros_like(abuf)
    dots(0)
    deliver(jnp.int32(NCH - 1))

    gsend[...] = jnp.broadcast_to(jnp.sum(gbuf[...], axis=0, keepdims=True), (8, QP))

    def gcopy(t):
        return pltpu.make_async_remote_copy(gsend, grecv.at[me], gs_sem.at[t], gr_sem.at[t],
                                            device_id=at(peer(t)), device_id_type=MESH)

    for t in range(1, NDEV):
        gcopy(t).start()
    gown = pltpu.make_async_copy(gsend, grecv.at[me], gs_sem.at[0])
    gown.start()

    for c in (NCH - 2, NCH - 1):
        for t in range(1, NDEV):
            send(c, c % 2, t).wait_send()
        own(c, c % 2).wait()
    for t in range(1, NDEV):
        src = lax.rem(me + NDEV - t, NDEV)
        whole = arecv.at[src // NORB, :, pl.ds(pl.multiple_of(lax.rem(src, NORB) * MP, 8), MP), :]
        pltpu.make_async_remote_copy(whole, whole, rsem.at[t], rsem.at[t],
                                     device_id=at(src), device_id_type=MESH).wait_recv()
        pltpu.make_async_remote_copy(gsend, grecv.at[src], gs_sem.at[t], gr_sem.at[t],
                                     device_id=at(src), device_id_type=MESH).wait()
    gown.wait()
    mcopy.wait()


def half_transform(ints, ct, co, mdiag):
    vmem, hbm = pl.BlockSpec(memory_space=pltpu.VMEM), pl.BlockSpec(memory_space=pl.ANY)
    return pl.pallas_call(
        half_kernel,
        name='half',
        out_shape=(jax.ShapeDtypeStruct((NAUX, IV, NORB * MP, QP), BF16),
                   jax.ShapeDtypeStruct((NDEV, 8, QP), F32),
                   jax.ShapeDtypeStruct((QB, QB), F32)),
        in_specs=[hbm, vmem, vmem, hbm],
        out_specs=(hbm, hbm, hbm),
        scratch_shapes=[
            pltpu.VMEM((NBUF, GR, QB, NB), F32),
            pltpu.VMEM((2 * GR, 3, QB, NB), BF16),
            pltpu.VMEM((128, NB), BF16),
            pltpu.VMEM((4, NDEV * SP, 128), F32),
            pltpu.VMEM((2, NDEV, IV, MC, QP), BF16),
            pltpu.VMEM((MC, QP), F32),
            pltpu.VMEM((8, QP), F32),
            pltpu.SemaphoreType.DMA((NBUF,)),
            pltpu.SemaphoreType.DMA((2, NDEV)),
            pltpu.SemaphoreType.DMA((NDEV,)),
            pltpu.SemaphoreType.DMA((2,)),
            pltpu.SemaphoreType.DMA((NDEV,)),
            pltpu.SemaphoreType.DMA((NDEV,)),
            pltpu.SemaphoreType.DMA,
            pltpu.SemaphoreType.DMA,
        ],
        compiler_params=pltpu.CompilerParams(collective_id=0, has_side_effects=True, vmem_limit_bytes=60 * 2 ** 20),
    )(ints, ct, co, mdiag)


JB = 12
OB = NB // NAUX


def fock_kernel(b_hbm, a_ref, md_ref, mo_ref, mx_ref, g_ref, out_ref,
                ms, ts, jbuf, wb, jp, kacc, kout, kin, jsem, ssem, rsem):
    aux, orb = lax.axis_index('aux'), lax.axis_index('orb')
    me = aux * NORB + orb
    side = (aux, 1 - aux)

    def at(d):
        return {'aux': d // NORB, 'orb': lax.rem(d, NORB)}

    def fetch(m, slot):
        return pltpu.make_async_copy(b_hbm.at[m], jbuf.at[slot], jsem.at[slot])

    for c in range(2 * JB):
        fetch(c, c).start()

    barrier = pltpu.get_barrier_semaphore()
    for t in range(1, NDEV):
        pl.semaphore_signal(barrier, inc=1, device_id=at(lax.rem(me + t, NDEV)), device_id_type=MESH)

    off = mo_ref[...]
    blocks = ((md_ref[...], off), (off.T, mx_ref[...]))

    gam = [sum(g_ref[side[r] * NORB + o][0:1, 0:QB] for o in range(NORB)) for r in range(2)]
    fit = [sum(jnp.sum(blocks[r][s] * gam[s], axis=1, keepdims=True) for s in range(2)) for r in range(2)]
    wrow = sum(jnp.sum(blocks[r][0] * fit[r], axis=0, keepdims=True) for r in range(2))
    wb[...] = jnp.broadcast_to(wrow, (128, QB)).T

    ms[...] = jnp.zeros_like(ms)
    for r in range(2):
        for s in range(2):
            parts = split3(blocks[r][s])
            for j in range(3):
                ms[j, r * QP:r * QP + QB, s * QP:s * QP + QB] = parts[j]
    kacc[...] = jnp.zeros_like(kacc)

    def arrive(lo, base):
        for x in range(JB):
            @pl.when(lo + x < MB)
            def _():
                fetch(lo + x, base + x).wait()

    def coulomb(lo, base):
        for x in range(JB):
            acc = [None] * 4
            for g in range(QB // 8):
                w = wb[8 * g:8 * g + 8, :]
                for lt in range(4):
                    l0, l1 = lt * 128, min(lt * 128 + 128, NB)
                    y = jbuf[base + x, 8 * g:8 * g + 8, l0:l1] * w[:, 0:l1 - l0]
                    acc[lt] = y if acc[lt] is None else acc[lt] + y
            for lt in range(4):
                l0, l1 = lt * 128, min(lt * 128 + 128, NB)
                jp[lo + x, :, l0:l1] = acc[lt]

    def refill(lo, base):
        for x in range(JB):
            @pl.when(lo + 2 * JB + x < MB)
            def _():
                fetch(lo + 2 * JB + x, base + x).start()

    @pl.loop(0, IV)
    def _(v):
        lo = v * 2 * JB
        arrive(lo, 0)
        t = None
        for s in range(2):
            a = a_ref[side[s], v]
            for j in range(3):
                x = jnp.dot(a, ms[j, s * QP:(s + 1) * QP, :], preferred_element_type=F32)
                t = x if t is None else t + x
        ts[0], ts[1], ts[2] = split3(t)
        coulomb(lo, 0)
        refill(lo, 0)
        arrive(lo + JB, JB)
        half = jnp.asarray(0.5, BF16)
        t1, t2, t3 = ts[0], ts[1], ts[2]
        s1 = lax.dot_general(t1, t1 * half, NT, preferred_element_type=F32)
        s1 = s1 + lax.dot_general(t1, t2, NT, preferred_element_type=F32)
        s1 = s1 + lax.dot_general(t1, t3, NT, preferred_element_type=F32)
        s1 = s1 + lax.dot_general(t2, t2 * half, NT, preferred_element_type=F32)
        kacc[...] += s1
        coulomb(lo + JB, JB)
        refill(lo + JB, JB)

    k = kacc[...]
    k = k + k.T
    for a in range(NAUX):
        cols = jnp.concatenate([k[:, o * MP:o * MP + MB] for o in (2 * a, 2 * a + 1)], axis=1)
        for o in range(NORB):
            kout[a * NORB + o, :, 0:OB] = -cols[o * MP:(o + 1) * MP]
    j = jnp.sum(jp[...], axis=1)
    for a in range(NAUX):
        kout[a * NORB + orb, :, 0:OB] += 2.0 * j[:, a * OB:(a + 1) * OB]

    def send(t):
        d = lax.rem(me + t, NDEV)
        return pltpu.make_async_remote_copy(kout.at[d], kin.at[t], ssem.at[t], rsem.at[t],
                                            device_id=at(d), device_id_type=MESH)

    pl.semaphore_wait(barrier, NDEV - 1)
    for t in range(1, NDEV):
        send(t).start()
    total = kout[me]
    for t in range(1, NDEV):
        send(t).wait_recv()
        total = total + kin[t]
    out_ref[...] = total[0:MB, 0:OB]
    for t in range(1, NDEV):
        send(t).wait_send()


def fock_parts(ints, arecv, md, mo, mx, g):
    vmem, hbm = pl.BlockSpec(memory_space=pltpu.VMEM), pl.BlockSpec(memory_space=pl.ANY)
    return pl.pallas_call(
        fock_kernel,
        name='fock',
        out_shape=jax.ShapeDtypeStruct((MB, OB), F32),
        in_specs=[hbm] + [vmem] * 5,
        out_specs=vmem,
        scratch_shapes=[
            pltpu.VMEM((3, 2 * QP, 2 * QP), BF16),
            pltpu.VMEM((3, NORB * MP, 2 * QP), BF16),
            pltpu.VMEM((2 * JB, QB, NB), F32),
            pltpu.VMEM((QB, 128), F32),
            pltpu.VMEM((MP, 8, NB), F32),
            pltpu.VMEM((NORB * MP, NORB * MP), F32),
            pltpu.VMEM((NDEV, MP, 256), F32),
            pltpu.VMEM((NDEV, MP, 256), F32),
            pltpu.SemaphoreType.DMA((2 * JB,)),
            pltpu.SemaphoreType.DMA((NDEV,)),
            pltpu.SemaphoreType.DMA((NDEV,)),
        ],
        compiler_params=pltpu.CompilerParams(collective_id=1, has_side_effects=True, vmem_limit_bytes=63 * 2 ** 20),
    )(ints, arecv, md, mo, mx, g)


def solution(mesh):
    def local_fock(ints, metric, orbitals):
        aux, orb = lax.axis_index('aux'), lax.axis_index('orb')
        c = orbitals[0]
        ints = jnp.transpose(ints, (1, 0, 2))
        co = jnp.pad(lax.dynamic_slice_in_dim(c, orb * MB, MB, 0), ((0, MP - MB), (0, 128 - NI)))
        md = lax.dynamic_slice_in_dim(metric, aux * QB, QB, 1)
        mo = lax.dynamic_slice_in_dim(metric, (1 - aux) * QB, QB, 1)
        arecv, grecv, mx = half_transform(ints, c.T, co, md)
        return fock_parts(ints, arecv, md, mo, mx, grecv)[None]

    return jax.shard_map(local_fock, mesh=mesh,
                         in_specs=(P(('sys', 'aux'), 'orb', None), P(('sys', 'aux'), None), P('sys', None, None)),
                         out_specs=P('sys', 'orb', 'aux'), check_vma=False)
```

```python
import jax
import jax.numpy as jnp
from jax import lax
from jax.experimental import pallas as pl
from jax.experimental.pallas import tpu as pltpu

P = jax.sharding.PartitionSpec
F32, BF16 = jnp.float32, jnp.bfloat16
MESH = pl.DeviceIdType.MESH
NT = (((1,), (1,)), ((), ()))
LN2 = 0.6931471805599453
TOP = 126.0
ROUND = 1.5 * 2.0 ** 15

NAUX, NORB, NDEV = 2, 4, 8
QB, MB, NB, NI = 464, 116, 464, 40
IV = NI // NDEV
QP, MP = 512, 120
MC = 8
NCH = MP // MC
TAIL = MB - MC * (NCH - 1)
SP = 48
GR = 4
NG = MB // GR
NBUF = 4
NST = (NG + 1) // 2
OB = NB // NAUX
HQ = QB // 2


def split3(x):
    a = x.astype(BF16)
    r = x - a.astype(F32)
    b = r.astype(BF16)
    c = (r - b.astype(F32)).astype(BF16)
    return a, b, c


def kernel(b_hbm, ct_ref, co_ref, m_ref, out_ref,
           bbuf, bs, cw, abuf, sbuf, arecv, own, gbuf, gsend, grecv,
           md, mx, ms, aspl, af, ts, wb, jp, kacc, kout, kin,
           bsem, ssem, rsem, gs_sem, gr_sem, ms_sem, mr_sem, ks_sem, kr_sem):
    aux, orb = lax.axis_index('aux'), lax.axis_index('orb')
    me = aux * NORB + orb
    core = lax.rem(orb, 2)
    side = (aux, 1 - aux)

    def at(d):
        return {'aux': d // NORB, 'orb': lax.rem(d, NORB)}

    def peer(t):
        return lax.rem(me + t, NDEV)

    def fetch(g):
        slot = g % NBUF if isinstance(g, int) else lax.rem(g, NBUF)
        return pltpu.make_async_copy(b_hbm.at[pl.ds(g * GR, GR)], bbuf.at[slot], bsem.at[slot])

    for g in range(NBUF - 1):
        fetch(g).start()

    barrier = pltpu.get_barrier_semaphore()
    for t in range(1, NDEV):
        pl.semaphore_signal(barrier, inc=1, device_id=at(peer(t)), device_id_type=MESH)

    for a in range(NAUX):
        @pl.when(aux == a)
        def _():
            md[...] = m_ref[:, a * QB:(a + 1) * QB]

    abuf[...] = jnp.zeros_like(abuf)
    gbuf[...] = jnp.zeros_like(gbuf)
    c1, c2, c3 = split3(ct_ref[...])
    cw[...] = jnp.concatenate(
        [c1.astype(F32), c2.astype(F32), c3.astype(F32), jnp.zeros((8, NB), F32)], axis=0).astype(BF16)

    pl.semaphore_wait(barrier, NDEV - 1)

    def mcopy(src, k, rows, dev):
        block = pl.ds(pl.multiple_of(rows * HQ, 8), HQ)
        return pltpu.make_async_remote_copy(src.at[block], mx.at[block], ms_sem.at[k], mr_sem.at[k],
                                            device_id=dev, device_id_type=MESH)
    mfirst = mcopy(md, 0, core, {'aux': 1 - aux, 'orb': orb})
    mfirst.start()

    def send(c, slot, t):
        d = peer(t)
        return pltpu.make_async_remote_copy(sbuf.at[slot, d], arecv.at[aux, :, orb * NCH + c],
                                            ssem.at[slot, t], rsem.at[t], device_id=at(d), device_id_type=MESH)

    def cut(g, half):
        slot = lax.rem(g, NBUF)
        for k in range(GR):
            for r in range(0, QB, 16):
                parts = split3(bbuf[slot, k, r:r + 16, :])
                for j in range(3):
                    bs[half * GR + k, j, r:r + 16, :] = parts[j]

    def dots(half):
        for k in range(half * GR, (half + 1) * GR):
            r = None
            for j in range(3):
                x = lax.dot_general(cw[...], bs[k, j], NT, preferred_element_type=F32)
                r = x if r is None else r + x
            a2 = r[0:NI] + r[NI:2 * NI] + r[2 * NI:3 * NI]
            for v in range(IV):
                for lt in range(4):
                    l0, l1 = lt * 128, min(lt * 128 + 128, QB)
                    abuf[lt, pl.ds(v * MC + k, NDEV, stride=SP), 0:l1 - l0] = a2[8 * v:8 * v + 8, l0:l1]

    lane = lax.broadcasted_iota(jnp.int32, (MC, QP), 1)

    def deliver(c):
        two = lax.rem(c, 2)
        g = gbuf[...]
        for s in range(NDEV):
            for v in range(IV):
                r0 = s * SP + v * MC
                col = co_ref[pl.ds(pl.multiple_of(c * MC, MC), MC), 8 * v + s:8 * v + s + 1]
                x = jnp.concatenate([abuf[lt, r0:r0 + MC, :] for lt in range(4)], axis=1)
                g = g + x * col
                big = jnp.maximum(jnp.max(jnp.abs(x), axis=1, keepdims=True), 2.0 ** -100)
                j = jnp.ceil(jnp.log(big * (1.0 / TOP)) * (1.0 / LN2) + 0.01)
                up = jnp.exp2(j).astype(BF16).astype(F32)
                down = jnp.exp2(-j).astype(BF16).astype(F32)
                y = jnp.exp2(x * down)
                sbuf[two, s, v] = jnp.where(lane < QB, y, up).astype(BF16)
        gbuf[...] = g
        for v in range(IV):
            r0 = pl.multiple_of(me * SP + v * MC, 8)
            own[v, pl.ds(pl.multiple_of(c * MC, MC), MC), :] = jnp.concatenate(
                [abuf[lt, pl.ds(r0, MC), :] for lt in range(4)], axis=1)
        for t in range(1, NDEV):
            send(c, two, t).start()

    def reuse(c):
        two = lax.rem(c, 2)

        @pl.when(c >= 2)
        def _():
            for t in range(1, NDEV):
                send(c - 2, two, t).wait_send()

    fetch(0).wait()
    cut(jnp.int32(0), 0)

    @pl.loop(0, NCH - 1)
    def _(c):
        fetch(2 * c + 1).wait()
        fetch(2 * c + 2).wait()

        @pl.when(2 * c + 3 < NG)
        def _():
            fetch(2 * c + 3).start()

        @pl.when(2 * c + 4 < NG)
        def _():
            fetch(2 * c + 4).start()

        reuse(c)
        cut(2 * c + 1, 1)
        dots(0)
        cut(2 * c + 2, 0)
        dots(1)
        deliver(c)

    for g in range(NBUF):
        fetch(g).start()
    reuse(jnp.int32(NCH - 1))
    abuf[...] = jnp.zeros_like(abuf)
    dots(0)
    deliver(jnp.int32(NCH - 1))

    gsend[...] = jnp.broadcast_to(jnp.sum(gbuf[...], axis=0, keepdims=True), (8, QP))

    def gcopy(t):
        return pltpu.make_async_remote_copy(gsend, grecv.at[me], gs_sem.at[t], gr_sem.at[t],
                                            device_id=at(peer(t)), device_id_type=MESH)

    for t in range(1, NDEV):
        gcopy(t).start()
    grecv[me] = gsend[...]

    mfirst.wait()
    msecond = mcopy(mx, 1, core, {'orb': orb + 1 - 2 * core})
    msecond.start()

    ms[...] = jnp.zeros_like(ms)

    def parts_of(x, r, s):
        parts = split3(x)
        for j in range(3):
            ms[j, r * QP:r * QP + QB, s * QP:s * QP + QB] = parts[j]

    parts_of(md[...], 0, 0)
    for a in range(NAUX):
        @pl.when(aux == a)
        def _():
            off = m_ref[:, (1 - a) * QB:(2 - a) * QB]
            af[0:QB, 0:QB] = off
    parts_of(af[0:QB, 0:QB], 0, 1)
    parts_of(af[0:QB, 0:QB].T, 1, 0)
    msecond.wait_send()
    mcopy(mx, 1, 1 - core, {'orb': orb + 1 - 2 * core}).wait_recv()
    parts_of(mx[...], 1, 1)
    kacc[...] = jnp.zeros_like(kacc)

    for t in range(1, NDEV):
        src = lax.rem(me + NDEV - t, NDEV)
        pltpu.make_async_remote_copy(gsend, grecv.at[src], gs_sem.at[t], gr_sem.at[t],
                                     device_id=at(src), device_id_type=MESH).wait()
    off = af[0:QB, 0:QB]
    gam = [sum(grecv[side[r] * NORB + o][0:1, 0:QB] for o in range(NORB)) for r in range(2)]
    fit0 = jnp.sum(md[...] * gam[0], axis=1, keepdims=True) + jnp.sum(off * gam[1], axis=1, keepdims=True)
    turn = jnp.broadcast_to(gam[0], (128, QB)).T
    fit1 = (jnp.sum(off * turn[:, 0:1], axis=0, keepdims=True)
            + jnp.sum(mx[...] * jnp.broadcast_to(gam[1], (128, QB)).T[:, 0:1], axis=0, keepdims=True))
    wcol = jnp.sum(off * fit1, axis=1, keepdims=True)
    wrow = jnp.sum(md[...] * fit0, axis=0, keepdims=True)
    wb[...] = jnp.broadcast_to(wrow, (128, QB)).T + wcol

    def coulomb(s, base):
        for x in range(2):
            @pl.when(2 * s + x < NG)
            def _():
                fetch(2 * s + x).wait()
        for x in range(2 * GR):
            for l0, l1 in ((0, 128), (128, 256), (256, 384), (384, NB)):
                y = bbuf[base + x // GR, x % GR, :, l0:l1] * wb[:, 0:l1 - l0]
                jp[2 * GR * s + x, :, l0:l1] = jnp.sum(y.reshape(QB // 8, 8, l1 - l0), axis=0)
        for x in range(2):
            @pl.when(2 * s + NBUF + x < NG)
            def _():
                fetch(2 * s + NBUF + x).start()

    EARLY = NST - 2 * IV

    @pl.loop(0, EARLY)
    def _(s):
        coulomb(s, 2 * lax.rem(s, 2))

    for c in (NCH - 2, NCH - 1):
        for t in range(1, NDEV):
            send(c, c % 2, t).wait_send()
    for t in range(1, NDEV):
        src = lax.rem(me + NDEV - t, NDEV)
        whole = arecv.at[src // NORB, :, pl.ds(lax.rem(src, NORB) * NCH, NCH)]
        pltpu.make_async_remote_copy(whole, whole, rsem.at[t], rsem.at[t],
                                     device_id=at(src), device_id_type=MESH).wait_recv()

    PAIRS = ((0, 0), (0, 1), (1, 0), (1, 1), (0, 2), (2, 0))

    @pl.loop(0, IV)
    def _(v):
        def decode(sd, r):
            y = arecv[side[sd], v, r // MC:r // MC + 2].astype(F32).reshape(2 * MC, QP)
            u = jnp.log(y) * (1.0 / LN2)
            return ((u + ROUND) - ROUND) * y[:, QB:QB + 1]

        for r in range(0, NORB * MP, 16):
            af[r:r + 16, :] = decode(0, r)
        af[pl.ds(pl.multiple_of(orb * MP, 8), MP), :] = own[v]
        for r in range(0, NORB * MP, 16):
            for j, x in enumerate(split3(af[r:r + 16, :])):
                aspl[j, r:r + 16, :] = x
            for j, x in enumerate(split3(decode(1, r))[:2]):
                aspl[3 + j, r:r + 16, :] = x
        t = None
        for sd in range(2):
            for i, j in PAIRS[:6 - sd]:
                x = jnp.dot(aspl[3 * sd + i], ms[j, sd * QP:(sd + 1) * QP, :], preferred_element_type=F32)
                t = x if t is None else t + x
        ts[0], ts[1], ts[2] = split3(t)
        coulomb(EARLY + 2 * v, 2 * (EARLY % 2))
        half = jnp.asarray(0.5, BF16)
        t1, t2, t3 = ts[0], ts[1], ts[2]
        s1 = lax.dot_general(t1, t1 * half, NT, preferred_element_type=F32)
        s1 = s1 + lax.dot_general(t1, t2, NT, preferred_element_type=F32)
        s1 = s1 + lax.dot_general(t1, t3, NT, preferred_element_type=F32)
        s1 = s1 + lax.dot_general(t2, t2 * half, NT, preferred_element_type=F32)
        kacc[...] += s1
        coulomb(EARLY + 2 * v + 1, 2 - 2 * (EARLY % 2))

    k = kacc[...]
    k = k + k.T
    for a in range(NAUX):
        cols = jnp.concatenate([k[:, o * MP:o * MP + MB] for o in (2 * a, 2 * a + 1)], axis=1)
        for o in range(NORB):
            kout[a * NORB + o, :, 0:OB] = -cols[o * MP:(o + 1) * MP]
    j = jnp.sum(jp[...], axis=1)
    for a in range(NAUX):
        kout[a * NORB + orb, :, 0:OB] += 2.0 * j[:, a * OB:(a + 1) * OB]

    def give(t):
        d = peer(t)
        return pltpu.make_async_remote_copy(kout.at[d], kin.at[t], ks_sem.at[t], kr_sem.at[t],
                                            device_id=at(d), device_id_type=MESH)

    for t in range(1, NDEV):
        give(t).start()
    total = kout[me]
    for t in range(1, NDEV):
        give(t).wait_recv()
        total = total + kin[t]
    out_ref[...] = total[0:MB, 0:OB]
    for t in range(1, NDEV):
        give(t).wait_send()


def fock(ints, ct, co, metric):
    vmem, hbm = pl.BlockSpec(memory_space=pltpu.VMEM), pl.BlockSpec(memory_space=pl.ANY)
    dma = pltpu.SemaphoreType.DMA
    return pl.pallas_call(
        kernel,
        name='fock',
        out_shape=jax.ShapeDtypeStruct((MB, OB), F32),
        in_specs=[hbm, vmem, vmem, vmem],
        out_specs=vmem,
        scratch_shapes=[
            pltpu.VMEM((NBUF, GR, QB, NB), F32),
            pltpu.VMEM((2 * GR, 3, QB, NB), BF16),
            pltpu.VMEM((128, NB), BF16),
            pltpu.VMEM((4, NDEV * SP, 128), F32),
            pltpu.VMEM((2, NDEV, IV, MC, QP), BF16),
            pltpu.VMEM((NAUX, IV, NORB * NCH, MC, QP), BF16),
            pltpu.VMEM((IV, MP, QP), F32),
            pltpu.VMEM((MC, QP), F32),
            pltpu.VMEM((8, QP), F32),
            pltpu.VMEM((NDEV, 8, QP), F32),
            pltpu.VMEM((QB, QB), F32),
            pltpu.VMEM((QB, QB), F32),
            pltpu.VMEM((3, 2 * QP, 2 * QP), BF16),
            pltpu.VMEM((5, NORB * MP, QP), BF16),
            pltpu.VMEM((NORB * MP, QP), F32),
            pltpu.VMEM((3, NORB * MP, 2 * QP), BF16),
            pltpu.VMEM((QB, 128), F32),
            pltpu.VMEM((MP, 8, NB), F32),
            pltpu.VMEM((NORB * MP, NORB * MP), F32),
            pltpu.VMEM((NDEV, MP, 256), F32),
            pltpu.VMEM((NDEV, MP, 256), F32),
            dma((NBUF,)), dma((2, NDEV)), dma((NDEV,)), dma((NDEV,)), dma((NDEV,)),
            dma((2,)), dma((2,)), dma((NDEV,)), dma((NDEV,)),
        ],
        compiler_params=pltpu.CompilerParams(collective_id=0, has_side_effects=True, vmem_limit_bytes=67043328),
    )(ints, ct, co, metric)


def solution(mesh):
    def local_fock(ints, metric, orbitals):
        orb = lax.axis_index('orb')
        c = orbitals[0]
        co = jnp.pad(lax.dynamic_slice_in_dim(c, orb * MB, MB, 0), ((0, MP - MB), (0, 128 - NI)))
        return fock(jnp.transpose(ints, (1, 0, 2)), c.T, co, metric)[None]

    return jax.shard_map(local_fock, mesh=mesh,
                         in_specs=(P(('sys', 'aux'), 'orb', None), P(('sys', 'aux'), None), P('sys', None, None)),
                         out_specs=P('sys', 'orb', 'aux'), check_vma=False)
```

```python
import jax
import jax.numpy as jnp
from jax import lax
from jax.experimental import pallas as pl
from jax.experimental.pallas import tpu as pltpu

P = jax.sharding.PartitionSpec
F32, BF16 = jnp.float32, jnp.bfloat16
MESH = pl.DeviceIdType.MESH
NT = (((1,), (1,)), ((), ()))
LN2 = 0.6931471805599453
TOP = 126.0
ROUND = 1.5 * 2.0 ** 15

NAUX, NORB, NDEV = 2, 4, 8
QB, MB, NB, NI = 464, 116, 464, 40
IV = NI // NDEV
QP, MP = 512, 120
MC = 8
NCH = MP // MC
TAIL = MB - MC * (NCH - 1)
SP = 48
GR = 4
NG = MB // GR
NBUF = 4
NST = (NG + 1) // 2
OB = NB // NAUX
HQ = QB // 2


def split3(x):
    a = x.astype(BF16)
    r = x - a.astype(F32)
    b = r.astype(BF16)
    c = (r - b.astype(F32)).astype(BF16)
    return a, b, c


def kernel(b_hbm, ct_ref, co_ref, m_ref, out_ref,
           bbuf, bs, cw, abuf, sbuf, arecv, own, gbuf, gsend, grecv,
           md, mx, ms, af, wb, jp, kacc, kout, kin,
           bsem, ssem, rsem, gs_sem, gr_sem, ms_sem, mr_sem, ks_sem, kr_sem):
    aux, orb = lax.axis_index('aux'), lax.axis_index('orb')
    me = aux * NORB + orb
    core = lax.rem(orb, 2)
    side = (aux, 1 - aux)

    def at(d):
        return {'aux': d // NORB, 'orb': lax.rem(d, NORB)}

    def peer(t):
        return lax.rem(me + t, NDEV)

    def fetch(g):
        slot = g % NBUF if isinstance(g, int) else lax.rem(g, NBUF)
        return pltpu.make_async_copy(b_hbm.at[pl.ds(g * GR, GR)], bbuf.at[pl.ds(slot * GR, GR)], bsem.at[slot])

    for g in range(NBUF - 1):
        fetch(g).start()

    barrier = pltpu.get_barrier_semaphore()
    for t in range(1, NDEV):
        pl.semaphore_signal(barrier, inc=1, device_id=at(peer(t)), device_id_type=MESH)

    for a in range(NAUX):
        @pl.when(aux == a)
        def _():
            md[...] = m_ref[:, a * QB:(a + 1) * QB]

    abuf[...] = jnp.zeros_like(abuf)
    gbuf[...] = jnp.zeros_like(gbuf)
    c1, c2, c3 = split3(ct_ref[...])
    cw[...] = jnp.concatenate(
        [c1.astype(F32), c2.astype(F32), c3.astype(F32), jnp.zeros((8, NB), F32)], axis=0).astype(BF16)

    pl.semaphore_wait(barrier, NDEV - 1)

    def mcopy(src, k, rows, dev):
        block = pl.ds(pl.multiple_of(rows * HQ, 8), HQ)
        return pltpu.make_async_remote_copy(src.at[block], mx.at[block], ms_sem.at[k], mr_sem.at[k],
                                            device_id=dev, device_id_type=MESH)
    mfirst = mcopy(md, 0, core, {'aux': 1 - aux, 'orb': orb})
    mfirst.start()

    def send(c, t):
        d = peer(t)
        return pltpu.make_async_remote_copy(sbuf.at[c, d], arecv.at[aux, :, orb * NCH + c],
                                            ssem.at[t], rsem.at[t], device_id=at(d), device_id_type=MESH)

    def cut(g, half):
        slot = lax.rem(g, NBUF)
        for k in range(GR):
            for r in range(0, QB, 16):
                parts = split3(bbuf[slot * GR + k, r:r + 16, :])
                for j in range(3):
                    bs[3 * (half * GR + k) + j, r:r + 16, 0:NB] = parts[j]

    def dots(half):
        for k in range(half * GR, (half + 1) * GR):
            r = None
            for j in range(3):
                x = lax.dot_general(cw[...], bs[3 * k + j, 0:QB, 0:NB], NT, preferred_element_type=F32)
                r = x if r is None else r + x
            a2 = r[0:NI] + r[NI:2 * NI] + r[2 * NI:3 * NI]
            for v in range(IV):
                for lt in range(4):
                    l0, l1 = lt * 128, min(lt * 128 + 128, QB)
                    abuf[lt, pl.ds(v * MC + k, NDEV, stride=SP), 0:l1 - l0] = a2[8 * v:8 * v + 8, l0:l1]

    lane = lax.broadcasted_iota(jnp.int32, (MC, QP), 1)

    def deliver(c):
        g = gbuf[...]
        for s in range(NDEV):
            for v in range(IV):
                r0 = s * SP + v * MC
                col = co_ref[pl.ds(pl.multiple_of(c * MC, MC), MC), 8 * v + s:8 * v + s + 1]
                x = jnp.concatenate([abuf[lt, r0:r0 + MC, :] for lt in range(4)], axis=1)
                g = g + x * col
                big = jnp.maximum(jnp.max(jnp.abs(x), axis=1, keepdims=True), 2.0 ** -100)
                j = jnp.ceil(jnp.log(big * (1.0 / TOP)) * (1.0 / LN2) + 0.01)
                up = jnp.exp2(j).astype(BF16).astype(F32)
                down = jnp.exp2(-j).astype(BF16).astype(F32)
                y = jnp.exp2(x * down)
                sbuf[c, s, v] = jnp.where(lane < QB, y, up).astype(BF16)
        gbuf[...] = g
        for v in range(IV):
            r0 = pl.multiple_of(me * SP + v * MC, 8)
            own[v, pl.ds(pl.multiple_of(c * MC, MC), MC), :] = jnp.concatenate(
                [abuf[lt, pl.ds(r0, MC), :] for lt in range(4)], axis=1)
        for t in range(1, NDEV):
            send(c, t).start()

    fetch(0).wait()
    cut(jnp.int32(0), 0)

    @pl.loop(0, NCH - 1)
    def _(c):
        fetch(2 * c + 1).wait()
        fetch(2 * c + 2).wait()

        @pl.when(2 * c + 3 < NG)
        def _():
            fetch(2 * c + 3).start()

        @pl.when(2 * c + 4 < NG)
        def _():
            fetch(2 * c + 4).start()

        cut(2 * c + 1, 1)
        dots(0)
        cut(2 * c + 2, 0)
        dots(1)
        deliver(c)

    for g in range(NBUF):
        fetch(g).start()
    abuf[...] = jnp.zeros_like(abuf)
    dots(0)
    deliver(jnp.int32(NCH - 1))

    gsend[...] = jnp.broadcast_to(jnp.sum(gbuf[...], axis=0, keepdims=True), (8, QP))

    def gcopy(t):
        return pltpu.make_async_remote_copy(gsend, grecv.at[me], gs_sem.at[t], gr_sem.at[t],
                                            device_id=at(peer(t)), device_id_type=MESH)

    for t in range(1, NDEV):
        gcopy(t).start()
    grecv[me] = gsend[...]

    mfirst.wait()
    msecond = mcopy(mx, 1, core, {'orb': orb + 1 - 2 * core})
    msecond.start()

    ms[...] = jnp.zeros_like(ms)

    def parts_of(x, r, s):
        parts = split3(x)
        for j in range(3):
            ms[j, r * QP:r * QP + QB, s * QP:s * QP + QB] = parts[j]

    parts_of(md[...], 0, 0)
    for a in range(NAUX):
        @pl.when(aux == a)
        def _():
            off = m_ref[:, (1 - a) * QB:(2 - a) * QB]
            af[0:QB, 0:QB] = off
    parts_of(af[0:QB, 0:QB], 0, 1)
    parts_of(af[0:QB, 0:QB].T, 1, 0)
    msecond.wait_send()
    mcopy(mx, 1, 1 - core, {'orb': orb + 1 - 2 * core}).wait_recv()
    parts_of(mx[...], 1, 1)
    kacc[...] = jnp.zeros_like(kacc)

    for t in range(1, NDEV):
        src = lax.rem(me + NDEV - t, NDEV)
        pltpu.make_async_remote_copy(gsend, grecv.at[src], gs_sem.at[t], gr_sem.at[t],
                                     device_id=at(src), device_id_type=MESH).wait()
    off = af[0:QB, 0:QB]
    gam = [sum(grecv[side[r] * NORB + o][0:1, 0:QB] for o in range(NORB)) for r in range(2)]
    fit0 = jnp.sum(md[...] * gam[0], axis=1, keepdims=True) + jnp.sum(off * gam[1], axis=1, keepdims=True)
    turn = jnp.broadcast_to(gam[0], (128, QB)).T
    fit1 = (jnp.sum(off * turn[:, 0:1], axis=0, keepdims=True)
            + jnp.sum(mx[...] * jnp.broadcast_to(gam[1], (128, QB)).T[:, 0:1], axis=0, keepdims=True))
    wcol = jnp.sum(off * fit1, axis=1, keepdims=True)
    wrow = jnp.sum(md[...] * fit0, axis=0, keepdims=True)
    wb[...] = jnp.broadcast_to(wrow, (128, QB)).T + wcol

    def coulomb(s, base):
        for x in range(2):
            @pl.when(2 * s + x < NG)
            def _():
                fetch(2 * s + x).wait()
        @pl.loop(0, 2 * GR)
        def _(x):
            for l0, l1 in ((0, 128), (128, 256), (256, 384), (384, NB)):
                y = bbuf[base * GR + x, :, l0:l1] * wb[:, 0:l1 - l0]
                jp[2 * GR * s + x, :, l0:l1] = jnp.sum(y.reshape(QB // 8, 8, l1 - l0), axis=0)

        for x in range(2):
            @pl.when(2 * s + NBUF + x < NG)
            def _():
                fetch(2 * s + NBUF + x).start()

    EARLY = NST - 2 * IV

    @pl.loop(0, EARLY)
    def _(s):
        coulomb(s, 2 * lax.rem(s, 2))

    for t in range(1, NDEV):
        src = lax.rem(me + NDEV - t, NDEV)
        whole = arecv.at[src // NORB, :, pl.ds(lax.rem(src, NORB) * NCH, NCH)]
        arrived = pltpu.make_async_remote_copy(whole, whole, ssem.at[t], rsem.at[t],
                                               device_id=at(src), device_id_type=MESH)
        arrived.wait_send()
        arrived.wait_recv()

    PAIRS = ((0, 0), (0, 1), (1, 0), (1, 1), (0, 2), (2, 0))

    @pl.loop(0, IV)
    def _(v):
        def decode(sd, r):
            y = arecv[side[sd], v, r // MC:r // MC + 2].astype(F32).reshape(2 * MC, QP)
            u = jnp.log(y) * (1.0 / LN2)
            return ((u + ROUND) - ROUND) * y[:, QB:QB + 1]

        for r in range(0, NORB * MP, 16):
            af[r:r + 16, :] = decode(0, r)
        af[pl.ds(pl.multiple_of(orb * MP, 8), MP), :] = own[v]
        for r in range(0, NORB * MP, 16):
            for j, x in enumerate(split3(af[r:r + 16, :])):
                bs[j, r:r + 16, :] = x
            for j, x in enumerate(split3(decode(1, r))[:2]):
                bs[3 + j, r:r + 16, :] = x
        t = None
        for sd in range(2):
            for i, j in PAIRS[:6 - sd]:
                x = jnp.dot(bs[3 * sd + i], ms[j, sd * QP:(sd + 1) * QP, :], preferred_element_type=F32)
                t = x if t is None else t + x
        for j, x in enumerate(split3(t)):
            bs[5 + j], bs[8 + j] = x[:, 0:QP], x[:, QP:2 * QP]
        coulomb(EARLY + 2 * v, 2 * (EARLY % 2))
        half = jnp.asarray(0.5, BF16)
        s1 = None
        for b in (5, 8):
            t1, t2, t3 = bs[b], bs[b + 1], bs[b + 2]
            for x, y in ((t1, t1 * half), (t1, t2), (t1, t3), (t2, t2 * half)):
                z = lax.dot_general(x, y, NT, preferred_element_type=F32)
                s1 = z if s1 is None else s1 + z
        kacc[...] += s1
        coulomb(EARLY + 2 * v + 1, 2 - 2 * (EARLY % 2))

    k = kacc[...]
    k = k + k.T
    for a in range(NAUX):
        cols = jnp.concatenate([k[:, o * MP:o * MP + MB] for o in (2 * a, 2 * a + 1)], axis=1)
        for o in range(NORB):
            kout[a * NORB + o, :, 0:OB] = -cols[o * MP:(o + 1) * MP]
    j = jnp.sum(jp[...], axis=1)
    for a in range(NAUX):
        kout[a * NORB + orb, :, 0:OB] += 2.0 * j[:, a * OB:(a + 1) * OB]

    def give(t):
        d = peer(t)
        return pltpu.make_async_remote_copy(kout.at[d], kin.at[t], ks_sem.at[t], kr_sem.at[t],
                                            device_id=at(d), device_id_type=MESH)

    for t in range(1, NDEV):
        give(t).start()
    total = kout[me]
    for t in range(1, NDEV):
        give(t).wait_recv()
        total = total + kin[t]
    out_ref[...] = total[0:MB, 0:OB]
    for t in range(1, NDEV):
        give(t).wait_send()


def fock(ints, ct, co, metric):
    vmem, hbm = pl.BlockSpec(memory_space=pltpu.VMEM), pl.BlockSpec(memory_space=pl.ANY)
    dma = pltpu.SemaphoreType.DMA
    return pl.pallas_call(
        kernel,
        name='fock',
        out_shape=jax.ShapeDtypeStruct((MB, OB), F32),
        in_specs=[hbm, vmem, vmem, vmem],
        out_specs=vmem,
        scratch_shapes=[
            pltpu.VMEM((NBUF * GR, QB, NB), F32),
            pltpu.VMEM((6 * GR, NORB * MP, QP), BF16),
            pltpu.VMEM((128, NB), BF16),
            pltpu.VMEM((4, NDEV * SP, 128), F32),
            pltpu.VMEM((NCH, NDEV, IV, MC, QP), BF16),
            pltpu.VMEM((NAUX, IV, NORB * NCH, MC, QP), BF16),
            pltpu.VMEM((IV, MP, QP), F32),
            pltpu.VMEM((MC, QP), F32),
            pltpu.VMEM((8, QP), F32),
            pltpu.VMEM((NDEV, 8, QP), F32),
            pltpu.VMEM((QB, QB), F32),
            pltpu.VMEM((QB, QB), F32),
            pltpu.VMEM((3, 2 * QP, 2 * QP), BF16),
            pltpu.VMEM((NORB * MP, QP), F32),
            pltpu.VMEM((QB, 128), F32),
            pltpu.VMEM((MP, 8, NB), F32),
            pltpu.VMEM((NORB * MP, NORB * MP), F32),
            pltpu.VMEM((NDEV, MP, 256), F32),
            pltpu.VMEM((NDEV, MP, 256), F32),
            dma((NBUF,)), dma((NDEV,)), dma((NDEV,)), dma((NDEV,)), dma((NDEV,)),
            dma((2,)), dma((2,)), dma((NDEV,)), dma((NDEV,)),
        ],
        compiler_params=pltpu.CompilerParams(collective_id=0, has_side_effects=True, vmem_limit_bytes=67043328),
    )(ints, ct, co, metric)


def solution(mesh):
    def local_fock(ints, metric, orbitals):
        orb = lax.axis_index('orb')
        c = orbitals[0]
        co = jnp.pad(lax.dynamic_slice_in_dim(c, orb * MB, MB, 0), ((0, MP - MB), (0, 128 - NI)))
        return fock(jnp.transpose(ints, (1, 0, 2)), c.T, co, metric)[None]

    return jax.shard_map(local_fock, mesh=mesh,
                         in_specs=(P(('sys', 'aux'), 'orb', None), P(('sys', 'aux'), None), P('sys', None, None)),
                         out_specs=P('sys', 'orb', 'aux'), check_vma=False)
```

```python
import jax
import jax.numpy as jnp
from jax import lax
from jax.experimental import pallas as pl
from jax.experimental.pallas import tpu as pltpu

P = jax.sharding.PartitionSpec
F32, BF16 = jnp.float32, jnp.bfloat16
MESH = pl.DeviceIdType.MESH
NT = (((1,), (1,)), ((), ()))
LN2 = 0.6931471805599453
TOP = 126.0
ROUND = 1.5 * 2.0 ** 15

NAUX, NORB, NDEV = 2, 4, 8
QB, MB, NB, NI = 464, 116, 464, 40
IV = NI // NDEV
QP, MP = 512, 120
MC = 8
NCH = MP // MC
TAIL = MB - MC * (NCH - 1)
SP = 48
GR = 4
NG = MB // GR
NBUF = 4
NST = (NG + 1) // 2
OB = NB // NAUX
HQ = QB // 2


def split3(x):
    a = x.astype(BF16)
    r = x - a.astype(F32)
    b = r.astype(BF16)
    c = (r - b.astype(F32)).astype(BF16)
    return a, b, c


def kernel(b_hbm, ct_ref, co_ref, m_ref, out_ref,
           bbuf, bs, cw, abuf, sbuf, arecv, own, gbuf, gsend, grecv,
           md, mx, ms, af, wb, jp, kacc, kout, kin,
           bsem, ssem, rsem, gs_sem, gr_sem, ms_sem, mr_sem, ks_sem, kr_sem):
    aux, orb = lax.axis_index('aux'), lax.axis_index('orb')
    me = aux * NORB + orb
    core = lax.rem(orb, 2)
    side = (aux, 1 - aux)

    chip = orb // 2

    STEPS = tuple((core, 1 - core, k) for k in range(2)) + tuple((1 - core, core, k) for k in range(2)) \
        + ((1, 1, 0), (1, 1, 1), (0, 0, 1))

    def peer(n):
        y, x, k = STEPS[n]
        return lax.rem(aux + y, 2), 2 * lax.rem(chip + x, 2) + lax.rem(core + k, 2)

    def name(n):
        y, x, k = STEPS[n]
        return 4 * y + 2 * x + k

    def at(n):
        a, o = peer(n)
        return {'aux': a, 'orb': o}

    def index(n):
        a, o = peer(n)
        return a * NORB + o

    def fetch(g):
        slot = g % NBUF if isinstance(g, int) else lax.rem(g, NBUF)
        return pltpu.make_async_copy(b_hbm.at[pl.ds(g * GR, GR)], bbuf.at[pl.ds(slot * GR, GR)], bsem.at[slot])

    for g in range(NBUF - 1):
        fetch(g).start()

    barrier = pltpu.get_barrier_semaphore()
    for t in range(NDEV - 1):
        pl.semaphore_signal(barrier, inc=1, device_id=at(t), device_id_type=MESH)

    for a in range(NAUX):
        @pl.when(aux == a)
        def _():
            md[...] = m_ref[:, a * QB:(a + 1) * QB]

    abuf[...] = jnp.zeros_like(abuf)
    gbuf[...] = jnp.zeros_like(gbuf)
    c1, c2, c3 = split3(ct_ref[...])
    cw[...] = jnp.concatenate(
        [c1.astype(F32), c2.astype(F32), c3.astype(F32), jnp.zeros((8, NB), F32)], axis=0).astype(BF16)

    pl.semaphore_wait(barrier, NDEV - 1)

    def mcopy(src, k, rows, dev):
        block = pl.ds(pl.multiple_of(rows * HQ, 8), HQ)
        return pltpu.make_async_remote_copy(src.at[block], mx.at[block], ms_sem.at[k], mr_sem.at[k],
                                            device_id=dev, device_id_type=MESH)
    mfirst = mcopy(md, 0, core, {'aux': 1 - aux, 'orb': orb})
    mfirst.start()

    def send(c, t):
        return pltpu.make_async_remote_copy(sbuf.at[c, index(t)], arecv.at[aux, :, orb * NCH + c],
                                            ssem.at[name(t)], rsem.at[name(t)], device_id=at(t), device_id_type=MESH)

    def cut(g, half):
        slot = lax.rem(g, NBUF)
        for k in range(GR):
            for r in range(0, QB, 16):
                parts = split3(bbuf[slot * GR + k, r:r + 16, :])
                for j in range(3):
                    bs[3 * (half * GR + k) + j, r:r + 16, 0:NB] = parts[j]

    def dots(half):
        for k in range(half * GR, (half + 1) * GR):
            r = None
            for j in range(3):
                x = lax.dot_general(cw[...], bs[3 * k + j, 0:QB, 0:NB], NT, preferred_element_type=F32)
                r = x if r is None else r + x
            a2 = r[0:NI] + r[NI:2 * NI] + r[2 * NI:3 * NI]
            for v in range(IV):
                for lt in range(4):
                    l0, l1 = lt * 128, min(lt * 128 + 128, QB)
                    abuf[lt, pl.ds(v * MC + k, NDEV, stride=SP), 0:l1 - l0] = a2[8 * v:8 * v + 8, l0:l1]

    lane = lax.broadcasted_iota(jnp.int32, (MC, QP), 1)

    def deliver(c):
        g = gbuf[...]
        for s in range(NDEV):
            for v in range(IV):
                r0 = s * SP + v * MC
                col = co_ref[pl.ds(pl.multiple_of(c * MC, MC), MC), 8 * v + s:8 * v + s + 1]
                x = jnp.concatenate([abuf[lt, r0:r0 + MC, :] for lt in range(4)], axis=1)
                g = g + x * col
                big = jnp.maximum(jnp.max(jnp.abs(x), axis=1, keepdims=True), 2.0 ** -100)
                j = jnp.ceil(jnp.log(big * (1.0 / TOP)) * (1.0 / LN2) + 0.01)
                up = jnp.exp2(j).astype(BF16).astype(F32)
                down = jnp.exp2(-j).astype(BF16).astype(F32)
                y = jnp.exp2(x * down)
                sbuf[c, s, v] = jnp.where(lane < QB, y, up).astype(BF16)
        gbuf[...] = g
        for v in range(IV):
            r0 = pl.multiple_of(me * SP + v * MC, 8)
            own[v, pl.ds(pl.multiple_of(c * MC, MC), MC), :] = jnp.concatenate(
                [abuf[lt, pl.ds(r0, MC), :] for lt in range(4)], axis=1)
        for t in range(NDEV - 1):
            send(c, t).start()

    fetch(0).wait()
    cut(jnp.int32(0), 0)

    @pl.loop(0, NCH - 1)
    def _(c):
        fetch(2 * c + 1).wait()
        fetch(2 * c + 2).wait()

        @pl.when(2 * c + 3 < NG)
        def _():
            fetch(2 * c + 3).start()

        @pl.when(2 * c + 4 < NG)
        def _():
            fetch(2 * c + 4).start()

        cut(2 * c + 1, 1)
        dots(0)
        cut(2 * c + 2, 0)
        dots(1)
        deliver(c)

    for g in range(NBUF):
        fetch(g).start()
    abuf[...] = jnp.zeros_like(abuf)
    dots(0)
    deliver(jnp.int32(NCH - 1))

    gsend[...] = jnp.broadcast_to(jnp.sum(gbuf[...], axis=0, keepdims=True), (8, QP))

    def gcopy(t):
        return pltpu.make_async_remote_copy(gsend, grecv.at[me], gs_sem.at[name(t)], gr_sem.at[name(t)],
                                            device_id=at(t), device_id_type=MESH)

    for t in range(NDEV - 1):
        gcopy(t).start()
    grecv[me] = gsend[...]

    mfirst.wait()
    msecond = mcopy(mx, 1, core, {'orb': orb + 1 - 2 * core})
    msecond.start()

    ms[...] = jnp.zeros_like(ms)

    def parts_of(x, r, s):
        parts = split3(x)
        for j in range(3):
            ms[j, r * QP:r * QP + QB, s * QP:s * QP + QB] = parts[j]

    parts_of(md[...], 0, 0)
    for a in range(NAUX):
        @pl.when(aux == a)
        def _():
            off = m_ref[:, (1 - a) * QB:(2 - a) * QB]
            af[0:QB, 0:QB] = off
    parts_of(af[0:QB, 0:QB], 0, 1)
    parts_of(af[0:QB, 0:QB].T, 1, 0)
    msecond.wait_send()
    mcopy(mx, 1, 1 - core, {'orb': orb + 1 - 2 * core}).wait_recv()
    parts_of(mx[...], 1, 1)
    kacc[...] = jnp.zeros_like(kacc)

    for t in range(NDEV - 1):
        pltpu.make_async_remote_copy(gsend, grecv.at[index(t)], gs_sem.at[name(t)], gr_sem.at[name(t)],
                                     device_id=at(t), device_id_type=MESH).wait()
    off = af[0:QB, 0:QB]
    gam = [sum(grecv[side[r] * NORB + o][0:1, 0:QB] for o in range(NORB)) for r in range(2)]
    fit0 = jnp.sum(md[...] * gam[0], axis=1, keepdims=True) + jnp.sum(off * gam[1], axis=1, keepdims=True)
    turn = jnp.broadcast_to(gam[0], (128, QB)).T
    fit1 = (jnp.sum(off * turn[:, 0:1], axis=0, keepdims=True)
            + jnp.sum(mx[...] * jnp.broadcast_to(gam[1], (128, QB)).T[:, 0:1], axis=0, keepdims=True))
    wcol = jnp.sum(off * fit1, axis=1, keepdims=True)
    wrow = jnp.sum(md[...] * fit0, axis=0, keepdims=True)
    wb[...] = jnp.broadcast_to(wrow, (128, QB)).T + wcol

    def coulomb(s, base):
        for x in range(2):
            @pl.when(2 * s + x < NG)
            def _():
                fetch(2 * s + x).wait()
        @pl.loop(0, 2 * GR)
        def _(x):
            for l0, l1 in ((0, 128), (128, 256), (256, 384), (384, NB)):
                y = bbuf[base * GR + x, :, l0:l1] * wb[:, 0:l1 - l0]
                jp[2 * GR * s + x, :, l0:l1] = jnp.sum(y.reshape(QB // 8, 8, l1 - l0), axis=0)

        for x in range(2):
            @pl.when(2 * s + NBUF + x < NG)
            def _():
                fetch(2 * s + NBUF + x).start()

    EARLY = NST - 2 * IV

    @pl.loop(0, EARLY)
    def _(s):
        coulomb(s, 2 * lax.rem(s, 2))

    for t in range(NDEV - 1):
        a, o = peer(t)
        whole = arecv.at[a, :, pl.ds(o * NCH, NCH)]
        arrived = pltpu.make_async_remote_copy(whole, whole, ssem.at[name(t)], rsem.at[name(t)],
                                               device_id=at(t), device_id_type=MESH)
        arrived.wait_send()
        arrived.wait_recv()

    PAIRS = ((0, 0), (0, 1), (1, 0), (1, 1), (0, 2), (2, 0))

    @pl.loop(0, IV)
    def _(v):
        def decode(sd, r):
            y = arecv[side[sd], v, r // MC:r // MC + 2].astype(F32).reshape(2 * MC, QP)
            u = jnp.log(y) * (1.0 / LN2)
            return ((u + ROUND) - ROUND) * y[:, QB:QB + 1]

        for r in range(0, NORB * MP, 16):
            af[r:r + 16, :] = decode(0, r)
        af[pl.ds(pl.multiple_of(orb * MP, 8), MP), :] = own[v]
        for r in range(0, NORB * MP, 16):
            for j, x in enumerate(split3(af[r:r + 16, :])):
                bs[j, r:r + 16, :] = x
            for j, x in enumerate(split3(decode(1, r))[:2]):
                bs[3 + j, r:r + 16, :] = x
        t = None
        for sd in range(2):
            for i, j in PAIRS[:6 - sd]:
                x = jnp.dot(bs[3 * sd + i], ms[j, sd * QP:(sd + 1) * QP, :], preferred_element_type=F32)
                t = x if t is None else t + x
        for j, x in enumerate(split3(t)):
            bs[5 + j], bs[8 + j] = x[:, 0:QP], x[:, QP:2 * QP]
        coulomb(EARLY + 2 * v, 2 * (EARLY % 2))
        half = jnp.asarray(0.5, BF16)
        s1 = None
        for b in (5, 8):
            t1, t2, t3 = bs[b], bs[b + 1], bs[b + 2]
            for x, y in ((t1, t1 * half), (t1, t2), (t1, t3), (t2, t2 * half)):
                z = lax.dot_general(x, y, NT, preferred_element_type=F32)
                s1 = z if s1 is None else s1 + z
        kacc[...] += s1
        coulomb(EARLY + 2 * v + 1, 2 - 2 * (EARLY % 2))

    k = kacc[...]
    k = k + k.T
    for a in range(NAUX):
        cols = jnp.concatenate([k[:, o * MP:o * MP + MB] for o in (2 * a, 2 * a + 1)], axis=1)
        for o in range(NORB):
            kout[a * NORB + o, :, 0:OB] = -cols[o * MP:(o + 1) * MP]
    j = jnp.sum(jp[...], axis=1)
    for a in range(NAUX):
        kout[a * NORB + orb, :, 0:OB] += 2.0 * j[:, a * OB:(a + 1) * OB]

    def give(t):
        return pltpu.make_async_remote_copy(kout.at[index(t)], kin.at[name(t)], ks_sem.at[name(t)], kr_sem.at[name(t)],
                                            device_id=at(t), device_id_type=MESH)

    for t in range(NDEV - 1):
        give(t).start()
    total = kout[me]
    for t in range(NDEV - 1):
        give(t).wait_recv()
        total = total + kin[name(t)]
    out_ref[...] = total[0:MB, 0:OB]
    for t in range(NDEV - 1):
        give(t).wait_send()


def fock(ints, ct, co, metric):
    vmem, hbm = pl.BlockSpec(memory_space=pltpu.VMEM), pl.BlockSpec(memory_space=pl.ANY)
    dma = pltpu.SemaphoreType.DMA
    return pl.pallas_call(
        kernel,
        name='fock',
        out_shape=jax.ShapeDtypeStruct((MB, OB), F32),
        in_specs=[hbm, vmem, vmem, vmem],
        out_specs=vmem,
        scratch_shapes=[
            pltpu.VMEM((NBUF * GR, QB, NB), F32),
            pltpu.VMEM((6 * GR, NORB * MP, QP), BF16),
            pltpu.VMEM((128, NB), BF16),
            pltpu.VMEM((4, NDEV * SP, 128), F32),
            pltpu.VMEM((NCH, NDEV, IV, MC, QP), BF16),
            pltpu.VMEM((NAUX, IV, NORB * NCH, MC, QP), BF16),
            pltpu.VMEM((IV, MP, QP), F32),
            pltpu.VMEM((MC, QP), F32),
            pltpu.VMEM((8, QP), F32),
            pltpu.VMEM((NDEV, 8, QP), F32),
            pltpu.VMEM((QB, QB), F32),
            pltpu.VMEM((QB, QB), F32),
            pltpu.VMEM((3, 2 * QP, 2 * QP), BF16),
            pltpu.VMEM((NORB * MP, QP), F32),
            pltpu.VMEM((QB, 128), F32),
            pltpu.VMEM((MP, 8, NB), F32),
            pltpu.VMEM((NORB * MP, NORB * MP), F32),
            pltpu.VMEM((NDEV, MP, 256), F32),
            pltpu.VMEM((NDEV, MP, 256), F32),
            dma((NBUF,)), dma((NDEV,)), dma((NDEV,)), dma((NDEV,)), dma((NDEV,)),
            dma((2,)), dma((2,)), dma((NDEV,)), dma((NDEV,)),
        ],
        compiler_params=pltpu.CompilerParams(collective_id=0, has_side_effects=True, vmem_limit_bytes=67043328),
    )(ints, ct, co, metric)


def solution(mesh):
    def local_fock(ints, metric, orbitals):
        orb = lax.axis_index('orb')
        c = orbitals[0]
        co = jnp.pad(lax.dynamic_slice_in_dim(c, orb * MB, MB, 0), ((0, MP - MB), (0, 128 - NI)))
        return fock(jnp.transpose(ints, (1, 0, 2)), c.T, co, metric)[None]

    return jax.shard_map(local_fock, mesh=mesh,
                         in_specs=(P(('sys', 'aux'), 'orb', None), P(('sys', 'aux'), None), P('sys', None, None)),
                         out_specs=P('sys', 'orb', 'aux'), check_vma=False)
```

```python
import jax
import jax.numpy as jnp
from jax import lax
from jax.experimental import pallas as pl
from jax.experimental.pallas import tpu as pltpu

P = jax.sharding.PartitionSpec
F32, BF16 = jnp.float32, jnp.bfloat16
MESH = pl.DeviceIdType.MESH
NT = (((1,), (1,)), ((), ()))
LN2 = 0.6931471805599453
TOP = 126.0
ROUND = 1.5 * 2.0 ** 15

NAUX, NORB, NDEV = 2, 4, 8
QB, MB, NB, NI = 464, 116, 464, 40
IV = NI // NDEV
QP, MP = 512, 120
MC = 8
NCH = MP // MC
TAIL = MB - MC * (NCH - 1)
SP = 48
GR = 4
NG = MB // GR
NBUF = 4
GROUPS = (2, 2, 3, 3, 3, 2)
NST = (NG + 1) // 2
OB = NB // NAUX
HQ = QB // 2


def split3(x):
    a = x.astype(BF16)
    r = x - a.astype(F32)
    b = r.astype(BF16)
    c = (r - b.astype(F32)).astype(BF16)
    return a, b, c


def kernel(b_hbm, ct_ref, co_ref, m_ref, out_ref,
           bbuf, bs, cw, abuf, sbuf, arecv, own, gbuf, gsend, grecv,
           md, mx, ms, af, wb, jp, kacc, kout, kin,
           bsem, ssem, rsem, gs_sem, gr_sem, ms_sem, mr_sem, ks_sem, kr_sem):
    aux, orb = lax.axis_index('aux'), lax.axis_index('orb')
    me = aux * NORB + orb
    core = lax.rem(orb, 2)
    side = (aux, 1 - aux)

    chip = orb // 2

    STEPS = tuple((core, 1 - core, k) for k in range(2)) + tuple((1 - core, core, k) for k in range(2)) \
        + ((1, 1, 0), (1, 1, 1), (0, 0, 1))

    def peer(n):
        y, x, k = STEPS[n]
        return lax.rem(aux + y, 2), 2 * lax.rem(chip + x, 2) + lax.rem(core + k, 2)

    def name(n):
        y, x, k = STEPS[n]
        return 4 * y + 2 * x + k

    def at(n):
        a, o = peer(n)
        return {'aux': a, 'orb': o}

    def index(n):
        a, o = peer(n)
        return a * NORB + o

    def fetch(g):
        slot = g % NBUF if isinstance(g, int) else lax.rem(g, NBUF)
        return pltpu.make_async_copy(b_hbm.at[pl.ds(g * GR, GR)], bbuf.at[pl.ds(slot * GR, GR)], bsem.at[slot])

    for g in range(NBUF - 1):
        fetch(g).start()

    barrier = pltpu.get_barrier_semaphore()
    for t in range(NDEV - 1):
        pl.semaphore_signal(barrier, inc=1, device_id=at(t), device_id_type=MESH)

    for a in range(NAUX):
        @pl.when(aux == a)
        def _():
            md[...] = m_ref[:, a * QB:(a + 1) * QB]

    abuf[...] = jnp.zeros_like(abuf)
    gbuf[...] = jnp.zeros_like(gbuf)
    c1, c2, c3 = split3(ct_ref[...])
    cw[...] = jnp.concatenate(
        [c1.astype(F32), c2.astype(F32), c3.astype(F32), jnp.zeros((8, NB), F32)], axis=0).astype(BF16)

    pl.semaphore_wait(barrier, NDEV - 1)

    def mcopy(src, k, rows, dev):
        block = pl.ds(pl.multiple_of(rows * HQ, 8), HQ)
        return pltpu.make_async_remote_copy(src.at[block], mx.at[block], ms_sem.at[k], mr_sem.at[k],
                                            device_id=dev, device_id_type=MESH)
    mfirst = mcopy(md, 0, core, {'aux': 1 - aux, 'orb': orb})
    mfirst.start()

    def send(c, n, t):
        return pltpu.make_async_remote_copy(sbuf.at[index(t), :, c:c + n], arecv.at[aux, :, pl.ds(orb * NCH + c, n)],
                                            ssem.at[name(t)], rsem.at[name(t)], device_id=at(t), device_id_type=MESH)

    def cut(g, half):
        slot = lax.rem(g, NBUF)
        for k in range(GR):
            for r in range(0, QB, 16):
                parts = split3(bbuf[slot * GR + k, r:r + 16, :])
                for j in range(3):
                    bs[3 * (half * GR + k) + j, r:r + 16, 0:NB] = parts[j]

    def dots(half):
        for k in range(half * GR, (half + 1) * GR):
            r = None
            for j in range(3):
                x = lax.dot_general(cw[...], bs[3 * k + j, 0:QB, 0:NB], NT, preferred_element_type=F32)
                r = x if r is None else r + x
            a2 = r[0:NI] + r[NI:2 * NI] + r[2 * NI:3 * NI]
            for v in range(IV):
                for lt in range(4):
                    l0, l1 = lt * 128, min(lt * 128 + 128, QB)
                    abuf[lt, pl.ds(v * MC + k, NDEV, stride=SP), 0:l1 - l0] = a2[8 * v:8 * v + 8, l0:l1]

    lane = lax.broadcasted_iota(jnp.int32, (MC, QP), 1)

    def deliver(c):
        g = gbuf[...]
        for s in range(NDEV):
            for v in range(IV):
                r0 = s * SP + v * MC
                col = co_ref[pl.ds(pl.multiple_of(c * MC, MC), MC), 8 * v + s:8 * v + s + 1]
                x = jnp.concatenate([abuf[lt, r0:r0 + MC, :] for lt in range(4)], axis=1)
                g = g + x * col
                big = jnp.maximum(jnp.max(jnp.abs(x), axis=1, keepdims=True), 2.0 ** -100)
                j = jnp.ceil(jnp.log(big * (1.0 / TOP)) * (1.0 / LN2) + 0.01)
                up = jnp.exp2(j).astype(BF16).astype(F32)
                down = jnp.exp2(-j).astype(BF16).astype(F32)
                y = jnp.exp2(x * down)
                sbuf[s, v, c] = jnp.where(lane < QB, y, up).astype(BF16)
        gbuf[...] = g
        for v in range(IV):
            r0 = pl.multiple_of(me * SP + v * MC, 8)
            own[v, pl.ds(pl.multiple_of(c * MC, MC), MC), :] = jnp.concatenate(
                [abuf[lt, pl.ds(r0, MC), :] for lt in range(4)], axis=1)
        for e in range(len(GROUPS)):
            @pl.when(c == sum(GROUPS[:e + 1]) - 1)
            def _():
                for t in range(NDEV - 1):
                    send(sum(GROUPS[:e]), GROUPS[e], t).start()

    fetch(0).wait()
    cut(jnp.int32(0), 0)

    @pl.loop(0, NCH - 1)
    def _(c):
        fetch(2 * c + 1).wait()
        fetch(2 * c + 2).wait()

        @pl.when(2 * c + 3 < NG)
        def _():
            fetch(2 * c + 3).start()

        @pl.when(2 * c + 4 < NG)
        def _():
            fetch(2 * c + 4).start()

        cut(2 * c + 1, 1)
        dots(0)
        cut(2 * c + 2, 0)
        dots(1)
        deliver(c)

    for g in range(NBUF):
        fetch(g).start()
    abuf[...] = jnp.zeros_like(abuf)
    dots(0)
    deliver(jnp.int32(NCH - 1))

    gsend[...] = jnp.broadcast_to(jnp.sum(gbuf[...], axis=0, keepdims=True), (8, QP))

    def gcopy(t):
        return pltpu.make_async_remote_copy(gsend, grecv.at[me], gs_sem.at[name(t)], gr_sem.at[name(t)],
                                            device_id=at(t), device_id_type=MESH)

    for t in range(NDEV - 1):
        gcopy(t).start()
    grecv[me] = gsend[...]

    mfirst.wait()
    msecond = mcopy(mx, 1, core, {'orb': orb + 1 - 2 * core})
    msecond.start()

    ms[...] = jnp.zeros_like(ms)

    def parts_of(x, r, s):
        parts = split3(x)
        for j in range(3):
            ms[j, r * QP:r * QP + QB, s * QP:s * QP + QB] = parts[j]

    parts_of(md[...], 0, 0)
    for a in range(NAUX):
        @pl.when(aux == a)
        def _():
            off = m_ref[:, (1 - a) * QB:(2 - a) * QB]
            af[0:QB, 0:QB] = off
    parts_of(af[0:QB, 0:QB], 0, 1)
    parts_of(af[0:QB, 0:QB].T, 1, 0)
    msecond.wait_send()
    mcopy(mx, 1, 1 - core, {'orb': orb + 1 - 2 * core}).wait_recv()
    parts_of(mx[...], 1, 1)
    kacc[...] = jnp.zeros_like(kacc)

    for t in range(NDEV - 1):
        pltpu.make_async_remote_copy(gsend, grecv.at[index(t)], gs_sem.at[name(t)], gr_sem.at[name(t)],
                                     device_id=at(t), device_id_type=MESH).wait()
    off = af[0:QB, 0:QB]
    gam = [sum(grecv[side[r] * NORB + o][0:1, 0:QB] for o in range(NORB)) for r in range(2)]
    fit0 = jnp.sum(md[...] * gam[0], axis=1, keepdims=True) + jnp.sum(off * gam[1], axis=1, keepdims=True)
    turn = jnp.broadcast_to(gam[0], (128, QB)).T
    fit1 = (jnp.sum(off * turn[:, 0:1], axis=0, keepdims=True)
            + jnp.sum(mx[...] * jnp.broadcast_to(gam[1], (128, QB)).T[:, 0:1], axis=0, keepdims=True))
    wcol = jnp.sum(off * fit1, axis=1, keepdims=True)
    wrow = jnp.sum(md[...] * fit0, axis=0, keepdims=True)
    wb[...] = jnp.broadcast_to(wrow, (128, QB)).T + wcol

    def coulomb(s, base):
        for x in range(2):
            @pl.when(2 * s + x < NG)
            def _():
                fetch(2 * s + x).wait()
        @pl.loop(0, 2 * GR)
        def _(x):
            for l0, l1 in ((0, 128), (128, 256), (256, 384), (384, NB)):
                y = bbuf[base * GR + x, :, l0:l1] * wb[:, 0:l1 - l0]
                jp[2 * GR * s + x, :, l0:l1] = jnp.sum(y.reshape(QB // 8, 8, l1 - l0), axis=0)

        for x in range(2):
            @pl.when(2 * s + NBUF + x < NG)
            def _():
                fetch(2 * s + NBUF + x).start()

    EARLY = NST - 2 * IV

    @pl.loop(0, EARLY)
    def _(s):
        coulomb(s, 2 * lax.rem(s, 2))

    for t in range(NDEV - 1):
        a, o = peer(t)
        whole = arecv.at[a, :, pl.ds(o * NCH, NCH)]
        arrived = pltpu.make_async_remote_copy(whole, whole, ssem.at[name(t)], rsem.at[name(t)],
                                               device_id=at(t), device_id_type=MESH)
        arrived.wait_send()
        arrived.wait_recv()

    PAIRS = ((0, 0), (0, 1), (1, 0), (1, 1), (0, 2), (2, 0))

    @pl.loop(0, IV)
    def _(v):
        def decode(sd, r):
            y = arecv[side[sd], v, r // MC:r // MC + 2].astype(F32).reshape(2 * MC, QP)
            u = jnp.log(y) * (1.0 / LN2)
            return ((u + ROUND) - ROUND) * y[:, QB:QB + 1]

        for r in range(0, NORB * MP, 16):
            af[r:r + 16, :] = decode(0, r)
        af[pl.ds(pl.multiple_of(orb * MP, 8), MP), :] = own[v]
        for r in range(0, NORB * MP, 16):
            for j, x in enumerate(split3(af[r:r + 16, :])):
                bs[j, r:r + 16, :] = x
            for j, x in enumerate(split3(decode(1, r))[:2]):
                bs[3 + j, r:r + 16, :] = x
        t = None
        for sd in range(2):
            for i, j in PAIRS[:6 - sd]:
                x = jnp.dot(bs[3 * sd + i], ms[j, sd * QP:(sd + 1) * QP, :], preferred_element_type=F32)
                t = x if t is None else t + x
        for j, x in enumerate(split3(t)):
            bs[5 + j], bs[8 + j] = x[:, 0:QP], x[:, QP:2 * QP]
        coulomb(EARLY + 2 * v, 2 * (EARLY % 2))
        half = jnp.asarray(0.5, BF16)
        s1 = None
        for b in (5, 8):
            t1, t2, t3 = bs[b], bs[b + 1], bs[b + 2]
            for x, y in ((t1, t1 * half), (t1, t2), (t1, t3), (t2, t2 * half)):
                z = lax.dot_general(x, y, NT, preferred_element_type=F32)
                s1 = z if s1 is None else s1 + z
        kacc[...] += s1
        coulomb(EARLY + 2 * v + 1, 2 - 2 * (EARLY % 2))

    k = kacc[...]
    k = k + k.T
    for a in range(NAUX):
        cols = jnp.concatenate([k[:, o * MP:o * MP + MB] for o in (2 * a, 2 * a + 1)], axis=1)
        for o in range(NORB):
            kout[a * NORB + o, :, 0:OB] = -cols[o * MP:(o + 1) * MP]
    j = jnp.sum(jp[...], axis=1)
    for a in range(NAUX):
        kout[a * NORB + orb, :, 0:OB] += 2.0 * j[:, a * OB:(a + 1) * OB]

    def give(t):
        return pltpu.make_async_remote_copy(kout.at[index(t)], kin.at[name(t)], ks_sem.at[name(t)], kr_sem.at[name(t)],
                                            device_id=at(t), device_id_type=MESH)

    for t in range(NDEV - 1):
        give(t).start()
    total = kout[me]
    for t in range(NDEV - 1):
        give(t).wait_recv()
        total = total + kin[name(t)]
    out_ref[...] = total[0:MB, 0:OB]
    for t in range(NDEV - 1):
        give(t).wait_send()


def fock(ints, ct, co, metric):
    vmem, hbm = pl.BlockSpec(memory_space=pltpu.VMEM), pl.BlockSpec(memory_space=pl.ANY)
    dma = pltpu.SemaphoreType.DMA
    return pl.pallas_call(
        kernel,
        name='fock',
        out_shape=jax.ShapeDtypeStruct((MB, OB), F32),
        in_specs=[hbm, vmem, vmem, vmem],
        out_specs=vmem,
        scratch_shapes=[
            pltpu.VMEM((NBUF * GR, QB, NB), F32),
            pltpu.VMEM((6 * GR, NORB * MP, QP), BF16),
            pltpu.VMEM((128, NB), BF16),
            pltpu.VMEM((4, NDEV * SP, 128), F32),
            pltpu.VMEM((NDEV, IV, NCH, MC, QP), BF16),
            pltpu.VMEM((NAUX, IV, NORB * NCH, MC, QP), BF16),
            pltpu.VMEM((IV, MP, QP), F32),
            pltpu.VMEM((MC, QP), F32),
            pltpu.VMEM((8, QP), F32),
            pltpu.VMEM((NDEV, 8, QP), F32),
            pltpu.VMEM((QB, QB), F32),
            pltpu.VMEM((QB, QB), F32),
            pltpu.VMEM((3, 2 * QP, 2 * QP), BF16),
            pltpu.VMEM((NORB * MP, QP), F32),
            pltpu.VMEM((QB, 128), F32),
            pltpu.VMEM((MP, 8, NB), F32),
            pltpu.VMEM((NORB * MP, NORB * MP), F32),
            pltpu.VMEM((NDEV, MP, 256), F32),
            pltpu.VMEM((NDEV, MP, 256), F32),
            dma((NBUF,)), dma((NDEV,)), dma((NDEV,)), dma((NDEV,)), dma((NDEV,)),
            dma((2,)), dma((2,)), dma((NDEV,)), dma((NDEV,)),
        ],
        compiler_params=pltpu.CompilerParams(collective_id=0, has_side_effects=True, vmem_limit_bytes=67043328),
    )(ints, ct, co, metric)


def solution(mesh):
    def local_fock(ints, metric, orbitals):
        orb = lax.axis_index('orb')
        c = orbitals[0]
        co = jnp.pad(lax.dynamic_slice_in_dim(c, orb * MB, MB, 0), ((0, MP - MB), (0, 128 - NI)))
        return fock(jnp.transpose(ints, (1, 0, 2)), c.T, co, metric)[None]

    return jax.shard_map(local_fock, mesh=mesh,
                         in_specs=(P(('sys', 'aux'), 'orb', None), P(('sys', 'aux'), None), P('sys', None, None)),
                         out_specs=P('sys', 'orb', 'aux'), check_vma=False)
```

```python
import jax
import jax.numpy as jnp
from jax import lax
from jax.experimental import pallas as pl
from jax.experimental.pallas import tpu as pltpu

P = jax.sharding.PartitionSpec
F32, BF16 = jnp.float32, jnp.bfloat16
MESH = pl.DeviceIdType.MESH
NT = (((1,), (1,)), ((), ()))
LN2 = 0.6931471805599453
TOP = 126.0
ROUND = 1.5 * 2.0 ** 15

NAUX, NORB, NDEV = 2, 4, 8
QB, MB, NB, NI = 464, 116, 464, 40
IV = NI // NDEV
QP, MP = 512, 120
MC = 8
NCH = MP // MC
TAIL = MB - MC * (NCH - 1)
SP = 48
GR = 4
NG = MB // GR
NBUF = 4
MTURN = 6
NST = (NG + 1) // 2
OB = NB // NAUX
HQ = QB // 2


def split3(x):
    a = x.astype(BF16)
    r = x - a.astype(F32)
    b = r.astype(BF16)
    c = (r - b.astype(F32)).astype(BF16)
    return a, b, c


def kernel(b_hbm, ct_ref, co_ref, m_ref, out_ref,
           bbuf, bs, cw, abuf, sbuf, arecv, own, gbuf, gsend, grecv,
           md, mx, ms, af, wb, jp, kacc, kout, kin,
           bsem, ssem, rsem, gs_sem, gr_sem, ms_sem, mr_sem, ks_sem, kr_sem):
    aux, orb = lax.axis_index('aux'), lax.axis_index('orb')
    me = aux * NORB + orb
    core = lax.rem(orb, 2)
    side = (aux, 1 - aux)

    chip = orb // 2

    STEPS = tuple((core, 1 - core, k) for k in range(2)) + tuple((1 - core, core, k) for k in range(2)) \
        + ((1, 1, 0), (1, 1, 1), (0, 0, 1))

    def peer(n):
        y, x, k = STEPS[n]
        return lax.rem(aux + y, 2), 2 * lax.rem(chip + x, 2) + lax.rem(core + k, 2)

    def name(n):
        y, x, k = STEPS[n]
        return 4 * y + 2 * x + k

    def at(n):
        a, o = peer(n)
        return {'aux': a, 'orb': o}

    def index(n):
        a, o = peer(n)
        return a * NORB + o

    def fetch(g):
        slot = g % NBUF if isinstance(g, int) else lax.rem(g, NBUF)
        return pltpu.make_async_copy(b_hbm.at[pl.ds(g * GR, GR)], bbuf.at[pl.ds(slot * GR, GR)], bsem.at[slot])

    for g in range(NBUF - 1):
        fetch(g).start()

    barrier = pltpu.get_barrier_semaphore()
    for t in range(NDEV - 1):
        pl.semaphore_signal(barrier, inc=1, device_id=at(t), device_id_type=MESH)

    for a in range(NAUX):
        @pl.when(aux == a)
        def _():
            md[...] = m_ref[:, a * QB:(a + 1) * QB]

    abuf[...] = jnp.zeros_like(abuf)
    gbuf[...] = jnp.zeros_like(gbuf)
    c1, c2, c3 = split3(ct_ref[...])
    cw[...] = jnp.concatenate(
        [c1.astype(F32), c2.astype(F32), c3.astype(F32), jnp.zeros((8, NB), F32)], axis=0).astype(BF16)

    pl.semaphore_wait(barrier, NDEV - 1)

    def mcopy(src, k, rows, dev):
        block = pl.ds(pl.multiple_of(rows * HQ, 8), HQ)
        return pltpu.make_async_remote_copy(src.at[block], mx.at[block], ms_sem.at[k], mr_sem.at[k],
                                            device_id=dev, device_id_type=MESH)
    mfirst = mcopy(md, 0, core, {'aux': 1 - aux, 'orb': orb})
    mfirst.start()

    def send(c, t):
        return pltpu.make_async_remote_copy(sbuf.at[c, index(t)], arecv.at[aux, :, orb * NCH + c],
                                            ssem.at[name(t)], rsem.at[name(t)], device_id=at(t), device_id_type=MESH)

    def cut(g, half):
        slot = lax.rem(g, NBUF)
        for k in range(GR):
            for r in range(0, QB, 16):
                parts = split3(bbuf[slot * GR + k, r:r + 16, :])
                for j in range(3):
                    bs[3 * (half * GR + k) + j, r:r + 16, 0:NB] = parts[j]

    def dots(half):
        for k in range(half * GR, (half + 1) * GR):
            r = None
            for j in range(3):
                x = lax.dot_general(cw[...], bs[3 * k + j, 0:QB, 0:NB], NT, preferred_element_type=F32)
                r = x if r is None else r + x
            a2 = r[0:NI] + r[NI:2 * NI] + r[2 * NI:3 * NI]
            for v in range(IV):
                for lt in range(4):
                    l0, l1 = lt * 128, min(lt * 128 + 128, QB)
                    abuf[lt, pl.ds(v * MC + k, NDEV, stride=SP), 0:l1 - l0] = a2[8 * v:8 * v + 8, l0:l1]

    lane = lax.broadcasted_iota(jnp.int32, (MC, QP), 1)

    def deliver(c):
        g = gbuf[...]
        for s in range(NDEV):
            for v in range(IV):
                r0 = s * SP + v * MC
                col = co_ref[pl.ds(pl.multiple_of(c * MC, MC), MC), 8 * v + s:8 * v + s + 1]
                x = jnp.concatenate([abuf[lt, r0:r0 + MC, :] for lt in range(4)], axis=1)
                g = g + x * col
                big = jnp.maximum(jnp.max(jnp.abs(x), axis=1, keepdims=True), 2.0 ** -100)
                j = jnp.ceil(jnp.log(big * (1.0 / TOP)) * (1.0 / LN2) + 0.01)
                up = jnp.exp2(j).astype(BF16).astype(F32)
                down = jnp.exp2(-j).astype(BF16).astype(F32)
                y = jnp.exp2(x * down)
                sbuf[c, s, v] = jnp.where(lane < QB, y, up).astype(BF16)
        gbuf[...] = g
        for v in range(IV):
            r0 = pl.multiple_of(me * SP + v * MC, 8)
            own[v, pl.ds(pl.multiple_of(c * MC, MC), MC), :] = jnp.concatenate(
                [abuf[lt, pl.ds(r0, MC), :] for lt in range(4)], axis=1)
        for t in range(NDEV - 1):
            send(c, t).start()

    fetch(0).wait()
    cut(jnp.int32(0), 0)

    msecond = mcopy(mx, 1, core, {'orb': orb + 1 - 2 * core})

    @pl.loop(0, NCH - 1)
    def _(c):
        @pl.when(c == MTURN)
        def _():
            mfirst.wait()
            msecond.start()

        fetch(2 * c + 1).wait()
        fetch(2 * c + 2).wait()

        @pl.when(2 * c + 3 < NG)
        def _():
            fetch(2 * c + 3).start()

        @pl.when(2 * c + 4 < NG)
        def _():
            fetch(2 * c + 4).start()

        cut(2 * c + 1, 1)
        dots(0)
        cut(2 * c + 2, 0)
        dots(1)
        deliver(c)

    for g in range(NBUF):
        fetch(g).start()
    abuf[...] = jnp.zeros_like(abuf)
    dots(0)
    deliver(jnp.int32(NCH - 1))

    gsend[...] = jnp.broadcast_to(jnp.sum(gbuf[...], axis=0, keepdims=True), (8, QP))

    def gcopy(t):
        return pltpu.make_async_remote_copy(gsend, grecv.at[me], gs_sem.at[name(t)], gr_sem.at[name(t)],
                                            device_id=at(t), device_id_type=MESH)

    for t in range(NDEV - 1):
        gcopy(t).start()
    grecv[me] = gsend[...]

    ms[...] = jnp.zeros_like(ms)

    def parts_of(x, r, s):
        parts = split3(x)
        for j in range(3):
            ms[j, r * QP:r * QP + QB, s * QP:s * QP + QB] = parts[j]

    parts_of(md[...], 0, 0)
    for a in range(NAUX):
        @pl.when(aux == a)
        def _():
            off = m_ref[:, (1 - a) * QB:(2 - a) * QB]
            af[0:QB, 0:QB] = off
    parts_of(af[0:QB, 0:QB], 0, 1)
    parts_of(af[0:QB, 0:QB].T, 1, 0)
    msecond.wait_send()
    mcopy(mx, 1, 1 - core, {'orb': orb + 1 - 2 * core}).wait_recv()
    parts_of(mx[...], 1, 1)
    kacc[...] = jnp.zeros_like(kacc)

    def coulomb(s, base):
        for x in range(2):
            @pl.when(2 * s + x < NG)
            def _():
                fetch(2 * s + x).wait()
        @pl.loop(0, 2 * GR)
        def _(x):
            for l0, l1 in ((0, 128), (128, 256), (256, 384), (384, NB)):
                y = bbuf[base * GR + x, :, l0:l1] * wb[:, 0:l1 - l0]
                jp[2 * GR * s + x, :, l0:l1] = jnp.sum(y.reshape(QB // 8, 8, l1 - l0), axis=0)

        for x in range(2):
            @pl.when(2 * s + NBUF + x < NG)
            def _():
                fetch(2 * s + NBUF + x).start()

    for t in range(NDEV - 1):
        a, o = peer(t)
        whole = arecv.at[a, :, pl.ds(o * NCH, NCH)]
        arrived = pltpu.make_async_remote_copy(whole, whole, ssem.at[name(t)], rsem.at[name(t)],
                                               device_id=at(t), device_id_type=MESH)
        arrived.wait_send()
        arrived.wait_recv()

    for t in range(NDEV - 1):
        pltpu.make_async_remote_copy(gsend, grecv.at[index(t)], gs_sem.at[name(t)], gr_sem.at[name(t)],
                                     device_id=at(t), device_id_type=MESH).wait()
    off = af[0:QB, 0:QB]
    gam = [sum(grecv[side[r] * NORB + o][0:1, 0:QB] for o in range(NORB)) for r in range(2)]
    fit0 = jnp.sum(md[...] * gam[0], axis=1, keepdims=True) + jnp.sum(off * gam[1], axis=1, keepdims=True)
    turn = jnp.broadcast_to(gam[0], (128, QB)).T
    fit1 = (jnp.sum(off * turn[:, 0:1], axis=0, keepdims=True)
            + jnp.sum(mx[...] * jnp.broadcast_to(gam[1], (128, QB)).T[:, 0:1], axis=0, keepdims=True))
    wcol = jnp.sum(off * fit1, axis=1, keepdims=True)
    wrow = jnp.sum(md[...] * fit0, axis=0, keepdims=True)
    wb[...] = jnp.broadcast_to(wrow, (128, QB)).T + wcol

    PAIRS = ((0, 0), (0, 1), (1, 0), (1, 1), (0, 2), (2, 0))

    @pl.loop(0, IV)
    def _(v):
        def decode(sd, r):
            y = arecv[side[sd], v, r // MC:r // MC + 2].astype(F32).reshape(2 * MC, QP)
            u = jnp.log(y) * (1.0 / LN2)
            return ((u + ROUND) - ROUND) * y[:, QB:QB + 1]

        for r in range(0, NORB * MP, 16):
            af[r:r + 16, :] = decode(0, r)
        af[pl.ds(pl.multiple_of(orb * MP, 8), MP), :] = own[v]
        for r in range(0, NORB * MP, 16):
            for j, x in enumerate(split3(af[r:r + 16, :])):
                bs[j, r:r + 16, :] = x
            for j, x in enumerate(split3(decode(1, r))[:2]):
                bs[3 + j, r:r + 16, :] = x
        t = None
        for sd in range(2):
            for i, j in PAIRS[:6 - sd]:
                x = jnp.dot(bs[3 * sd + i], ms[j, sd * QP:(sd + 1) * QP, :], preferred_element_type=F32)
                t = x if t is None else t + x
        for j, x in enumerate(split3(t)):
            bs[5 + j], bs[8 + j] = x[:, 0:QP], x[:, QP:2 * QP]
        coulomb(3 * v, 2 * lax.rem(v, 2))
        half = jnp.asarray(0.5, BF16)
        s1 = None
        for b in (5, 8):
            t1, t2, t3 = bs[b], bs[b + 1], bs[b + 2]
            for x, y in ((t1, t1 * half), (t1, t2), (t1, t3), (t2, t2 * half)):
                z = lax.dot_general(x, y, NT, preferred_element_type=F32)
                s1 = z if s1 is None else s1 + z
        kacc[...] += s1
        coulomb(3 * v + 1, 2 - 2 * lax.rem(v, 2))
        coulomb(3 * v + 2, 2 * lax.rem(v, 2))

    k = kacc[...]
    k = k + k.T
    for a in range(NAUX):
        cols = jnp.concatenate([k[:, o * MP:o * MP + MB] for o in (2 * a, 2 * a + 1)], axis=1)
        for o in range(NORB):
            kout[a * NORB + o, :, 0:OB] = -cols[o * MP:(o + 1) * MP]
    j = jnp.sum(jp[...], axis=1)
    for a in range(NAUX):
        kout[a * NORB + orb, :, 0:OB] += 2.0 * j[:, a * OB:(a + 1) * OB]

    def give(t):
        return pltpu.make_async_remote_copy(kout.at[index(t)], kin.at[name(t)], ks_sem.at[name(t)], kr_sem.at[name(t)],
                                            device_id=at(t), device_id_type=MESH)

    for t in range(NDEV - 1):
        give(t).start()
    total = kout[me]
    for t in range(NDEV - 1):
        give(t).wait_recv()
        total = total + kin[name(t)]
    out_ref[...] = total[0:MB, 0:OB]
    for t in range(NDEV - 1):
        give(t).wait_send()


def fock(ints, ct, co, metric):
    vmem, hbm = pl.BlockSpec(memory_space=pltpu.VMEM), pl.BlockSpec(memory_space=pl.ANY)
    dma = pltpu.SemaphoreType.DMA
    return pl.pallas_call(
        kernel,
        name='fock',
        out_shape=jax.ShapeDtypeStruct((MB, OB), F32),
        in_specs=[hbm, vmem, vmem, vmem],
        out_specs=vmem,
        scratch_shapes=[
            pltpu.VMEM((NBUF * GR, QB, NB), F32),
            pltpu.VMEM((6 * GR, NORB * MP, QP), BF16),
            pltpu.VMEM((128, NB), BF16),
            pltpu.VMEM((4, NDEV * SP, 128), F32),
            pltpu.VMEM((NCH, NDEV, IV, MC, QP), BF16),
            pltpu.VMEM((NAUX, IV, NORB * NCH, MC, QP), BF16),
            pltpu.VMEM((IV, MP, QP), F32),
            pltpu.VMEM((MC, QP), F32),
            pltpu.VMEM((8, QP), F32),
            pltpu.VMEM((NDEV, 8, QP), F32),
            pltpu.VMEM((QB, QB), F32),
            pltpu.VMEM((QB, QB), F32),
            pltpu.VMEM((3, 2 * QP, 2 * QP), BF16),
            pltpu.VMEM((NORB * MP, QP), F32),
            pltpu.VMEM((QB, 128), F32),
            pltpu.VMEM((MP, 8, NB), F32),
            pltpu.VMEM((NORB * MP, NORB * MP), F32),
            pltpu.VMEM((NDEV, MP, 256), F32),
            pltpu.VMEM((NDEV, MP, 256), F32),
            dma((NBUF,)), dma((NDEV,)), dma((NDEV,)), dma((NDEV,)), dma((NDEV,)),
            dma((2,)), dma((2,)), dma((NDEV,)), dma((NDEV,)),
        ],
        compiler_params=pltpu.CompilerParams(collective_id=0, has_side_effects=True, vmem_limit_bytes=67043328),
    )(ints, ct, co, metric)


def solution(mesh):
    def local_fock(ints, metric, orbitals):
        orb = lax.axis_index('orb')
        c = orbitals[0]
        co = jnp.pad(lax.dynamic_slice_in_dim(c, orb * MB, MB, 0), ((0, MP - MB), (0, 128 - NI)))
        return fock(jnp.transpose(ints, (1, 0, 2)), c.T, co, metric)[None]

    return jax.shard_map(local_fock, mesh=mesh,
                         in_specs=(P(('sys', 'aux'), 'orb', None), P(('sys', 'aux'), None), P('sys', None, None)),
                         out_specs=P('sys', 'orb', 'aux'), check_vma=False)
```

```python
import jax
import jax.numpy as jnp
from jax import lax
from jax.experimental import pallas as pl
from jax.experimental.pallas import tpu as pltpu

P = jax.sharding.PartitionSpec
F32, BF16 = jnp.float32, jnp.bfloat16
MESH = pl.DeviceIdType.MESH
NT = (((1,), (1,)), ((), ()))
LN2 = 0.6931471805599453
TOP = 126.0
ROUND = 1.5 * 2.0 ** 15

NAUX, NORB, NDEV = 2, 4, 8
QB, MB, NB, NI = 464, 116, 464, 40
IV = NI // NDEV
QP, MP = 512, 120
MC = 8
NCH = MP // MC
TAIL = MB - MC * (NCH - 1)
SP = 48
GR = 4
NG = MB // GR
NBUF = 4
LAG = 4
MTURN = 6
NST = (NG + 1) // 2
OB = NB // NAUX
HQ = QB // 2


def split3(x):
    a = x.astype(BF16)
    r = x - a.astype(F32)
    b = r.astype(BF16)
    c = (r - b.astype(F32)).astype(BF16)
    return a, b, c


def kernel(b_hbm, ct_ref, co_ref, m_ref, out_ref,
           bbuf, bs, cw, abuf, sbuf, arecv, own, gbuf, gsend, grecv,
           md, mx, ms, af, wb, jp, kacc, kout, kin,
           bsem, ssem, rsem, gs_sem, gr_sem, ms_sem, mr_sem, ks_sem, kr_sem, rbuf, lsem, fsem):
    aux, orb = lax.axis_index('aux'), lax.axis_index('orb')
    me = aux * NORB + orb
    core = lax.rem(orb, 2)
    side = (aux, 1 - aux)

    chip = orb // 2

    STEPS = tuple((core, 1 - core, k) for k in range(2)) + tuple((1 - core, core, k) for k in range(2)) \
        + ((1, 1, 0), (1, 1, 1), (0, 0, 1))

    def peer(n):
        y, x, k = STEPS[n]
        return lax.rem(aux + y, 2), 2 * lax.rem(chip + x, 2) + lax.rem(core + k, 2)

    def name(n):
        y, x, k = STEPS[n]
        return 4 * y + 2 * x + k

    def at(n):
        a, o = peer(n)
        return {'aux': a, 'orb': o}

    def index(n):
        a, o = peer(n)
        return a * NORB + o

    def fetch(g):
        slot = g % NBUF if isinstance(g, int) else lax.rem(g, NBUF)
        return pltpu.make_async_copy(b_hbm.at[pl.ds(g * GR, GR)], bbuf.at[pl.ds(slot * GR, GR)], bsem.at[slot])

    for g in range(NBUF - 1):
        fetch(g).start()

    barrier = pltpu.get_barrier_semaphore()
    for t in range(NDEV - 1):
        pl.semaphore_signal(barrier, inc=1, device_id=at(t), device_id_type=MESH)

    for a in range(NAUX):
        @pl.when(aux == a)
        def _():
            md[...] = m_ref[:, a * QB:(a + 1) * QB]

    abuf[...] = jnp.zeros_like(abuf)
    gbuf[...] = jnp.zeros_like(gbuf)
    c1, c2, c3 = split3(ct_ref[...])
    cw[...] = jnp.concatenate(
        [c1.astype(F32), c2.astype(F32), c3.astype(F32), jnp.zeros((8, NB), F32)], axis=0).astype(BF16)

    pl.semaphore_wait(barrier, NDEV - 1)

    def mcopy(src, k, rows, dev):
        block = pl.ds(pl.multiple_of(rows * HQ, 8), HQ)
        return pltpu.make_async_remote_copy(src.at[block], mx.at[block], ms_sem.at[k], mr_sem.at[k],
                                            device_id=dev, device_id_type=MESH)
    mfirst = mcopy(md, 0, core, {'aux': 1 - aux, 'orb': orb})
    mfirst.start()

    def send(c, t):
        return pltpu.make_async_remote_copy(sbuf.at[c, index(t)], arecv.at[aux, :, orb * NCH + c],
                                            ssem.at[name(t)], rsem.at[name(t)], device_id=at(t), device_id_type=MESH)

    def relay(c, k):
        o = 2 * chip + lax.rem(core + k, 2)
        d = (1 - aux) * NORB + 2 * (1 - chip) + lax.rem(core + k, 2)
        return pltpu.make_async_remote_copy(sbuf.at[c, d], rbuf.at[core, c], ssem.at[6 + k], lsem.at[core, c],
                                            device_id={'aux': 1 - aux, 'orb': o}, device_id_type=MESH)

    def onward(c, k):
        return pltpu.make_async_remote_copy(
            rbuf.at[k, c], arecv.at[1 - aux, :, (2 * chip + k) * NCH + c], fsem.at[k],
            rsem.at[6 + lax.rem(k + core, 2)], device_id={'orb': 2 * (1 - chip) + core}, device_id_type=MESH)

    def arrived_relay(c, k):
        return pltpu.make_async_remote_copy(rbuf.at[k, c], rbuf.at[k, c], fsem.at[k], lsem.at[k, c],
                                            device_id={'orb': orb}, device_id_type=MESH)

    def pass_on(c):
        for k in range(2):
            arrived_relay(c, k).wait_recv()
            onward(c, k).start()

    def cut(g, half):
        slot = lax.rem(g, NBUF)
        for k in range(GR):
            for r in range(0, QB, 16):
                parts = split3(bbuf[slot * GR + k, r:r + 16, :])
                for j in range(3):
                    bs[3 * (half * GR + k) + j, r:r + 16, 0:NB] = parts[j]

    def dots(half):
        for k in range(half * GR, (half + 1) * GR):
            r = None
            for j in range(3):
                x = lax.dot_general(cw[...], bs[3 * k + j, 0:QB, 0:NB], NT, preferred_element_type=F32)
                r = x if r is None else r + x
            a2 = r[0:NI] + r[NI:2 * NI] + r[2 * NI:3 * NI]
            for v in range(IV):
                for lt in range(4):
                    l0, l1 = lt * 128, min(lt * 128 + 128, QB)
                    abuf[lt, pl.ds(v * MC + k, NDEV, stride=SP), 0:l1 - l0] = a2[8 * v:8 * v + 8, l0:l1]

    lane = lax.broadcasted_iota(jnp.int32, (MC, QP), 1)

    def deliver(c):
        g = gbuf[...]
        for s in range(NDEV):
            for v in range(IV):
                r0 = s * SP + v * MC
                col = co_ref[pl.ds(pl.multiple_of(c * MC, MC), MC), 8 * v + s:8 * v + s + 1]
                x = jnp.concatenate([abuf[lt, r0:r0 + MC, :] for lt in range(4)], axis=1)
                g = g + x * col
                big = jnp.maximum(jnp.max(jnp.abs(x), axis=1, keepdims=True), 2.0 ** -100)
                j = jnp.ceil(jnp.log(big * (1.0 / TOP)) * (1.0 / LN2) + 0.01)
                up = jnp.exp2(j).astype(BF16).astype(F32)
                down = jnp.exp2(-j).astype(BF16).astype(F32)
                y = jnp.exp2(x * down)
                sbuf[c, s, v] = jnp.where(lane < QB, y, up).astype(BF16)
        gbuf[...] = g
        for v in range(IV):
            r0 = pl.multiple_of(me * SP + v * MC, 8)
            own[v, pl.ds(pl.multiple_of(c * MC, MC), MC), :] = jnp.concatenate(
                [abuf[lt, pl.ds(r0, MC), :] for lt in range(4)], axis=1)
        for k in range(2):
            relay(c, k).start()
        for t in (0, 1, 2, 3, 6):
            send(c, t).start()

    fetch(0).wait()
    cut(jnp.int32(0), 0)

    msecond = mcopy(mx, 1, core, {'orb': orb + 1 - 2 * core})

    @pl.loop(0, NCH - 1)
    def _(c):
        @pl.when(c == MTURN)
        def _():
            mfirst.wait()
            msecond.start()

        fetch(2 * c + 1).wait()
        fetch(2 * c + 2).wait()

        @pl.when(2 * c + 3 < NG)
        def _():
            fetch(2 * c + 3).start()

        @pl.when(2 * c + 4 < NG)
        def _():
            fetch(2 * c + 4).start()

        cut(2 * c + 1, 1)
        dots(0)
        cut(2 * c + 2, 0)
        dots(1)
        deliver(c)

        @pl.when(c >= LAG)
        def _():
            pass_on(c - LAG)

    for g in range(NBUF):
        fetch(g).start()
    abuf[...] = jnp.zeros_like(abuf)
    dots(0)
    deliver(jnp.int32(NCH - 1))

    gsend[...] = jnp.broadcast_to(jnp.sum(gbuf[...], axis=0, keepdims=True), (8, QP))

    def gcopy(t):
        return pltpu.make_async_remote_copy(gsend, grecv.at[me], gs_sem.at[name(t)], gr_sem.at[name(t)],
                                            device_id=at(t), device_id_type=MESH)

    for t in range(NDEV - 1):
        gcopy(t).start()
    grecv[me] = gsend[...]

    ms[...] = jnp.zeros_like(ms)

    def parts_of(x, r, s):
        parts = split3(x)
        for j in range(3):
            ms[j, r * QP:r * QP + QB, s * QP:s * QP + QB] = parts[j]

    parts_of(md[...], 0, 0)
    for a in range(NAUX):
        @pl.when(aux == a)
        def _():
            off = m_ref[:, (1 - a) * QB:(2 - a) * QB]
            af[0:QB, 0:QB] = off
    parts_of(af[0:QB, 0:QB], 0, 1)
    parts_of(af[0:QB, 0:QB].T, 1, 0)
    msecond.wait_send()
    mcopy(mx, 1, 1 - core, {'orb': orb + 1 - 2 * core}).wait_recv()
    parts_of(mx[...], 1, 1)
    kacc[...] = jnp.zeros_like(kacc)

    def coulomb(s, base):
        for x in range(2):
            @pl.when(2 * s + x < NG)
            def _():
                fetch(2 * s + x).wait()
        @pl.loop(0, 2 * GR)
        def _(x):
            for l0, l1 in ((0, 128), (128, 256), (256, 384), (384, NB)):
                y = bbuf[base * GR + x, :, l0:l1] * wb[:, 0:l1 - l0]
                jp[2 * GR * s + x, :, l0:l1] = jnp.sum(y.reshape(QB // 8, 8, l1 - l0), axis=0)

        for x in range(2):
            @pl.when(2 * s + NBUF + x < NG)
            def _():
                fetch(2 * s + NBUF + x).start()

    @pl.loop(NCH - 1 - LAG, NCH)
    def _(c):
        pass_on(c)

    for t in range(NDEV - 1):
        a, o = peer(t)
        whole = arecv.at[a, :, pl.ds(o * NCH, NCH)]
        arrived = pltpu.make_async_remote_copy(whole, whole, ssem.at[name(t)], rsem.at[name(t)],
                                               device_id=at(t), device_id_type=MESH)
        arrived.wait_send()
        arrived.wait_recv()
    for k in range(2):
        whole = rbuf.at[k]
        pltpu.make_async_remote_copy(whole, whole, fsem.at[k], fsem.at[k],
                                     device_id={'orb': orb}, device_id_type=MESH).wait_send()

    for t in range(NDEV - 1):
        pltpu.make_async_remote_copy(gsend, grecv.at[index(t)], gs_sem.at[name(t)], gr_sem.at[name(t)],
                                     device_id=at(t), device_id_type=MESH).wait()
    off = af[0:QB, 0:QB]
    gam = [sum(grecv[side[r] * NORB + o][0:1, 0:QB] for o in range(NORB)) for r in range(2)]
    fit0 = jnp.sum(md[...] * gam[0], axis=1, keepdims=True) + jnp.sum(off * gam[1], axis=1, keepdims=True)
    turn = jnp.broadcast_to(gam[0], (128, QB)).T
    fit1 = (jnp.sum(off * turn[:, 0:1], axis=0, keepdims=True)
            + jnp.sum(mx[...] * jnp.broadcast_to(gam[1], (128, QB)).T[:, 0:1], axis=0, keepdims=True))
    wcol = jnp.sum(off * fit1, axis=1, keepdims=True)
    wrow = jnp.sum(md[...] * fit0, axis=0, keepdims=True)
    wb[...] = jnp.broadcast_to(wrow, (128, QB)).T + wcol

    PAIRS = ((0, 0), (0, 1), (1, 0), (1, 1), (0, 2), (2, 0))

    @pl.loop(0, IV)
    def _(v):
        def decode(sd, r):
            y = arecv[side[sd], v, r // MC:r // MC + 2].astype(F32).reshape(2 * MC, QP)
            u = jnp.log(y) * (1.0 / LN2)
            return ((u + ROUND) - ROUND) * y[:, QB:QB + 1]

        for r in range(0, NORB * MP, 16):
            af[r:r + 16, :] = decode(0, r)
        af[pl.ds(pl.multiple_of(orb * MP, 8), MP), :] = own[v]
        for r in range(0, NORB * MP, 16):
            for j, x in enumerate(split3(af[r:r + 16, :])):
                bs[j, r:r + 16, :] = x
            for j, x in enumerate(split3(decode(1, r))[:2]):
                bs[3 + j, r:r + 16, :] = x
        t = None
        for sd in range(2):
            for i, j in PAIRS[:6 - sd]:
                x = jnp.dot(bs[3 * sd + i], ms[j, sd * QP:(sd + 1) * QP, :], preferred_element_type=F32)
                t = x if t is None else t + x
        for j, x in enumerate(split3(t)):
            bs[5 + j], bs[8 + j] = x[:, 0:QP], x[:, QP:2 * QP]
        coulomb(3 * v, 2 * lax.rem(v, 2))
        half = jnp.asarray(0.5, BF16)
        s1 = None
        for b in (5, 8):
            t1, t2, t3 = bs[b], bs[b + 1], bs[b + 2]
            for x, y in ((t1, t1 * half), (t1, t2), (t1, t3), (t2, t2 * half)):
                z = lax.dot_general(x, y, NT, preferred_element_type=F32)
                s1 = z if s1 is None else s1 + z
        kacc[...] += s1
        coulomb(3 * v + 1, 2 - 2 * lax.rem(v, 2))
        coulomb(3 * v + 2, 2 * lax.rem(v, 2))

    k = kacc[...]
    k = k + k.T
    for a in range(NAUX):
        cols = jnp.concatenate([k[:, o * MP:o * MP + MB] for o in (2 * a, 2 * a + 1)], axis=1)
        for o in range(NORB):
            kout[a * NORB + o, :, 0:OB] = -cols[o * MP:(o + 1) * MP]
    j = jnp.sum(jp[...], axis=1)
    for a in range(NAUX):
        kout[a * NORB + orb, :, 0:OB] += 2.0 * j[:, a * OB:(a + 1) * OB]

    def give(t):
        return pltpu.make_async_remote_copy(kout.at[index(t)], kin.at[name(t)], ks_sem.at[name(t)], kr_sem.at[name(t)],
                                            device_id=at(t), device_id_type=MESH)

    for t in range(NDEV - 1):
        give(t).start()
    total = kout[me]
    for t in range(NDEV - 1):
        give(t).wait_recv()
        total = total + kin[name(t)]
    out_ref[...] = total[0:MB, 0:OB]
    for t in range(NDEV - 1):
        give(t).wait_send()


def fock(ints, ct, co, metric):
    vmem, hbm = pl.BlockSpec(memory_space=pltpu.VMEM), pl.BlockSpec(memory_space=pl.ANY)
    dma = pltpu.SemaphoreType.DMA
    return pl.pallas_call(
        kernel,
        name='fock',
        out_shape=jax.ShapeDtypeStruct((MB, OB), F32),
        in_specs=[hbm, vmem, vmem, vmem],
        out_specs=vmem,
        scratch_shapes=[
            pltpu.VMEM((NBUF * GR, QB, NB), F32),
            pltpu.VMEM((6 * GR, NORB * MP, QP), BF16),
            pltpu.VMEM((128, NB), BF16),
            pltpu.VMEM((4, NDEV * SP, 128), F32),
            pltpu.VMEM((NCH, NDEV, IV, MC, QP), BF16),
            pltpu.VMEM((NAUX, IV, NORB * NCH, MC, QP), BF16),
            pltpu.VMEM((IV, MP, QP), F32),
            pltpu.VMEM((MC, QP), F32),
            pltpu.VMEM((8, QP), F32),
            pltpu.VMEM((NDEV, 8, QP), F32),
            pltpu.VMEM((QB, QB), F32),
            pltpu.VMEM((QB, QB), F32),
            pltpu.VMEM((3, 2 * QP, 2 * QP), BF16),
            pltpu.VMEM((NORB * MP, QP), F32),
            pltpu.VMEM((QB, 128), F32),
            pltpu.VMEM((MP, 8, NB), F32),
            pltpu.VMEM((NORB * MP, NORB * MP), F32),
            pltpu.VMEM((NDEV, MP, 256), F32),
            pltpu.VMEM((NDEV, MP, 256), F32),
            dma((NBUF,)), dma((NDEV,)), dma((NDEV,)), dma((NDEV,)), dma((NDEV,)),
            dma((2,)), dma((2,)), dma((NDEV,)), dma((NDEV,)),
            pltpu.VMEM((2, NCH, IV, MC, QP), BF16), dma((2, NCH)), dma((2,)),
        ],
        compiler_params=pltpu.CompilerParams(collective_id=0, has_side_effects=True, vmem_limit_bytes=67043328),
    )(ints, ct, co, metric)


def solution(mesh):
    def local_fock(ints, metric, orbitals):
        orb = lax.axis_index('orb')
        c = orbitals[0]
        co = jnp.pad(lax.dynamic_slice_in_dim(c, orb * MB, MB, 0), ((0, MP - MB), (0, 128 - NI)))
        return fock(jnp.transpose(ints, (1, 0, 2)), c.T, co, metric)[None]

    return jax.shard_map(local_fock, mesh=mesh,
                         in_specs=(P(('sys', 'aux'), 'orb', None), P(('sys', 'aux'), None), P('sys', None, None)),
                         out_specs=P('sys', 'orb', 'aux'), check_vma=False)
```

```python
import jax
import jax.numpy as jnp
from jax import lax
from jax.experimental import pallas as pl
from jax.experimental.pallas import tpu as pltpu

P = jax.sharding.PartitionSpec
F32, BF16 = jnp.float32, jnp.bfloat16
MESH = pl.DeviceIdType.MESH
NT = (((1,), (1,)), ((), ()))
LN2 = 0.6931471805599453
TOP = 126.0
ROUND = 1.5 * 2.0 ** 15

NAUX, NORB, NDEV = 2, 4, 8
QB, MB, NB, NI = 464, 116, 464, 40
IV = NI // NDEV
QP, MP = 512, 120
MC = 8
NCH = MP // MC
TAIL = MB - MC * (NCH - 1)
SP = 48
GR = 4
NG = MB // GR
NBUF = 4
MTURN = 6
NST = (NG + 1) // 2
OB = NB // NAUX
HQ = QB // 2


def split3(x):
    a = x.astype(BF16)
    r = x - a.astype(F32)
    b = r.astype(BF16)
    c = (r - b.astype(F32)).astype(BF16)
    return a, b, c


def kernel(b_hbm, ct_ref, co_ref, m_ref, out_ref,
           bbuf, bs, cw, abuf, sbuf, arecv, own, gbuf, gsend, grecv,
           md, mx, ms, af, wb, jp, kacc, kout, kin,
           bsem, ssem, rsem, gs_sem, gr_sem, ms_sem, mr_sem, ks_sem, kr_sem):
    aux, orb = lax.axis_index('aux'), lax.axis_index('orb')
    me = aux * NORB + orb
    core = lax.rem(orb, 2)
    side = (aux, 1 - aux)

    chip = orb // 2

    STEPS = tuple((core, 1 - core, k) for k in range(2)) + tuple((1 - core, core, k) for k in range(2)) \
        + ((1, 1, 0), (1, 1, 1), (0, 0, 1))

    def peer(n):
        y, x, k = STEPS[n]
        return lax.rem(aux + y, 2), 2 * lax.rem(chip + x, 2) + lax.rem(core + k, 2)

    def name(n):
        y, x, k = STEPS[n]
        return 4 * y + 2 * x + k

    def at(n):
        a, o = peer(n)
        return {'aux': a, 'orb': o}

    def index(n):
        a, o = peer(n)
        return a * NORB + o

    def fetch(g):
        slot = g % NBUF if isinstance(g, int) else lax.rem(g, NBUF)
        return pltpu.make_async_copy(b_hbm.at[pl.ds(g * GR, GR)], bbuf.at[pl.ds(slot * GR, GR)], bsem.at[slot])

    for g in range(NBUF - 1):
        fetch(g).start()

    barrier = pltpu.get_barrier_semaphore()
    for t in range(NDEV - 1):
        pl.semaphore_signal(barrier, inc=1, device_id=at(t), device_id_type=MESH)

    for a in range(NAUX):
        @pl.when(aux == a)
        def _():
            md[...] = m_ref[:, a * QB:(a + 1) * QB]

    abuf[...] = jnp.zeros_like(abuf)
    gbuf[...] = jnp.zeros_like(gbuf)
    c1, c2, c3 = split3(ct_ref[...])
    cw[...] = jnp.concatenate(
        [c1.astype(F32), c2.astype(F32), c3.astype(F32), jnp.zeros((8, NB), F32)], axis=0).T.astype(BF16)

    pl.semaphore_wait(barrier, NDEV - 1)

    def mcopy(src, k, rows, dev):
        block = pl.ds(pl.multiple_of(rows * HQ, 8), HQ)
        return pltpu.make_async_remote_copy(src.at[block], mx.at[block], ms_sem.at[k], mr_sem.at[k],
                                            device_id=dev, device_id_type=MESH)
    mfirst = mcopy(md, 0, core, {'aux': 1 - aux, 'orb': orb})
    mfirst.start()

    def send(c, t):
        return pltpu.make_async_remote_copy(sbuf.at[c, index(t)], arecv.at[aux, :, orb * NCH + c],
                                            ssem.at[name(t)], rsem.at[name(t)], device_id=at(t), device_id_type=MESH)

    def cut(g, half):
        slot = lax.rem(g, NBUF)
        for k in range(GR):
            for r in range(0, QB, 16):
                parts = split3(bbuf[slot * GR + k, r:r + 16, :])
                for j in range(3):
                    bs[3 * (half * GR + k) + j, r:r + 16, 0:NB] = parts[j]

    def dots(half):
        for k in range(half * GR, (half + 1) * GR):
            r = None
            for j in range(3):
                x = jnp.dot(bs[3 * k + j, 0:QB, 0:NB], cw[...], preferred_element_type=F32)
                r = x if r is None else r + x
            r = r.T
            a2 = r[0:NI] + r[NI:2 * NI] + r[2 * NI:3 * NI]
            for v in range(IV):
                for lt in range(4):
                    l0, l1 = lt * 128, min(lt * 128 + 128, QB)
                    abuf[lt, pl.ds(v * MC + k, NDEV, stride=SP), 0:l1 - l0] = a2[8 * v:8 * v + 8, l0:l1]

    lane = lax.broadcasted_iota(jnp.int32, (MC, QP), 1)

    def deliver(c):
        g = gbuf[...]
        for s in range(NDEV):
            for v in range(IV):
                r0 = s * SP + v * MC
                col = co_ref[pl.ds(pl.multiple_of(c * MC, MC), MC), 8 * v + s:8 * v + s + 1]
                x = jnp.concatenate([abuf[lt, r0:r0 + MC, :] for lt in range(4)], axis=1)
                g = g + x * col
                big = jnp.maximum(jnp.max(jnp.abs(x), axis=1, keepdims=True), 2.0 ** -100)
                j = jnp.ceil(jnp.log(big * (1.0 / TOP)) * (1.0 / LN2) + 0.01)
                up = jnp.exp2(j).astype(BF16).astype(F32)
                down = jnp.exp2(-j).astype(BF16).astype(F32)
                y = jnp.exp2(x * down)
                sbuf[c, s, v] = jnp.where(lane < QB, y, up).astype(BF16)
        gbuf[...] = g
        for v in range(IV):
            r0 = pl.multiple_of(me * SP + v * MC, 8)
            own[v, pl.ds(pl.multiple_of(c * MC, MC), MC), :] = jnp.concatenate(
                [abuf[lt, pl.ds(r0, MC), :] for lt in range(4)], axis=1)
        for t in range(NDEV - 1):
            send(c, t).start()

    fetch(0).wait()
    cut(jnp.int32(0), 0)

    msecond = mcopy(mx, 1, core, {'orb': orb + 1 - 2 * core})

    @pl.loop(0, NCH - 1)
    def _(c):
        @pl.when(c == MTURN)
        def _():
            mfirst.wait()
            msecond.start()

        fetch(2 * c + 1).wait()
        fetch(2 * c + 2).wait()

        @pl.when(2 * c + 3 < NG)
        def _():
            fetch(2 * c + 3).start()

        @pl.when(2 * c + 4 < NG)
        def _():
            fetch(2 * c + 4).start()

        cut(2 * c + 1, 1)
        dots(0)
        cut(2 * c + 2, 0)
        dots(1)
        deliver(c)

    for g in range(NBUF):
        fetch(g).start()
    abuf[...] = jnp.zeros_like(abuf)
    dots(0)
    deliver(jnp.int32(NCH - 1))

    gsend[...] = jnp.broadcast_to(jnp.sum(gbuf[...], axis=0, keepdims=True), (8, QP))

    def gcopy(t):
        return pltpu.make_async_remote_copy(gsend, grecv.at[me], gs_sem.at[name(t)], gr_sem.at[name(t)],
                                            device_id=at(t), device_id_type=MESH)

    for t in range(NDEV - 1):
        gcopy(t).start()
    grecv[me] = gsend[...]

    ms[...] = jnp.zeros_like(ms)

    def parts_of(x, r, s):
        parts = split3(x)
        for j in range(3):
            ms[j, r * QP:r * QP + QB, s * QP:s * QP + QB] = parts[j]

    parts_of(md[...], 0, 0)
    for a in range(NAUX):
        @pl.when(aux == a)
        def _():
            off = m_ref[:, (1 - a) * QB:(2 - a) * QB]
            af[0:QB, 0:QB] = off
    parts_of(af[0:QB, 0:QB], 0, 1)
    parts_of(af[0:QB, 0:QB].T, 1, 0)
    msecond.wait_send()
    mcopy(mx, 1, 1 - core, {'orb': orb + 1 - 2 * core}).wait_recv()
    parts_of(mx[...], 1, 1)
    kacc[...] = jnp.zeros_like(kacc)

    def coulomb(s, base):
        for x in range(2):
            @pl.when(2 * s + x < NG)
            def _():
                fetch(2 * s + x).wait()
        @pl.loop(0, 2 * GR)
        def _(x):
            for l0, l1 in ((0, 128), (128, 256), (256, 384), (384, NB)):
                y = bbuf[base * GR + x, :, l0:l1] * wb[:, 0:l1 - l0]
                jp[2 * GR * s + x, :, l0:l1] = jnp.sum(y.reshape(QB // 8, 8, l1 - l0), axis=0)

        for x in range(2):
            @pl.when(2 * s + NBUF + x < NG)
            def _():
                fetch(2 * s + NBUF + x).start()

    for t in range(NDEV - 1):
        a, o = peer(t)
        whole = arecv.at[a, :, pl.ds(o * NCH, NCH)]
        arrived = pltpu.make_async_remote_copy(whole, whole, ssem.at[name(t)], rsem.at[name(t)],
                                               device_id=at(t), device_id_type=MESH)
        arrived.wait_send()
        arrived.wait_recv()

    for t in range(NDEV - 1):
        pltpu.make_async_remote_copy(gsend, grecv.at[index(t)], gs_sem.at[name(t)], gr_sem.at[name(t)],
                                     device_id=at(t), device_id_type=MESH).wait()
    off = af[0:QB, 0:QB]
    gam = [sum(grecv[side[r] * NORB + o][0:1, 0:QB] for o in range(NORB)) for r in range(2)]
    fit0 = jnp.sum(md[...] * gam[0], axis=1, keepdims=True) + jnp.sum(off * gam[1], axis=1, keepdims=True)
    turn = jnp.broadcast_to(gam[0], (128, QB)).T
    fit1 = (jnp.sum(off * turn[:, 0:1], axis=0, keepdims=True)
            + jnp.sum(mx[...] * jnp.broadcast_to(gam[1], (128, QB)).T[:, 0:1], axis=0, keepdims=True))
    wcol = jnp.sum(off * fit1, axis=1, keepdims=True)
    wrow = jnp.sum(md[...] * fit0, axis=0, keepdims=True)
    wb[...] = jnp.broadcast_to(wrow, (128, QB)).T + wcol

    PAIRS = ((0, 0), (0, 1), (1, 0), (1, 1), (0, 2), (2, 0))

    @pl.loop(0, IV)
    def _(v):
        def decode(sd, r):
            y = arecv[side[sd], v, r // MC:r // MC + 2].astype(F32).reshape(2 * MC, QP)
            u = jnp.log(y) * (1.0 / LN2)
            return ((u + ROUND) - ROUND) * y[:, QB:QB + 1]

        for r in range(0, NORB * MP, 16):
            af[r:r + 16, :] = decode(0, r)
        af[pl.ds(pl.multiple_of(orb * MP, 8), MP), :] = own[v]
        for r in range(0, NORB * MP, 16):
            for j, x in enumerate(split3(af[r:r + 16, :])):
                bs[j, r:r + 16, :] = x
            for j, x in enumerate(split3(decode(1, r))[:2]):
                bs[3 + j, r:r + 16, :] = x
        t = None
        for sd in range(2):
            for i, j in PAIRS[:6 - sd]:
                x = jnp.dot(bs[3 * sd + i], ms[j, sd * QP:(sd + 1) * QP, :], preferred_element_type=F32)
                t = x if t is None else t + x
        for j, x in enumerate(split3(t)):
            bs[5 + j], bs[8 + j] = x[:, 0:QP], x[:, QP:2 * QP]
        coulomb(3 * v, 2 * lax.rem(v, 2))
        half = jnp.asarray(0.5, BF16)
        s1 = None
        for b in (5, 8):
            t1, t2, t3 = bs[b], bs[b + 1], bs[b + 2]
            for x, y in ((t1, t1 * half), (t1, t2), (t1, t3), (t2, t2 * half)):
                z = lax.dot_general(x, y, NT, preferred_element_type=F32)
                s1 = z if s1 is None else s1 + z
        kacc[...] += s1
        coulomb(3 * v + 1, 2 - 2 * lax.rem(v, 2))
        coulomb(3 * v + 2, 2 * lax.rem(v, 2))

    k = kacc[...]
    k = k + k.T
    for a in range(NAUX):
        cols = jnp.concatenate([k[:, o * MP:o * MP + MB] for o in (2 * a, 2 * a + 1)], axis=1)
        for o in range(NORB):
            kout[a * NORB + o, :, 0:OB] = -cols[o * MP:(o + 1) * MP]
    j = jnp.sum(jp[...], axis=1)
    for a in range(NAUX):
        kout[a * NORB + orb, :, 0:OB] += 2.0 * j[:, a * OB:(a + 1) * OB]

    def give(t):
        return pltpu.make_async_remote_copy(kout.at[index(t)], kin.at[name(t)], ks_sem.at[name(t)], kr_sem.at[name(t)],
                                            device_id=at(t), device_id_type=MESH)

    for t in range(NDEV - 1):
        give(t).start()
    total = kout[me]
    for t in range(NDEV - 1):
        give(t).wait_recv()
        total = total + kin[name(t)]
    out_ref[...] = total[0:MB, 0:OB]
    for t in range(NDEV - 1):
        give(t).wait_send()


def fock(ints, ct, co, metric):
    vmem, hbm = pl.BlockSpec(memory_space=pltpu.VMEM), pl.BlockSpec(memory_space=pl.ANY)
    dma = pltpu.SemaphoreType.DMA
    return pl.pallas_call(
        kernel,
        name='fock',
        out_shape=jax.ShapeDtypeStruct((MB, OB), F32),
        in_specs=[hbm, vmem, vmem, vmem],
        out_specs=vmem,
        scratch_shapes=[
            pltpu.VMEM((NBUF * GR, QB, NB), F32),
            pltpu.VMEM((6 * GR, NORB * MP, QP), BF16),
            pltpu.VMEM((NB, 128), BF16),
            pltpu.VMEM((4, NDEV * SP, 128), F32),
            pltpu.VMEM((NCH, NDEV, IV, MC, QP), BF16),
            pltpu.VMEM((NAUX, IV, NORB * NCH, MC, QP), BF16),
            pltpu.VMEM((IV, MP, QP), F32),
            pltpu.VMEM((MC, QP), F32),
            pltpu.VMEM((8, QP), F32),
            pltpu.VMEM((NDEV, 8, QP), F32),
            pltpu.VMEM((QB, QB), F32),
            pltpu.VMEM((QB, QB), F32),
            pltpu.VMEM((3, 2 * QP, 2 * QP), BF16),
            pltpu.VMEM((NORB * MP, QP), F32),
            pltpu.VMEM((QB, 128), F32),
            pltpu.VMEM((MP, 8, NB), F32),
            pltpu.VMEM((NORB * MP, NORB * MP), F32),
            pltpu.VMEM((NDEV, MP, 256), F32),
            pltpu.VMEM((NDEV, MP, 256), F32),
            dma((NBUF,)), dma((NDEV,)), dma((NDEV,)), dma((NDEV,)), dma((NDEV,)),
            dma((2,)), dma((2,)), dma((NDEV,)), dma((NDEV,)),
        ],
        compiler_params=pltpu.CompilerParams(collective_id=0, has_side_effects=True, vmem_limit_bytes=67043328),
    )(ints, ct, co, metric)


def solution(mesh):
    def local_fock(ints, metric, orbitals):
        orb = lax.axis_index('orb')
        c = orbitals[0]
        co = jnp.pad(lax.dynamic_slice_in_dim(c, orb * MB, MB, 0), ((0, MP - MB), (0, 128 - NI)))
        return fock(jnp.transpose(ints, (1, 0, 2)), c.T, co, metric)[None]

    return jax.shard_map(local_fock, mesh=mesh,
                         in_specs=(P(('sys', 'aux'), 'orb', None), P(('sys', 'aux'), None), P('sys', None, None)),
                         out_specs=P('sys', 'orb', 'aux'), check_vma=False)
```

```python
import jax
import jax.numpy as jnp
from jax import lax
from jax.experimental import pallas as pl
from jax.experimental.pallas import tpu as pltpu

P = jax.sharding.PartitionSpec
F32, BF16 = jnp.float32, jnp.bfloat16
MESH = pl.DeviceIdType.MESH
NT = (((1,), (1,)), ((), ()))
LN2 = 0.6931471805599453
TOP = 126.0
ROUND = 1.5 * 2.0 ** 15

NAUX, NORB, NDEV = 2, 4, 8
QB, MB, NB, NI = 464, 116, 464, 40
IV = NI // NDEV
QP, MP = 512, 120
MC = 8
NCH = MP // MC
TAIL = MB - MC * (NCH - 1)
SP = 48
GR = 4
NG = MB // GR
NBUF = 4
MTURN = 6
NST = (NG + 1) // 2
OB = NB // NAUX
HQ = QB // 2


def split3(x):
    a = x.astype(BF16)
    r = x - a.astype(F32)
    b = r.astype(BF16)
    c = (r - b.astype(F32)).astype(BF16)
    return a, b, c


def kernel(b_hbm, ct_ref, co_ref, m_ref, out_ref,
           bbuf, bs, cw, abuf, sbuf, arecv, own, gbuf, gsend, grecv,
           md, mx, ms, af, wb, jp, kacc, kout, kin,
           bsem, ssem, rsem, gs_sem, gr_sem, ms_sem, mr_sem, ks_sem, kr_sem):
    aux, orb = lax.axis_index('aux'), lax.axis_index('orb')
    me = aux * NORB + orb
    core = lax.rem(orb, 2)
    side = (aux, 1 - aux)

    chip = orb // 2

    STEPS = tuple((core, 1 - core, k) for k in range(2)) + tuple((1 - core, core, k) for k in range(2)) \
        + ((1, 1, 0), (1, 1, 1), (0, 0, 1))

    def peer(n):
        y, x, k = STEPS[n]
        return lax.rem(aux + y, 2), 2 * lax.rem(chip + x, 2) + lax.rem(core + k, 2)

    def name(n):
        y, x, k = STEPS[n]
        return 4 * y + 2 * x + k

    def at(n):
        a, o = peer(n)
        return {'aux': a, 'orb': o}

    def index(n):
        a, o = peer(n)
        return a * NORB + o

    def fetch(g):
        slot = g % NBUF if isinstance(g, int) else lax.rem(g, NBUF)
        return pltpu.make_async_copy(b_hbm.at[pl.ds(g * GR, GR)], bbuf.at[pl.ds(slot * GR, GR)], bsem.at[slot])

    for g in range(NBUF - 1):
        fetch(g).start()

    barrier = pltpu.get_barrier_semaphore()
    for t in range(NDEV - 1):
        pl.semaphore_signal(barrier, inc=1, device_id=at(t), device_id_type=MESH)

    for a in range(NAUX):
        @pl.when(aux == a)
        def _():
            md[...] = m_ref[:, a * QB:(a + 1) * QB]

    abuf[...] = jnp.zeros_like(abuf)
    gbuf[...] = jnp.zeros_like(gbuf)
    c1, c2, c3 = split3(ct_ref[...])
    cw[...] = jnp.concatenate(
        [c1.astype(F32), c2.astype(F32), c3.astype(F32), jnp.zeros((8, NB), F32)], axis=0).T.astype(BF16)

    pl.semaphore_wait(barrier, NDEV - 1)

    def mcopy(src, k, rows, dev):
        block = pl.ds(pl.multiple_of(rows * HQ, 8), HQ)
        return pltpu.make_async_remote_copy(src.at[block], mx.at[block], ms_sem.at[k], mr_sem.at[k],
                                            device_id=dev, device_id_type=MESH)
    mfirst = mcopy(md, 0, core, {'aux': 1 - aux, 'orb': orb})
    mfirst.start()

    def send(c, t):
        return pltpu.make_async_remote_copy(sbuf.at[c, index(t)], arecv.at[aux, :, orb * NCH + c],
                                            ssem.at[name(t)], rsem.at[name(t)], device_id=at(t), device_id_type=MESH)

    def cut(g, ks):
        slot = lax.rem(g, NBUF)
        for k in ks:
            for r in range(0, QB, 16):
                parts = split3(bbuf[slot * GR + k, r:r + 16, :])
                for j in range(3):
                    bs[3 * k + j, r:r + 16, 0:NB] = parts[j]

    def dots(half, ks):
        for k in ks:
            r = None
            for j in range(3):
                x = jnp.dot(bs[3 * k + j, 0:QB, 0:NB], cw[...], preferred_element_type=F32)
                r = x if r is None else r + x
            r = r.T
            a2 = r[0:NI] + r[NI:2 * NI] + r[2 * NI:3 * NI]
            for v in range(IV):
                for lt in range(4):
                    l0, l1 = lt * 128, min(lt * 128 + 128, QB)
                    abuf[lt, pl.ds(v * MC + half * GR + k, NDEV, stride=SP), 0:l1 - l0] = a2[8 * v:8 * v + 8, l0:l1]

    lane = lax.broadcasted_iota(jnp.int32, (MC, QP), 1)

    def deliver(c):
        g = gbuf[...]
        for s in range(NDEV):
            for v in range(IV):
                r0 = s * SP + v * MC
                col = co_ref[pl.ds(pl.multiple_of(c * MC, MC), MC), 8 * v + s:8 * v + s + 1]
                x = jnp.concatenate([abuf[lt, r0:r0 + MC, :] for lt in range(4)], axis=1)
                g = g + x * col
                big = jnp.maximum(jnp.max(jnp.abs(x), axis=1, keepdims=True), 2.0 ** -100)
                j = jnp.ceil(jnp.log(big * (1.0 / TOP)) * (1.0 / LN2) + 0.01)
                up = jnp.exp2(j).astype(BF16).astype(F32)
                down = jnp.exp2(-j).astype(BF16).astype(F32)
                y = jnp.exp2(x * down)
                sbuf[c, s, v] = jnp.where(lane < QB, y, up).astype(BF16)
        gbuf[...] = g
        for v in range(IV):
            r0 = pl.multiple_of(me * SP + v * MC, 8)
            own[v, pl.ds(pl.multiple_of(c * MC, MC), MC), :] = jnp.concatenate(
                [abuf[lt, pl.ds(r0, MC), :] for lt in range(4)], axis=1)
        for t in range(NDEV - 1):
            send(c, t).start()

    fetch(0).wait()
    cut(jnp.int32(0), range(GR))

    msecond = mcopy(mx, 1, core, {'orb': orb + 1 - 2 * core})

    @pl.loop(0, NCH - 1)
    def _(c):
        @pl.when(c == MTURN)
        def _():
            mfirst.wait()
            msecond.start()

        fetch(2 * c + 1).wait()
        fetch(2 * c + 2).wait()

        @pl.when(2 * c + 3 < NG)
        def _():
            fetch(2 * c + 3).start()

        @pl.when(2 * c + 4 < NG)
        def _():
            fetch(2 * c + 4).start()

        for half in range(2):
            for k in range(GR):
                dots(half, (k,))
                cut(2 * c + 1 + half, (k,))
        deliver(c)

    for g in range(NBUF):
        fetch(g).start()
    abuf[...] = jnp.zeros_like(abuf)
    dots(0, range(GR))
    deliver(jnp.int32(NCH - 1))

    gsend[...] = jnp.broadcast_to(jnp.sum(gbuf[...], axis=0, keepdims=True), (8, QP))

    def gcopy(t):
        return pltpu.make_async_remote_copy(gsend, grecv.at[me], gs_sem.at[name(t)], gr_sem.at[name(t)],
                                            device_id=at(t), device_id_type=MESH)

    for t in range(NDEV - 1):
        gcopy(t).start()
    grecv[me] = gsend[...]

    ms[...] = jnp.zeros_like(ms)

    def parts_of(x, r, s):
        parts = split3(x)
        for j in range(3):
            ms[j, r * QP:r * QP + QB, s * QP:s * QP + QB] = parts[j]

    parts_of(md[...], 0, 0)
    for a in range(NAUX):
        @pl.when(aux == a)
        def _():
            off = m_ref[:, (1 - a) * QB:(2 - a) * QB]
            af[0:QB, 0:QB] = off
    parts_of(af[0:QB, 0:QB], 0, 1)
    parts_of(af[0:QB, 0:QB].T, 1, 0)
    msecond.wait_send()
    mcopy(mx, 1, 1 - core, {'orb': orb + 1 - 2 * core}).wait_recv()
    parts_of(mx[...], 1, 1)
    kacc[...] = jnp.zeros_like(kacc)

    def coulomb(s, base):
        for x in range(2):
            @pl.when(2 * s + x < NG)
            def _():
                fetch(2 * s + x).wait()
        @pl.loop(0, 2 * GR)
        def _(x):
            for l0, l1 in ((0, 128), (128, 256), (256, 384), (384, NB)):
                y = bbuf[base * GR + x, :, l0:l1] * wb[:, 0:l1 - l0]
                jp[2 * GR * s + x, :, l0:l1] = jnp.sum(y.reshape(QB // 8, 8, l1 - l0), axis=0)

        for x in range(2):
            @pl.when(2 * s + NBUF + x < NG)
            def _():
                fetch(2 * s + NBUF + x).start()

    for t in range(NDEV - 1):
        a, o = peer(t)
        whole = arecv.at[a, :, pl.ds(o * NCH, NCH)]
        arrived = pltpu.make_async_remote_copy(whole, whole, ssem.at[name(t)], rsem.at[name(t)],
                                               device_id=at(t), device_id_type=MESH)
        arrived.wait_send()
        arrived.wait_recv()

    for t in range(NDEV - 1):
        pltpu.make_async_remote_copy(gsend, grecv.at[index(t)], gs_sem.at[name(t)], gr_sem.at[name(t)],
                                     device_id=at(t), device_id_type=MESH).wait()
    off = af[0:QB, 0:QB]
    gam = [sum(grecv[side[r] * NORB + o][0:1, 0:QB] for o in range(NORB)) for r in range(2)]
    fit0 = jnp.sum(md[...] * gam[0], axis=1, keepdims=True) + jnp.sum(off * gam[1], axis=1, keepdims=True)
    turn = jnp.broadcast_to(gam[0], (128, QB)).T
    fit1 = (jnp.sum(off * turn[:, 0:1], axis=0, keepdims=True)
            + jnp.sum(mx[...] * jnp.broadcast_to(gam[1], (128, QB)).T[:, 0:1], axis=0, keepdims=True))
    wcol = jnp.sum(off * fit1, axis=1, keepdims=True)
    wrow = jnp.sum(md[...] * fit0, axis=0, keepdims=True)
    wb[...] = jnp.broadcast_to(wrow, (128, QB)).T + wcol

    PAIRS = ((0, 0), (0, 1), (1, 0), (1, 1), (0, 2), (2, 0))

    @pl.loop(0, IV)
    def _(v):
        def decode(sd, r):
            y = arecv[side[sd], v, r // MC:r // MC + 2].astype(F32).reshape(2 * MC, QP)
            u = jnp.log(y) * (1.0 / LN2)
            return ((u + ROUND) - ROUND) * y[:, QB:QB + 1]

        for r in range(0, NORB * MP, 16):
            af[r:r + 16, :] = decode(0, r)
        af[pl.ds(pl.multiple_of(orb * MP, 8), MP), :] = own[v]
        for r in range(0, NORB * MP, 16):
            for j, x in enumerate(split3(af[r:r + 16, :])):
                bs[j, r:r + 16, :] = x
            for j, x in enumerate(split3(decode(1, r))[:2]):
                bs[3 + j, r:r + 16, :] = x
        t = None
        for sd in range(2):
            for i, j in PAIRS[:6 - sd]:
                x = jnp.dot(bs[3 * sd + i], ms[j, sd * QP:(sd + 1) * QP, :], preferred_element_type=F32)
                t = x if t is None else t + x
        for j, x in enumerate(split3(t)):
            bs[5 + j], bs[8 + j] = x[:, 0:QP], x[:, QP:2 * QP]
        coulomb(3 * v, 2 * lax.rem(v, 2))
        half = jnp.asarray(0.5, BF16)
        s1 = None
        for b in (5, 8):
            t1, t2, t3 = bs[b], bs[b + 1], bs[b + 2]
            for x, y in ((t1, t1 * half), (t1, t2), (t1, t3), (t2, t2 * half)):
                z = lax.dot_general(x, y, NT, preferred_element_type=F32)
                s1 = z if s1 is None else s1 + z
        kacc[...] += s1
        coulomb(3 * v + 1, 2 - 2 * lax.rem(v, 2))
        coulomb(3 * v + 2, 2 * lax.rem(v, 2))

    k = kacc[...]
    k = k + k.T
    for a in range(NAUX):
        cols = jnp.concatenate([k[:, o * MP:o * MP + MB] for o in (2 * a, 2 * a + 1)], axis=1)
        for o in range(NORB):
            kout[a * NORB + o, :, 0:OB] = -cols[o * MP:(o + 1) * MP]
    j = jnp.sum(jp[...], axis=1)
    for a in range(NAUX):
        kout[a * NORB + orb, :, 0:OB] += 2.0 * j[:, a * OB:(a + 1) * OB]

    def give(t):
        return pltpu.make_async_remote_copy(kout.at[index(t)], kin.at[name(t)], ks_sem.at[name(t)], kr_sem.at[name(t)],
                                            device_id=at(t), device_id_type=MESH)

    for t in range(NDEV - 1):
        give(t).start()
    total = kout[me]
    for t in range(NDEV - 1):
        give(t).wait_recv()
        total = total + kin[name(t)]
    out_ref[...] = total[0:MB, 0:OB]
    for t in range(NDEV - 1):
        give(t).wait_send()


def fock(ints, ct, co, metric):
    vmem, hbm = pl.BlockSpec(memory_space=pltpu.VMEM), pl.BlockSpec(memory_space=pl.ANY)
    dma = pltpu.SemaphoreType.DMA
    return pl.pallas_call(
        kernel,
        name='fock',
        out_shape=jax.ShapeDtypeStruct((MB, OB), F32),
        in_specs=[hbm, vmem, vmem, vmem],
        out_specs=vmem,
        scratch_shapes=[
            pltpu.VMEM((NBUF * GR, QB, NB), F32),
            pltpu.VMEM((3 * GR, NORB * MP, QP), BF16),
            pltpu.VMEM((NB, 128), BF16),
            pltpu.VMEM((4, NDEV * SP, 128), F32),
            pltpu.VMEM((NCH, NDEV, IV, MC, QP), BF16),
            pltpu.VMEM((NAUX, IV, NORB * NCH, MC, QP), BF16),
            pltpu.VMEM((IV, MP, QP), F32),
            pltpu.VMEM((MC, QP), F32),
            pltpu.VMEM((8, QP), F32),
            pltpu.VMEM((NDEV, 8, QP), F32),
            pltpu.VMEM((QB, QB), F32),
            pltpu.VMEM((QB, QB), F32),
            pltpu.VMEM((3, 2 * QP, 2 * QP), BF16),
            pltpu.VMEM((NORB * MP, QP), F32),
            pltpu.VMEM((QB, 128), F32),
            pltpu.VMEM((MP, 8, NB), F32),
            pltpu.VMEM((NORB * MP, NORB * MP), F32),
            pltpu.VMEM((NDEV, MP, 256), F32),
            pltpu.VMEM((NDEV, MP, 256), F32),
            dma((NBUF,)), dma((NDEV,)), dma((NDEV,)), dma((NDEV,)), dma((NDEV,)),
            dma((2,)), dma((2,)), dma((NDEV,)), dma((NDEV,)),
        ],
        compiler_params=pltpu.CompilerParams(collective_id=0, has_side_effects=True, vmem_limit_bytes=67043328),
    )(ints, ct, co, metric)


def solution(mesh):
    def local_fock(ints, metric, orbitals):
        orb = lax.axis_index('orb')
        c = orbitals[0]
        co = jnp.pad(lax.dynamic_slice_in_dim(c, orb * MB, MB, 0), ((0, MP - MB), (0, 128 - NI)))
        return fock(jnp.transpose(ints, (1, 0, 2)), c.T, co, metric)[None]

    return jax.shard_map(local_fock, mesh=mesh,
                         in_specs=(P(('sys', 'aux'), 'orb', None), P(('sys', 'aux'), None), P('sys', None, None)),
                         out_specs=P('sys', 'orb', 'aux'), check_vma=False)
```

```python
import jax
import jax.numpy as jnp
from jax import lax
from jax.experimental import pallas as pl
from jax.experimental.pallas import tpu as pltpu

P = jax.sharding.PartitionSpec
F32, BF16 = jnp.float32, jnp.bfloat16
MESH = pl.DeviceIdType.MESH
NT = (((1,), (1,)), ((), ()))
LN2 = 0.6931471805599453
TOP = 126.0
ROUND = 1.5 * 2.0 ** 15

NAUX, NORB, NDEV = 2, 4, 8
QB, MB, NB, NI = 464, 116, 464, 40
IV = NI // NDEV
QP, MP = 512, 120
MC = 8
NCH = MP // MC
TAIL = MB - MC * (NCH - 1)
SP = 48
GR = 4
NG = MB // GR
NBUF = 4
MTURN = 6
NST = (NG + 1) // 2
OB = NB // NAUX
HQ = QB // 2


def split3(x):
    a = x.astype(BF16)
    r = x - a.astype(F32)
    b = r.astype(BF16)
    c = (r - b.astype(F32)).astype(BF16)
    return a, b, c


def kernel(b_hbm, ct_ref, co_ref, m_ref, out_ref,
           bbuf, bs, cw, abuf, sbuf, arecv, own, gbuf, gsend, grecv,
           md, mx, ms, af, wb, jp, kacc, kout, kin,
           bsem, ssem, rsem, gs_sem, gr_sem, ms_sem, mr_sem, ks_sem, kr_sem):
    aux, orb = lax.axis_index('aux'), lax.axis_index('orb')
    me = aux * NORB + orb
    core = lax.rem(orb, 2)
    side = (aux, 1 - aux)

    chip = orb // 2

    STEPS = tuple((core, 1 - core, k) for k in range(2)) + tuple((1 - core, core, k) for k in range(2)) \
        + ((1, 1, 0), (1, 1, 1), (0, 0, 1))

    def peer(n):
        y, x, k = STEPS[n]
        return lax.rem(aux + y, 2), 2 * lax.rem(chip + x, 2) + lax.rem(core + k, 2)

    def name(n):
        y, x, k = STEPS[n]
        return 4 * y + 2 * x + k

    def at(n):
        a, o = peer(n)
        return {'aux': a, 'orb': o}

    def index(n):
        a, o = peer(n)
        return a * NORB + o

    def fetch(g):
        slot = g % NBUF if isinstance(g, int) else lax.rem(g, NBUF)
        return pltpu.make_async_copy(b_hbm.at[pl.ds(g * GR, GR)], bbuf.at[pl.ds(slot * GR, GR)], bsem.at[slot])

    for g in range(NBUF - 1):
        fetch(g).start()

    barrier = pltpu.get_barrier_semaphore()
    for t in range(NDEV - 1):
        pl.semaphore_signal(barrier, inc=1, device_id=at(t), device_id_type=MESH)

    for a in range(NAUX):
        @pl.when(aux == a)
        def _():
            md[...] = m_ref[:, a * QB:(a + 1) * QB]

    abuf[...] = jnp.zeros_like(abuf)
    gbuf[...] = jnp.zeros_like(gbuf)
    c1, c2, c3 = split3(ct_ref[...])
    cw[...] = jnp.concatenate(
        [c1.astype(F32), c2.astype(F32), c3.astype(F32), jnp.zeros((8, NB), F32)], axis=0).T.astype(BF16)

    ms[...] = jnp.zeros_like(ms)

    def parts_of(x, r, s):
        parts = split3(x)
        for j in range(3):
            ms[j, r * QP:r * QP + QB, s * QP:s * QP + QB] = parts[j]

    parts_of(md[...], 0, 0)
    for a in range(NAUX):
        @pl.when(aux == a)
        def _():
            off = m_ref[:, (1 - a) * QB:(2 - a) * QB]
            af[0:QB, 0:QB] = off
    parts_of(af[0:QB, 0:QB], 0, 1)
    parts_of(af[0:QB, 0:QB].T, 1, 0)

    pl.semaphore_wait(barrier, NDEV - 1)

    def mcopy(src, k, rows, dev):
        block = pl.ds(pl.multiple_of(rows * HQ, 8), HQ)
        return pltpu.make_async_remote_copy(src.at[block], mx.at[block], ms_sem.at[k], mr_sem.at[k],
                                            device_id=dev, device_id_type=MESH)
    mfirst = mcopy(md, 0, core, {'aux': 1 - aux, 'orb': orb})
    mfirst.start()

    def send(c, t):
        return pltpu.make_async_remote_copy(sbuf.at[c, index(t)], arecv.at[aux, :, orb * NCH + c],
                                            ssem.at[name(t)], rsem.at[name(t)], device_id=at(t), device_id_type=MESH)

    def cut(g, half):
        slot = lax.rem(g, NBUF)
        for k in range(GR):
            for r in range(0, QB, 16):
                parts = split3(bbuf[slot * GR + k, r:r + 16, :])
                for j in range(3):
                    bs[3 * (half * GR + k) + j, r:r + 16, 0:NB] = parts[j]

    def dots(half):
        for k in range(half * GR, (half + 1) * GR):
            r = None
            for j in range(3):
                x = jnp.dot(bs[3 * k + j, 0:QB, 0:NB], cw[...], preferred_element_type=F32)
                r = x if r is None else r + x
            r = r.T
            a2 = r[0:NI] + r[NI:2 * NI] + r[2 * NI:3 * NI]
            for v in range(IV):
                for lt in range(4):
                    l0, l1 = lt * 128, min(lt * 128 + 128, QB)
                    abuf[lt, pl.ds(v * MC + k, NDEV, stride=SP), 0:l1 - l0] = a2[8 * v:8 * v + 8, l0:l1]

    lane = lax.broadcasted_iota(jnp.int32, (MC, QP), 1)

    def deliver(c):
        g = gbuf[...]
        for s in range(NDEV):
            for v in range(IV):
                r0 = s * SP + v * MC
                col = co_ref[pl.ds(pl.multiple_of(c * MC, MC), MC), 8 * v + s:8 * v + s + 1]
                x = jnp.concatenate([abuf[lt, r0:r0 + MC, :] for lt in range(4)], axis=1)
                g = g + x * col
                big = jnp.maximum(jnp.max(jnp.abs(x), axis=1, keepdims=True), 2.0 ** -100)
                j = jnp.ceil(jnp.log(big * (1.0 / TOP)) * (1.0 / LN2) + 0.01)
                up = jnp.exp2(j).astype(BF16).astype(F32)
                down = jnp.exp2(-j).astype(BF16).astype(F32)
                y = jnp.exp2(x * down)
                sbuf[c, s, v] = jnp.where(lane < QB, y, up).astype(BF16)
        gbuf[...] = g
        for v in range(IV):
            r0 = pl.multiple_of(me * SP + v * MC, 8)
            own[v, pl.ds(pl.multiple_of(c * MC, MC), MC), :] = jnp.concatenate(
                [abuf[lt, pl.ds(r0, MC), :] for lt in range(4)], axis=1)
        for t in range(NDEV - 1):
            send(c, t).start()

    fetch(0).wait()
    cut(jnp.int32(0), 0)

    msecond = mcopy(mx, 1, core, {'orb': orb + 1 - 2 * core})

    @pl.loop(0, NCH - 1)
    def _(c):
        @pl.when(c == MTURN)
        def _():
            mfirst.wait()
            msecond.start()

        fetch(2 * c + 1).wait()
        fetch(2 * c + 2).wait()

        @pl.when(2 * c + 3 < NG)
        def _():
            fetch(2 * c + 3).start()

        @pl.when(2 * c + 4 < NG)
        def _():
            fetch(2 * c + 4).start()

        cut(2 * c + 1, 1)
        dots(0)
        cut(2 * c + 2, 0)
        dots(1)
        deliver(c)

    for g in range(NBUF):
        fetch(g).start()
    abuf[...] = jnp.zeros_like(abuf)
    dots(0)
    deliver(jnp.int32(NCH - 1))

    gsend[...] = jnp.broadcast_to(jnp.sum(gbuf[...], axis=0, keepdims=True), (8, QP))

    def gcopy(t):
        return pltpu.make_async_remote_copy(gsend, grecv.at[me], gs_sem.at[name(t)], gr_sem.at[name(t)],
                                            device_id=at(t), device_id_type=MESH)

    for t in range(NDEV - 1):
        gcopy(t).start()
    grecv[me] = gsend[...]

    msecond.wait_send()
    mcopy(mx, 1, 1 - core, {'orb': orb + 1 - 2 * core}).wait_recv()
    parts_of(mx[...], 1, 1)
    kacc[...] = jnp.zeros_like(kacc)

    def coulomb(s, base):
        for x in range(2):
            @pl.when(2 * s + x < NG)
            def _():
                fetch(2 * s + x).wait()
        @pl.loop(0, 2 * GR)
        def _(x):
            for l0, l1 in ((0, 128), (128, 256), (256, 384), (384, NB)):
                y = bbuf[base * GR + x, :, l0:l1] * wb[:, 0:l1 - l0]
                jp[2 * GR * s + x, :, l0:l1] = jnp.sum(y.reshape(QB // 8, 8, l1 - l0), axis=0)

        for x in range(2):
            @pl.when(2 * s + NBUF + x < NG)
            def _():
                fetch(2 * s + NBUF + x).start()

    for t in range(NDEV - 1):
        a, o = peer(t)
        whole = arecv.at[a, :, pl.ds(o * NCH, NCH)]
        arrived = pltpu.make_async_remote_copy(whole, whole, ssem.at[name(t)], rsem.at[name(t)],
                                               device_id=at(t), device_id_type=MESH)
        arrived.wait_send()
        arrived.wait_recv()

    for t in range(NDEV - 1):
        pltpu.make_async_remote_copy(gsend, grecv.at[index(t)], gs_sem.at[name(t)], gr_sem.at[name(t)],
                                     device_id=at(t), device_id_type=MESH).wait()
    off = af[0:QB, 0:QB]
    gam = [sum(grecv[side[r] * NORB + o][0:1, 0:QB] for o in range(NORB)) for r in range(2)]
    fit0 = jnp.sum(md[...] * gam[0], axis=1, keepdims=True) + jnp.sum(off * gam[1], axis=1, keepdims=True)
    turn = jnp.broadcast_to(gam[0], (128, QB)).T
    fit1 = (jnp.sum(off * turn[:, 0:1], axis=0, keepdims=True)
            + jnp.sum(mx[...] * jnp.broadcast_to(gam[1], (128, QB)).T[:, 0:1], axis=0, keepdims=True))
    wcol = jnp.sum(off * fit1, axis=1, keepdims=True)
    wrow = jnp.sum(md[...] * fit0, axis=0, keepdims=True)
    wb[...] = jnp.broadcast_to(wrow, (128, QB)).T + wcol

    PAIRS = ((0, 0), (0, 1), (1, 0), (1, 1), (0, 2), (2, 0))

    @pl.loop(0, IV)
    def _(v):
        def decode(sd, r):
            y = arecv[side[sd], v, r // MC:r // MC + 2].astype(F32).reshape(2 * MC, QP)
            u = jnp.log(y) * (1.0 / LN2)
            return ((u + ROUND) - ROUND) * y[:, QB:QB + 1]

        for r in range(0, NORB * MP, 16):
            af[r:r + 16, :] = decode(0, r)
        af[pl.ds(pl.multiple_of(orb * MP, 8), MP), :] = own[v]
        for r in range(0, NORB * MP, 16):
            for j, x in enumerate(split3(af[r:r + 16, :])):
                bs[j, r:r + 16, :] = x
            for j, x in enumerate(split3(decode(1, r))[:2]):
                bs[3 + j, r:r + 16, :] = x
        t = None
        for sd in range(2):
            for i, j in PAIRS[:6 - sd]:
                x = jnp.dot(bs[3 * sd + i], ms[j, sd * QP:(sd + 1) * QP, :], preferred_element_type=F32)
                t = x if t is None else t + x
        for j, x in enumerate(split3(t)):
            bs[5 + j], bs[8 + j] = x[:, 0:QP], x[:, QP:2 * QP]
        coulomb(3 * v, 2 * lax.rem(v, 2))
        half = jnp.asarray(0.5, BF16)
        s1 = None
        for b in (5, 8):
            t1, t2, t3 = bs[b], bs[b + 1], bs[b + 2]
            for x, y in ((t1, t1 * half), (t1, t2), (t1, t3), (t2, t2 * half)):
                z = lax.dot_general(x, y, NT, preferred_element_type=F32)
                s1 = z if s1 is None else s1 + z
        kacc[...] += s1
        coulomb(3 * v + 1, 2 - 2 * lax.rem(v, 2))
        coulomb(3 * v + 2, 2 * lax.rem(v, 2))

    k = kacc[...]
    k = k + k.T
    for a in range(NAUX):
        cols = jnp.concatenate([k[:, o * MP:o * MP + MB] for o in (2 * a, 2 * a + 1)], axis=1)
        for o in range(NORB):
            kout[o % 2, 2 * a + o // 2, :, 0:OB] = -cols[o * MP:(o + 1) * MP]
    j = jnp.sum(jp[...], axis=1)
    for a in range(NAUX):
        kout[core, 2 * a + chip, :, 0:OB] += 2.0 * j[:, a * OB:(a + 1) * OB]

    pair = pltpu.make_async_remote_copy(kout.at[1 - core], kin.at[pl.ds(0, 4)], ks_sem.at[0], kr_sem.at[0],
                                        device_id=at(6), device_id_type=MESH)
    pair.start()
    pair.wait()
    for b in range(4):
        kout[core, b] = kout[core, b] + kin[b]

    def give(t):
        a, o = peer(t)
        return pltpu.make_async_remote_copy(kout.at[core, 2 * a + o // 2], kin.at[3 + name(t) // 2],
                                            ks_sem.at[name(t)], kr_sem.at[name(t)],
                                            device_id=at(t), device_id_type=MESH)

    for t in (0, 2, 4):
        give(t).start()
    total = kout[core, 2 * aux + chip]
    for t in (0, 2, 4):
        give(t).wait_recv()
        total = total + kin[3 + name(t) // 2]
    out_ref[...] = total[0:MB, 0:OB]
    for t in (0, 2, 4):
        give(t).wait_send()


def fock(ints, ct, co, metric):
    vmem, hbm = pl.BlockSpec(memory_space=pltpu.VMEM), pl.BlockSpec(memory_space=pl.ANY)
    dma = pltpu.SemaphoreType.DMA
    return pl.pallas_call(
        kernel,
        name='fock',
        out_shape=jax.ShapeDtypeStruct((MB, OB), F32),
        in_specs=[hbm, vmem, vmem, vmem],
        out_specs=vmem,
        scratch_shapes=[
            pltpu.VMEM((NBUF * GR, QB, NB), F32),
            pltpu.VMEM((6 * GR, NORB * MP, QP), BF16),
            pltpu.VMEM((NB, 128), BF16),
            pltpu.VMEM((4, NDEV * SP, 128), F32),
            pltpu.VMEM((NCH, NDEV, IV, MC, QP), BF16),
            pltpu.VMEM((NAUX, IV, NORB * NCH, MC, QP), BF16),
            pltpu.VMEM((IV, MP, QP), F32),
            pltpu.VMEM((MC, QP), F32),
            pltpu.VMEM((8, QP), F32),
            pltpu.VMEM((NDEV, 8, QP), F32),
            pltpu.VMEM((QB, QB), F32),
            pltpu.VMEM((QB, QB), F32),
            pltpu.VMEM((3, 2 * QP, 2 * QP), BF16),
            pltpu.VMEM((NORB * MP, QP), F32),
            pltpu.VMEM((QB, 128), F32),
            pltpu.VMEM((MP, 8, NB), F32),
            pltpu.VMEM((NORB * MP, NORB * MP), F32),
            pltpu.VMEM((2, 4, MP, 256), F32),
            pltpu.VMEM((7, MP, 256), F32),
            dma((NBUF,)), dma((NDEV,)), dma((NDEV,)), dma((NDEV,)), dma((NDEV,)),
            dma((2,)), dma((2,)), dma((NDEV,)), dma((NDEV,)),
        ],
        compiler_params=pltpu.CompilerParams(collective_id=0, has_side_effects=True, vmem_limit_bytes=67043328),
    )(ints, ct, co, metric)


def solution(mesh):
    def local_fock(ints, metric, orbitals):
        orb = lax.axis_index('orb')
        c = orbitals[0]
        co = jnp.pad(lax.dynamic_slice_in_dim(c, orb * MB, MB, 0), ((0, MP - MB), (0, 128 - NI)))
        return fock(jnp.transpose(ints, (1, 0, 2)), c.T, co, metric)[None]

    return jax.shard_map(local_fock, mesh=mesh,
                         in_specs=(P(('sys', 'aux'), 'orb', None), P(('sys', 'aux'), None), P('sys', None, None)),
                         out_specs=P('sys', 'orb', 'aux'), check_vma=False)
```

```python
import jax
import jax.numpy as jnp
from jax import lax
from jax.experimental import pallas as pl
from jax.experimental.pallas import tpu as pltpu

P = jax.sharding.PartitionSpec
F32, BF16 = jnp.float32, jnp.bfloat16
MESH = pl.DeviceIdType.MESH
NT = (((1,), (1,)), ((), ()))
LN2 = 0.6931471805599453
TOP = 126.0
ROUND = 1.5 * 2.0 ** 15

NAUX, NORB, NDEV = 2, 4, 8
QB, MB, NB, NI = 464, 116, 464, 40
IV = NI // NDEV
QP, MP = 512, 120
MC = 8
NCH = MP // MC
TAIL = MB - MC * (NCH - 1)
SP = 40
GR = 4
NG = MB // GR
NBUF = 4
MTURN = 6
NST = (NG + 1) // 2
OB = NB // NAUX
HQ = QB // 2


def split3(x):
    a = x.astype(BF16)
    r = x - a.astype(F32)
    b = r.astype(BF16)
    c = (r - b.astype(F32)).astype(BF16)
    return a, b, c


def kernel(b_hbm, ct_ref, m_ref, out_ref,
           bbuf, bs, cw, abuf, sbuf, arecv, own, gbuf, gsend, grecv,
           md, mx, ms, af, wb, jp, kacc, kout, kin,
           bsem, ssem, rsem, gs_sem, gr_sem, ms_sem, mr_sem, ks_sem, kr_sem, co_ref):
    aux, orb = lax.axis_index('aux'), lax.axis_index('orb')
    me = aux * NORB + orb
    core = lax.rem(orb, 2)
    side = (aux, 1 - aux)

    chip = orb // 2

    STEPS = tuple((core, 1 - core, k) for k in range(2)) + tuple((1 - core, core, k) for k in range(2)) \
        + ((1, 1, 0), (1, 1, 1), (0, 0, 1))

    def peer(n):
        y, x, k = STEPS[n]
        return lax.rem(aux + y, 2), 2 * lax.rem(chip + x, 2) + lax.rem(core + k, 2)

    def name(n):
        y, x, k = STEPS[n]
        return 4 * y + 2 * x + k

    def at(n):
        a, o = peer(n)
        return {'aux': a, 'orb': o}

    def index(n):
        a, o = peer(n)
        return a * NORB + o

    def fetch(g):
        slot = g % NBUF if isinstance(g, int) else lax.rem(g, NBUF)
        return pltpu.make_async_copy(b_hbm.at[pl.ds(g * GR, GR)], bbuf.at[pl.ds(slot * GR, GR)], bsem.at[slot])

    for g in range(NBUF - 1):
        fetch(g).start()

    barrier = pltpu.get_barrier_semaphore()
    for t in range(NDEV - 1):
        pl.semaphore_signal(barrier, inc=1, device_id=at(t), device_id_type=MESH)

    for a in range(NAUX):
        @pl.when(aux == a)
        def _():
            md[...] = m_ref[:, a * QB:(a + 1) * QB]

    co_ref[...] = jnp.zeros_like(co_ref)
    for o in range(NORB):
        @pl.when(orb == o)
        def _():
            co_ref[0:MB, 0:NI] = ct_ref[:, o * MB:(o + 1) * MB].T

    abuf[...] = jnp.zeros_like(abuf)
    gbuf[...] = jnp.zeros_like(gbuf)
    c1, c2, c3 = split3(ct_ref[...])
    cw[...] = jnp.concatenate(
        [c1.astype(F32), c2.astype(F32), c3.astype(F32), jnp.zeros((8, NB), F32)], axis=0).T.astype(BF16)

    ms[...] = jnp.zeros_like(ms)

    def parts_of(x, r, s):
        parts = split3(x)
        for j in range(3):
            ms[j, r * QP:r * QP + QB, s * QP:s * QP + QB] = parts[j]

    parts_of(md[...], 0, 0)
    for a in range(NAUX):
        @pl.when(aux == a)
        def _():
            off = m_ref[:, (1 - a) * QB:(2 - a) * QB]
            af[0:QB, 0:QB] = off
    parts_of(af[0:QB, 0:QB], 0, 1)
    parts_of(af[0:QB, 0:QB].T, 1, 0)

    pl.semaphore_wait(barrier, NDEV - 1)

    def mcopy(src, k, rows, dev):
        block = pl.ds(pl.multiple_of(rows * HQ, 8), HQ)
        return pltpu.make_async_remote_copy(src.at[block], mx.at[block], ms_sem.at[k], mr_sem.at[k],
                                            device_id=dev, device_id_type=MESH)
    mfirst = mcopy(md, 0, core, {'aux': 1 - aux, 'orb': orb})
    mfirst.start()

    def send(c, t):
        return pltpu.make_async_remote_copy(sbuf.at[c, index(t)], arecv.at[aux, :, orb * NCH + c],
                                            ssem.at[name(t)], rsem.at[name(t)], device_id=at(t), device_id_type=MESH)

    def cut(g, half):
        slot = lax.rem(g, NBUF)
        for k in range(GR):
            for r in range(0, QB, 16):
                parts = split3(bbuf[slot * GR + k, r:r + 16, :])
                for j in range(3):
                    bs[3 * (half * GR + k) + j, r:r + 16, 0:NB] = parts[j]

    def dots(half):
        for k in range(half * GR, (half + 1) * GR):
            r = None
            for j in range(3):
                x = jnp.dot(bs[3 * k + j, 0:QB, 0:NB], cw[...], preferred_element_type=F32)
                r = x if r is None else r + x
            r = r.T
            a2 = r[0:NI] + r[NI:2 * NI] + r[2 * NI:3 * NI]
            for v in range(IV):
                for lt in range(4):
                    l0, l1 = lt * 128, min(lt * 128 + 128, QB)
                    abuf[lt, pl.ds(v * MC + k, NDEV, stride=SP), 0:l1 - l0] = a2[8 * v:8 * v + 8, l0:l1]

    lane = lax.broadcasted_iota(jnp.int32, (MC, QP), 1)

    def deliver(c):
        g = gbuf[...]
        for s in range(NDEV):
            for v in range(IV):
                r0 = s * SP + v * MC
                col = co_ref[pl.ds(pl.multiple_of(c * MC, MC), MC), 8 * v + s:8 * v + s + 1]
                x = jnp.concatenate([abuf[lt, r0:r0 + MC, :] for lt in range(4)], axis=1)
                g = g + x * col
                big = jnp.maximum(jnp.max(jnp.abs(x), axis=1, keepdims=True), 2.0 ** -100)
                j = jnp.ceil(jnp.log(big * (1.0 / TOP)) * (1.0 / LN2) + 0.01)
                up = jnp.exp2(j).astype(BF16).astype(F32)
                down = jnp.exp2(-j).astype(BF16).astype(F32)
                y = jnp.exp2(x * down)
                sbuf[c, s, v] = jnp.where(lane < QB, y, up).astype(BF16)
        gbuf[...] = g
        for v in range(IV):
            r0 = pl.multiple_of(me * SP + v * MC, 8)
            own[v, pl.ds(pl.multiple_of(c * MC, MC), MC), :] = jnp.concatenate(
                [abuf[lt, pl.ds(r0, MC), :] for lt in range(4)], axis=1)
        for t in range(NDEV - 1):
            send(c, t).start()

    fetch(0).wait()
    cut(jnp.int32(0), 0)

    msecond = mcopy(mx, 1, core, {'orb': orb + 1 - 2 * core})

    @pl.loop(0, NCH - 1)
    def _(c):
        @pl.when(c == MTURN)
        def _():
            mfirst.wait()
            msecond.start()

        fetch(2 * c + 1).wait()
        fetch(2 * c + 2).wait()

        @pl.when(2 * c + 3 < NG)
        def _():
            fetch(2 * c + 3).start()

        @pl.when(2 * c + 4 < NG)
        def _():
            fetch(2 * c + 4).start()

        cut(2 * c + 1, 1)
        dots(0)
        cut(2 * c + 2, 0)
        dots(1)
        deliver(c)

    for g in range(NBUF):
        fetch(g).start()
    abuf[...] = jnp.zeros_like(abuf)
    dots(0)
    deliver(jnp.int32(NCH - 1))

    gsend[...] = jnp.broadcast_to(jnp.sum(gbuf[...], axis=0, keepdims=True), (8, QP))

    def gcopy(t):
        return pltpu.make_async_remote_copy(gsend, grecv.at[me], gs_sem.at[name(t)], gr_sem.at[name(t)],
                                            device_id=at(t), device_id_type=MESH)

    for t in range(NDEV - 1):
        gcopy(t).start()
    grecv[me] = gsend[...]

    msecond.wait_send()
    mcopy(mx, 1, 1 - core, {'orb': orb + 1 - 2 * core}).wait_recv()
    parts_of(mx[...], 1, 1)
    kacc[...] = jnp.zeros_like(kacc)

    def coulomb(s, base):
        for x in range(2):
            @pl.when(2 * s + x < NG)
            def _():
                fetch(2 * s + x).wait()
        @pl.loop(0, 2 * GR)
        def _(x):
            for l0, l1 in ((0, 128), (128, 256), (256, 384), (384, NB)):
                y = bbuf[base * GR + x, :, l0:l1] * wb[:, 0:l1 - l0]
                jp[2 * GR * s + x, :, l0:l1] = jnp.sum(y.reshape(QB // 8, 8, l1 - l0), axis=0)

        for x in range(2):
            @pl.when(2 * s + NBUF + x < NG)
            def _():
                fetch(2 * s + NBUF + x).start()

    for t in range(NDEV - 1):
        a, o = peer(t)
        whole = arecv.at[a, :, pl.ds(o * NCH, NCH)]
        arrived = pltpu.make_async_remote_copy(whole, whole, ssem.at[name(t)], rsem.at[name(t)],
                                               device_id=at(t), device_id_type=MESH)
        arrived.wait_send()
        arrived.wait_recv()

    for t in range(NDEV - 1):
        pltpu.make_async_remote_copy(gsend, grecv.at[index(t)], gs_sem.at[name(t)], gr_sem.at[name(t)],
                                     device_id=at(t), device_id_type=MESH).wait()
    off = af[0:QB, 0:QB]
    gam = [sum(grecv[side[r] * NORB + o][0:1, 0:QB] for o in range(NORB)) for r in range(2)]
    fit0 = jnp.sum(md[...] * gam[0], axis=1, keepdims=True) + jnp.sum(off * gam[1], axis=1, keepdims=True)
    turn = jnp.broadcast_to(gam[0], (128, QB)).T
    fit1 = (jnp.sum(off * turn[:, 0:1], axis=0, keepdims=True)
            + jnp.sum(mx[...] * jnp.broadcast_to(gam[1], (128, QB)).T[:, 0:1], axis=0, keepdims=True))
    wcol = jnp.sum(off * fit1, axis=1, keepdims=True)
    wrow = jnp.sum(md[...] * fit0, axis=0, keepdims=True)
    wb[...] = jnp.broadcast_to(wrow, (128, QB)).T + wcol

    PAIRS = ((0, 0), (0, 1), (1, 0), (1, 1), (0, 2), (2, 0))

    @pl.loop(0, IV)
    def _(v):
        def decode(sd, r):
            y = arecv[side[sd], v, r // MC:r // MC + 2].astype(F32).reshape(2 * MC, QP)
            u = jnp.log(y) * (1.0 / LN2)
            return ((u + ROUND) - ROUND) * y[:, QB:QB + 1]

        for r in range(0, NORB * MP, 16):
            af[r:r + 16, :] = decode(0, r)
        af[pl.ds(pl.multiple_of(orb * MP, 8), MP), :] = own[v]
        for r in range(0, NORB * MP, 16):
            for j, x in enumerate(split3(af[r:r + 16, :])):
                bs[j, r:r + 16, :] = x
            for j, x in enumerate(split3(decode(1, r))[:2]):
                bs[3 + j, r:r + 16, :] = x
        t = None
        for sd in range(2):
            for i, j in PAIRS[:6 - sd]:
                x = jnp.dot(bs[3 * sd + i], ms[j, sd * QP:(sd + 1) * QP, :], preferred_element_type=F32)
                t = x if t is None else t + x
        for j, x in enumerate(split3(t)):
            bs[5 + j], bs[8 + j] = x[:, 0:QP], x[:, QP:2 * QP]
        coulomb(3 * v, 2 * lax.rem(v, 2))
        half = jnp.asarray(0.5, BF16)
        s1 = None
        for b in (5, 8):
            t1, t2, t3 = bs[b], bs[b + 1], bs[b + 2]
            for x, y in ((t1, t1 * half), (t1, t2), (t1, t3), (t2, t2 * half)):
                z = lax.dot_general(x, y, NT, preferred_element_type=F32)
                s1 = z if s1 is None else s1 + z
        kacc[...] += s1
        coulomb(3 * v + 1, 2 - 2 * lax.rem(v, 2))
        coulomb(3 * v + 2, 2 * lax.rem(v, 2))

    k = kacc[...]
    k = k + k.T
    for a in range(NAUX):
        cols = jnp.concatenate([k[:, o * MP:o * MP + MB] for o in (2 * a, 2 * a + 1)], axis=1)
        for o in range(NORB):
            kout[o % 2, 2 * a + o // 2, :, 0:OB] = -cols[o * MP:(o + 1) * MP]
    j = jnp.sum(jp[...], axis=1)
    for a in range(NAUX):
        kout[core, 2 * a + chip, :, 0:OB] += 2.0 * j[:, a * OB:(a + 1) * OB]

    pair = pltpu.make_async_remote_copy(kout.at[1 - core], kin.at[pl.ds(0, 4)], ks_sem.at[0], kr_sem.at[0],
                                        device_id=at(6), device_id_type=MESH)
    pair.start()
    pair.wait()
    for b in range(4):
        kout[core, b] = kout[core, b] + kin[b]

    def give(t):
        a, o = peer(t)
        return pltpu.make_async_remote_copy(kout.at[core, 2 * a + o // 2], kin.at[3 + name(t) // 2],
                                            ks_sem.at[name(t)], kr_sem.at[name(t)],
                                            device_id=at(t), device_id_type=MESH)

    for t in (0, 2, 4):
        give(t).start()
    total = kout[core, 2 * aux + chip]
    for t in (0, 2, 4):
        give(t).wait_recv()
        total = total + kin[3 + name(t) // 2]
    out_ref[...] = total[0:MB, 0:OB]
    for t in (0, 2, 4):
        give(t).wait_send()


def fock(ints, ct, metric):
    vmem, hbm = pl.BlockSpec(memory_space=pltpu.VMEM), pl.BlockSpec(memory_space=pl.ANY)
    dma = pltpu.SemaphoreType.DMA
    return pl.pallas_call(
        kernel,
        name='fock',
        out_shape=jax.ShapeDtypeStruct((MB, OB), F32),
        in_specs=[hbm, vmem, vmem],
        out_specs=vmem,
        scratch_shapes=[
            pltpu.VMEM((NBUF * GR, QB, NB), F32),
            pltpu.VMEM((6 * GR, NORB * MP, QP), BF16),
            pltpu.VMEM((NB, 128), BF16),
            pltpu.VMEM((4, NDEV * SP, 128), F32),
            pltpu.VMEM((NCH, NDEV, IV, MC, QP), BF16),
            pltpu.VMEM((NAUX, IV, NORB * NCH, MC, QP), BF16),
            pltpu.VMEM((IV, MP, QP), F32),
            pltpu.VMEM((MC, QP), F32),
            pltpu.VMEM((8, QP), F32),
            pltpu.VMEM((NDEV, 8, QP), F32),
            pltpu.VMEM((QB, QB), F32),
            pltpu.VMEM((QB, QB), F32),
            pltpu.VMEM((3, 2 * QP, 2 * QP), BF16),
            pltpu.VMEM((NORB * MP, QP), F32),
            pltpu.VMEM((QB, 128), F32),
            pltpu.VMEM((MP, 8, NB), F32),
            pltpu.VMEM((NORB * MP, NORB * MP), F32),
            pltpu.VMEM((2, 4, MP, 256), F32),
            pltpu.VMEM((7, MP, 256), F32),
            dma((NBUF,)), dma((NDEV,)), dma((NDEV,)), dma((NDEV,)), dma((NDEV,)),
            dma((2,)), dma((2,)), dma((NDEV,)), dma((NDEV,)),
            pltpu.VMEM((MP, 128), F32),
        ],
        compiler_params=pltpu.CompilerParams(collective_id=0, has_side_effects=True, vmem_limit_bytes=67043328),
    )(ints, ct, metric)


def solution(mesh):
    def local_fock(ints, metric, orbitals):
        return fock(jnp.transpose(ints, (1, 0, 2)), orbitals[0].T, metric)[None]

    return jax.shard_map(local_fock, mesh=mesh,
                         in_specs=(P(('sys', 'aux'), 'orb', None), P(('sys', 'aux'), None), P('sys', None, None)),
                         out_specs=P('sys', 'orb', 'aux'), check_vma=False)
```

```python
import jax
import jax.numpy as jnp
from jax import lax
from jax.experimental import pallas as pl
from jax.experimental.pallas import tpu as pltpu

P = jax.sharding.PartitionSpec
F32, BF16 = jnp.float32, jnp.bfloat16
MESH = pl.DeviceIdType.MESH
NT = (((1,), (1,)), ((), ()))
LN2 = 0.6931471805599453
TOP = 126.0
ROUND = 1.5 * 2.0 ** 15

NAUX, NORB, NDEV = 2, 4, 8
QB, MB, NB, NI = 464, 116, 464, 40
IV = NI // NDEV
QP, MP = 512, 120
MC = 8
NCH = MP // MC
TAIL = MB - MC * (NCH - 1)
SP = 40
GR = 4
NG = MB // GR
NBUF = 4
MTURN = 6
NST = (NG + 1) // 2
OB = NB // NAUX
HQ = QB // 2


def split3(x):
    a = x.astype(BF16)
    r = x - a.astype(F32)
    b = r.astype(BF16)
    c = (r - b.astype(F32)).astype(BF16)
    return a, b, c


def kernel(b_hbm, ct_ref, m_ref, out_ref,
           bbuf, bs, cw, abuf, sbuf, arecv, own, gbuf, gsend, grecv,
           md, mx, ms, af, wb, jp, kacc, kout, kin,
           bsem, ssem, rsem, gs_sem, gr_sem, ms_sem, mr_sem, ks_sem, kr_sem, co_ref):
    aux, orb = lax.axis_index('aux'), lax.axis_index('orb')
    me = aux * NORB + orb
    core = lax.rem(orb, 2)
    side = (aux, 1 - aux)

    chip = orb // 2

    STEPS = tuple((core, 1 - core, k) for k in range(2)) + tuple((1 - core, core, k) for k in range(2)) \
        + ((1, 1, 0), (1, 1, 1), (0, 0, 1))

    def peer(n):
        y, x, k = STEPS[n]
        return lax.rem(aux + y, 2), 2 * lax.rem(chip + x, 2) + lax.rem(core + k, 2)

    def name(n):
        y, x, k = STEPS[n]
        return 4 * y + 2 * x + k

    def at(n):
        a, o = peer(n)
        return {'aux': a, 'orb': o}

    def index(n):
        a, o = peer(n)
        return a * NORB + o

    def fetch(g):
        slot = g % NBUF if isinstance(g, int) else lax.rem(g, NBUF)
        return pltpu.make_async_copy(b_hbm.at[pl.ds(g * GR, GR)], bbuf.at[pl.ds(slot * GR, GR)], bsem.at[slot])

    for g in range(NBUF - 1):
        fetch(g).start()

    barrier = pltpu.get_barrier_semaphore()
    for t in range(NDEV - 1):
        pl.semaphore_signal(barrier, inc=1, device_id=at(t), device_id_type=MESH)

    for a in range(NAUX):
        @pl.when(aux == a)
        def _():
            md[...] = m_ref[:, a * QB:(a + 1) * QB]

    co_ref[...] = jnp.zeros_like(co_ref)
    for o in range(NORB):
        @pl.when(orb == o)
        def _():
            co_ref[0:MB, 0:NI] = ct_ref[:, o * MB:(o + 1) * MB].T

    abuf[...] = jnp.zeros_like(abuf)
    gbuf[...] = jnp.zeros_like(gbuf)
    c1, c2, c3 = split3(ct_ref[...])
    cw[...] = jnp.concatenate(
        [c1.astype(F32), c2.astype(F32), c3.astype(F32), jnp.zeros((8, NB), F32)], axis=0).T.astype(BF16)

    ms[...] = jnp.zeros_like(ms)

    def parts_of(x, r, s):
        parts = split3(x)
        for j in range(3):
            ms[j, r * QP:r * QP + QB, s * QP:s * QP + QB] = parts[j]

    parts_of(md[...], 0, 0)
    for a in range(NAUX):
        @pl.when(aux == a)
        def _():
            off = m_ref[:, (1 - a) * QB:(2 - a) * QB]
            af[0:QB, 0:QB] = off
    parts_of(af[0:QB, 0:QB], 0, 1)
    parts_of(af[0:QB, 0:QB].T, 1, 0)

    pl.semaphore_wait(barrier, NDEV - 1)

    def mcopy(src, k, rows, dev):
        block = pl.ds(pl.multiple_of(rows * HQ, 8), HQ)
        return pltpu.make_async_remote_copy(src.at[block], mx.at[block], ms_sem.at[k], mr_sem.at[k],
                                            device_id=dev, device_id_type=MESH)
    mfirst = mcopy(md, 0, core, {'aux': 1 - aux, 'orb': orb})
    mfirst.start()

    def send(c, t):
        return pltpu.make_async_remote_copy(sbuf.at[c, index(t)], arecv.at[aux, :, orb * NCH + c],
                                            ssem.at[name(t)], rsem.at[name(t)], device_id=at(t), device_id_type=MESH)

    def cut(g, half):
        slot = lax.rem(g, NBUF)
        for k in range(GR):
            for r in range(0, QB, 16):
                parts = split3(bbuf[slot * GR + k, r:r + 16, :])
                for j in range(3):
                    bs[3 * (half * GR + k) + j, r:r + 16, 0:NB] = parts[j]

    def dots(half):
        for k in range(half * GR, (half + 1) * GR):
            r = None
            for j in range(3):
                x = jnp.dot(bs[3 * k + j, 0:QB, 0:NB], cw[...], preferred_element_type=F32)
                r = x if r is None else r + x
            r = r.T
            a2 = r[0:NI] + r[NI:2 * NI] + r[2 * NI:3 * NI]
            for v in range(IV):
                for lt in range(4):
                    l0, l1 = lt * 128, min(lt * 128 + 128, QB)
                    abuf[lt, pl.ds(v * MC + k, NDEV, stride=SP), 0:l1 - l0] = a2[8 * v:8 * v + 8, l0:l1]

    lane = lax.broadcasted_iota(jnp.int32, (MC, QP), 1)

    def deliver(c):
        g = gbuf[...]
        for s in range(NDEV):
            for v in range(IV):
                r0 = s * SP + v * MC
                col = co_ref[pl.ds(pl.multiple_of(c * MC, MC), MC), 8 * v + s:8 * v + s + 1]
                x = jnp.concatenate([abuf[lt, r0:r0 + MC, :] for lt in range(4)], axis=1)
                g = g + x * col
                big = jnp.maximum(jnp.max(jnp.abs(x), axis=1, keepdims=True), 2.0 ** -100)
                j = jnp.ceil(jnp.log(big * (1.0 / TOP)) * (1.0 / LN2) + 0.01)
                up = jnp.exp2(j).astype(BF16).astype(F32)
                down = jnp.exp2(-j).astype(BF16).astype(F32)
                y = jnp.exp2(x * down)
                sbuf[c, s, v] = jnp.where(lane < QB, y, up).astype(BF16)
        gbuf[...] = g
        for v in range(IV):
            r0 = pl.multiple_of(me * SP + v * MC, 8)
            own[v, pl.ds(pl.multiple_of(c * MC, MC), MC), :] = jnp.concatenate(
                [abuf[lt, pl.ds(r0, MC), :] for lt in range(4)], axis=1)
        for t in range(NDEV - 1):
            send(c, t).start()

    fetch(0).wait()
    cut(jnp.int32(0), 0)

    msecond = mcopy(mx, 1, core, {'orb': orb + 1 - 2 * core})

    @pl.loop(0, NCH - 1)
    def _(c):
        @pl.when(c == MTURN)
        def _():
            mfirst.wait()
            msecond.start()

        fetch(2 * c + 1).wait()
        fetch(2 * c + 2).wait()

        @pl.when(2 * c + 3 < NG)
        def _():
            fetch(2 * c + 3).start()

        @pl.when(2 * c + 4 < NG)
        def _():
            fetch(2 * c + 4).start()

        cut(2 * c + 1, 1)
        dots(0)
        cut(2 * c + 2, 0)
        dots(1)
        deliver(c)

    for g in range(NBUF):
        fetch(g).start()
    abuf[...] = jnp.zeros_like(abuf)
    dots(0)
    deliver(jnp.int32(NCH - 1))

    gsend[...] = jnp.broadcast_to(jnp.sum(gbuf[...], axis=0, keepdims=True), (8, QP))

    def gcopy(t):
        return pltpu.make_async_remote_copy(gsend, grecv.at[me], gs_sem.at[name(t)], gr_sem.at[name(t)],
                                            device_id=at(t), device_id_type=MESH)

    for t in range(NDEV - 1):
        gcopy(t).start()
    grecv[me] = gsend[...]

    msecond.wait_send()
    mcopy(mx, 1, 1 - core, {'orb': orb + 1 - 2 * core}).wait_recv()
    parts_of(mx[...], 1, 1)
    kacc[...] = jnp.zeros_like(kacc)

    def coulomb(s, base):
        for x in range(2):
            @pl.when(2 * s + x < NG)
            def _():
                fetch(2 * s + x).wait()
        @pl.loop(0, 2 * GR)
        def _(x):
            acc = None
            for g in range(0, QB, 16):
                w = wb[g:g + 16, :]
                w = jnp.concatenate([w, w, w, w[:, 0:NB - 384]], axis=1)
                y = bbuf[base * GR + x, g:g + 16, :] * w
                acc = y if acc is None else acc + y
            jp[2 * GR * s + x] = acc[0:8] + acc[8:16]

        for x in range(2):
            @pl.when(2 * s + NBUF + x < NG)
            def _():
                fetch(2 * s + NBUF + x).start()

    for t in range(NDEV - 1):
        a, o = peer(t)
        whole = arecv.at[a, :, pl.ds(o * NCH, NCH)]
        arrived = pltpu.make_async_remote_copy(whole, whole, ssem.at[name(t)], rsem.at[name(t)],
                                               device_id=at(t), device_id_type=MESH)
        arrived.wait_send()
        arrived.wait_recv()

    for t in range(NDEV - 1):
        pltpu.make_async_remote_copy(gsend, grecv.at[index(t)], gs_sem.at[name(t)], gr_sem.at[name(t)],
                                     device_id=at(t), device_id_type=MESH).wait()
    off = af[0:QB, 0:QB]
    gam = [sum(grecv[side[r] * NORB + o][0:1, 0:QB] for o in range(NORB)) for r in range(2)]
    fit0 = jnp.sum(md[...] * gam[0], axis=1, keepdims=True) + jnp.sum(off * gam[1], axis=1, keepdims=True)
    turn = jnp.broadcast_to(gam[0], (128, QB)).T
    fit1 = (jnp.sum(off * turn[:, 0:1], axis=0, keepdims=True)
            + jnp.sum(mx[...] * jnp.broadcast_to(gam[1], (128, QB)).T[:, 0:1], axis=0, keepdims=True))
    wcol = jnp.sum(off * fit1, axis=1, keepdims=True)
    wrow = jnp.sum(md[...] * fit0, axis=0, keepdims=True)
    wb[...] = jnp.broadcast_to(wrow, (128, QB)).T + wcol

    PAIRS = ((0, 0), (0, 1), (1, 0), (1, 1), (0, 2), (2, 0))

    @pl.loop(0, IV)
    def _(v):
        def decode(sd, r):
            y = arecv[side[sd], v, r // MC:r // MC + 2].astype(F32).reshape(2 * MC, QP)
            u = jnp.log(y) * (1.0 / LN2)
            return ((u + ROUND) - ROUND) * y[:, QB:QB + 1]

        for r in range(0, NORB * MP, 16):
            af[r:r + 16, :] = decode(0, r)
        af[pl.ds(pl.multiple_of(orb * MP, 8), MP), :] = own[v]
        for r in range(0, NORB * MP, 16):
            for j, x in enumerate(split3(af[r:r + 16, :])):
                bs[j, r:r + 16, :] = x
            for j, x in enumerate(split3(decode(1, r))[:2]):
                bs[3 + j, r:r + 16, :] = x
        t = None
        for sd in range(2):
            for i, j in PAIRS[:6 - sd]:
                x = jnp.dot(bs[3 * sd + i], ms[j, sd * QP:(sd + 1) * QP, :], preferred_element_type=F32)
                t = x if t is None else t + x
        for j, x in enumerate(split3(t)):
            bs[5 + j], bs[8 + j] = x[:, 0:QP], x[:, QP:2 * QP]
        coulomb(3 * v, 2 * lax.rem(v, 2))
        half = jnp.asarray(0.5, BF16)
        s1 = None
        for b in (5, 8):
            t1, t2, t3 = bs[b], bs[b + 1], bs[b + 2]
            for x, y in ((t1, t1 * half), (t1, t2), (t1, t3), (t2, t2 * half)):
                z = lax.dot_general(x, y, NT, preferred_element_type=F32)
                s1 = z if s1 is None else s1 + z
        kacc[...] += s1
        coulomb(3 * v + 1, 2 - 2 * lax.rem(v, 2))
        coulomb(3 * v + 2, 2 * lax.rem(v, 2))

    k = kacc[...]
    k = k + k.T
    for a in range(NAUX):
        cols = jnp.concatenate([k[:, o * MP:o * MP + MB] for o in (2 * a, 2 * a + 1)], axis=1)
        for o in range(NORB):
            kout[o % 2, 2 * a + o // 2, :, 0:OB] = -cols[o * MP:(o + 1) * MP]
    j = jnp.sum(jp[...], axis=1)
    for a in range(NAUX):
        kout[core, 2 * a + chip, :, 0:OB] += 2.0 * j[:, a * OB:(a + 1) * OB]

    pair = pltpu.make_async_remote_copy(kout.at[1 - core], kin.at[pl.ds(0, 4)], ks_sem.at[0], kr_sem.at[0],
                                        device_id=at(6), device_id_type=MESH)
    pair.start()
    pair.wait()
    for b in range(4):
        kout[core, b] = kout[core, b] + kin[b]

    def give(t):
        a, o = peer(t)
        return pltpu.make_async_remote_copy(kout.at[core, 2 * a + o // 2], kin.at[3 + name(t) // 2],
                                            ks_sem.at[name(t)], kr_sem.at[name(t)],
                                            device_id=at(t), device_id_type=MESH)

    for t in (0, 2, 4):
        give(t).start()
    total = kout[core, 2 * aux + chip]
    for t in (0, 2, 4):
        give(t).wait_recv()
        total = total + kin[3 + name(t) // 2]
    out_ref[...] = total[0:MB, 0:OB]
    for t in (0, 2, 4):
        give(t).wait_send()


def fock(ints, ct, metric):
    vmem, hbm = pl.BlockSpec(memory_space=pltpu.VMEM), pl.BlockSpec(memory_space=pl.ANY)
    dma = pltpu.SemaphoreType.DMA
    return pl.pallas_call(
        kernel,
        name='fock',
        out_shape=jax.ShapeDtypeStruct((MB, OB), F32),
        in_specs=[hbm, vmem, vmem],
        out_specs=vmem,
        scratch_shapes=[
            pltpu.VMEM((NBUF * GR, QB, NB), F32),
            pltpu.VMEM((6 * GR, NORB * MP, QP), BF16),
            pltpu.VMEM((NB, 128), BF16),
            pltpu.VMEM((4, NDEV * SP, 128), F32),
            pltpu.VMEM((NCH, NDEV, IV, MC, QP), BF16),
            pltpu.VMEM((NAUX, IV, NORB * NCH, MC, QP), BF16),
            pltpu.VMEM((IV, MP, QP), F32),
            pltpu.VMEM((MC, QP), F32),
            pltpu.VMEM((8, QP), F32),
            pltpu.VMEM((NDEV, 8, QP), F32),
            pltpu.VMEM((QB, QB), F32),
            pltpu.VMEM((QB, QB), F32),
            pltpu.VMEM((3, 2 * QP, 2 * QP), BF16),
            pltpu.VMEM((NORB * MP, QP), F32),
            pltpu.VMEM((QB, 128), F32),
            pltpu.VMEM((MP, 8, NB), F32),
            pltpu.VMEM((NORB * MP, NORB * MP), F32),
            pltpu.VMEM((2, 4, MP, 256), F32),
            pltpu.VMEM((7, MP, 256), F32),
            dma((NBUF,)), dma((NDEV,)), dma((NDEV,)), dma((NDEV,)), dma((NDEV,)),
            dma((2,)), dma((2,)), dma((NDEV,)), dma((NDEV,)),
            pltpu.VMEM((MP, 128), F32),
        ],
        compiler_params=pltpu.CompilerParams(collective_id=0, has_side_effects=True, vmem_limit_bytes=67043328),
    )(ints, ct, metric)


def solution(mesh):
    def local_fock(ints, metric, orbitals):
        return fock(jnp.transpose(ints, (1, 0, 2)), orbitals[0].T, metric)[None]

    return jax.shard_map(local_fock, mesh=mesh,
                         in_specs=(P(('sys', 'aux'), 'orb', None), P(('sys', 'aux'), None), P('sys', None, None)),
                         out_specs=P('sys', 'orb', 'aux'), check_vma=False)
```

```python
import jax
import jax.numpy as jnp
from jax import lax
from jax.experimental import pallas as pl
from jax.experimental.pallas import tpu as pltpu

P = jax.sharding.PartitionSpec
F32, BF16 = jnp.float32, jnp.bfloat16
MESH = pl.DeviceIdType.MESH
NT = (((1,), (1,)), ((), ()))
LN2 = 0.6931471805599453
TOP = 126.0
ROUND = 1.5 * 2.0 ** 15

NAUX, NORB, NDEV = 2, 4, 8
QB, MB, NB, NI = 464, 116, 464, 40
IV = NI // NDEV
QP, MP = 512, 120
MC = 8
NCH = MP // MC
TAIL = MB - MC * (NCH - 1)
SP = 40
GR = 4
NG = MB // GR
NBUF = 4
MTURN = 6
NST = (NG + 1) // 2
OB = NB // NAUX
HQ = QB // 2


def split3(x):
    a = x.astype(BF16)
    r = x - a.astype(F32)
    b = r.astype(BF16)
    c = (r - b.astype(F32)).astype(BF16)
    return a, b, c


def kernel(b_hbm, ct_ref, m_ref, out_ref,
           bbuf, bs, cw, abuf, sbuf, arecv, own, gbuf, gsend, grecv,
           md, mx, ms, af, wb, jp, kacc, kout, kin,
           bsem, ssem, rsem, gs_sem, gr_sem, ms_sem, mr_sem, ks_sem, kr_sem, co_ref):
    aux, orb = lax.axis_index('aux'), lax.axis_index('orb')
    me = aux * NORB + orb
    core = lax.rem(orb, 2)
    side = (aux, 1 - aux)

    chip = orb // 2

    STEPS = tuple((core, 1 - core, k) for k in range(2)) + tuple((1 - core, core, k) for k in range(2)) \
        + ((1, 1, 0), (1, 1, 1), (0, 0, 1))

    def peer(n):
        y, x, k = STEPS[n]
        return lax.rem(aux + y, 2), 2 * lax.rem(chip + x, 2) + lax.rem(core + k, 2)

    def name(n):
        y, x, k = STEPS[n]
        return 4 * y + 2 * x + k

    def at(n):
        a, o = peer(n)
        return {'aux': a, 'orb': o}

    def index(n):
        a, o = peer(n)
        return a * NORB + o

    def fetch(g):
        slot = g % NBUF if isinstance(g, int) else lax.rem(g, NBUF)
        return pltpu.make_async_copy(b_hbm.at[pl.ds(g * GR, GR)], bbuf.at[pl.ds(slot * GR, GR)], bsem.at[slot])

    for g in range(NBUF - 1):
        fetch(g).start()

    barrier = pltpu.get_barrier_semaphore()
    for t in range(NDEV - 1):
        pl.semaphore_signal(barrier, inc=1, device_id=at(t), device_id_type=MESH)

    for a in range(NAUX):
        @pl.when(aux == a)
        def _():
            md[...] = m_ref[:, a * QB:(a + 1) * QB]

    co_ref[...] = jnp.zeros_like(co_ref)
    for o in range(NORB):
        @pl.when(orb == o)
        def _():
            co_ref[0:MB, 0:NI] = ct_ref[:, o * MB:(o + 1) * MB].T

    abuf[...] = jnp.zeros_like(abuf)
    gbuf[...] = jnp.zeros_like(gbuf)
    c1, c2, c3 = split3(ct_ref[...])
    cw[...] = jnp.concatenate(
        [c1.astype(F32), c2.astype(F32), c3.astype(F32), jnp.zeros((8, NB), F32)], axis=0).T.astype(BF16)

    ms[...] = jnp.zeros_like(ms)

    def parts_of(x, r, s):
        parts = split3(x)
        for j in range(3):
            ms[j, r * QP:r * QP + QB, s * QP:s * QP + QB] = parts[j]

    parts_of(md[...], 0, 0)
    for a in range(NAUX):
        @pl.when(aux == a)
        def _():
            off = m_ref[:, (1 - a) * QB:(2 - a) * QB]
            af[0:QB, 0:QB] = off
    parts_of(af[0:QB, 0:QB], 0, 1)
    parts_of(af[0:QB, 0:QB].T, 1, 0)

    pl.semaphore_wait(barrier, NDEV - 1)

    def mcopy(src, k, rows, dev):
        block = pl.ds(pl.multiple_of(rows * HQ, 8), HQ)
        return pltpu.make_async_remote_copy(src.at[block], mx.at[block], ms_sem.at[k], mr_sem.at[k],
                                            device_id=dev, device_id_type=MESH)
    mfirst = mcopy(md, 0, core, {'aux': 1 - aux, 'orb': orb})
    mfirst.start()

    def send(c, t):
        return pltpu.make_async_remote_copy(sbuf.at[c, index(t)], arecv.at[aux, :, orb * NCH + c],
                                            ssem.at[name(t)], rsem.at[name(t)], device_id=at(t), device_id_type=MESH)

    def cut(g, half):
        slot = lax.rem(g, NBUF)
        for k in range(GR):
            for r in range(0, QB, 16):
                parts = split3(bbuf[slot * GR + k, r:r + 16, :])
                for j in range(3):
                    bs[3 * (half * GR + k) + j, r:r + 16, 0:NB] = parts[j]

    def dots(half):
        for k in range(half * GR, (half + 1) * GR):
            r = None
            for j in range(3):
                x = jnp.dot(bs[3 * k + j, 0:QB, 0:NB], cw[...], preferred_element_type=F32)
                r = x if r is None else r + x
            r = r.T
            a2 = r[0:NI] + r[NI:2 * NI] + r[2 * NI:3 * NI]
            for v in range(IV):
                for lt in range(4):
                    l0, l1 = lt * 128, min(lt * 128 + 128, QB)
                    abuf[lt, pl.ds(v * MC + k, NDEV, stride=SP), 0:l1 - l0] = a2[8 * v:8 * v + 8, l0:l1]

    lane = lax.broadcasted_iota(jnp.int32, (MC, QP), 1)

    def deliver(c):
        g = gbuf[...]
        for s in range(NDEV):
            for v in range(IV):
                r0 = s * SP + v * MC
                col = co_ref[pl.ds(pl.multiple_of(c * MC, MC), MC), 8 * v + s:8 * v + s + 1]
                x = jnp.concatenate([abuf[lt, r0:r0 + MC, :] for lt in range(4)], axis=1)
                g = g + x * col
                big = jnp.maximum(jnp.max(jnp.abs(x), axis=1, keepdims=True), 2.0 ** -100)
                j = jnp.ceil(jnp.log(big * (1.0 / TOP)) * (1.0 / LN2) + 0.01)
                up = jnp.exp2(j).astype(BF16).astype(F32)
                down = jnp.exp2(-j).astype(BF16).astype(F32)
                y = jnp.exp2(x * down)
                sbuf[c, s, v] = jnp.where(lane < QB, y, up).astype(BF16)
        gbuf[...] = g
        for v in range(IV):
            r0 = pl.multiple_of(me * SP + v * MC, 8)
            own[v, pl.ds(pl.multiple_of(c * MC, MC), MC), :] = jnp.concatenate(
                [abuf[lt, pl.ds(r0, MC), :] for lt in range(4)], axis=1)
        for t in range(NDEV - 1):
            send(c, t).start()

    fetch(0).wait()
    cut(jnp.int32(0), 0)

    msecond = mcopy(mx, 1, core, {'orb': orb + 1 - 2 * core})

    @pl.loop(0, NCH - 1)
    def _(c):
        @pl.when(c == MTURN)
        def _():
            mfirst.wait()
            msecond.start()

        fetch(2 * c + 1).wait()
        fetch(2 * c + 2).wait()

        @pl.when(2 * c + 3 < NG)
        def _():
            fetch(2 * c + 3).start()

        @pl.when(2 * c + 4 < NG)
        def _():
            fetch(2 * c + 4).start()

        cut(2 * c + 1, 1)
        dots(0)
        cut(2 * c + 2, 0)
        dots(1)
        deliver(c)

    for g in range(NBUF):
        fetch(g).start()
    abuf[...] = jnp.zeros_like(abuf)
    dots(0)
    deliver(jnp.int32(NCH - 1))

    gsend[...] = jnp.broadcast_to(jnp.sum(gbuf[...], axis=0, keepdims=True), (8, QP))

    def gcopy(t):
        return pltpu.make_async_remote_copy(gsend, grecv.at[me], gs_sem.at[name(t)], gr_sem.at[name(t)],
                                            device_id=at(t), device_id_type=MESH)

    for t in range(NDEV - 1):
        gcopy(t).start()
    grecv[me] = gsend[...]

    msecond.wait_send()
    mcopy(mx, 1, 1 - core, {'orb': orb + 1 - 2 * core}).wait_recv()
    parts_of(mx[...], 1, 1)
    kacc[...] = jnp.zeros_like(kacc)

    def coulomb(s, base):
        for x in range(2):
            @pl.when(2 * s + x < NG)
            def _():
                fetch(2 * s + x).wait()
        @pl.loop(0, 2 * GR)
        def _(x):
            acc = None
            for g in range(0, QB, 16):
                w = wb[g:g + 16, :]
                w = jnp.concatenate([w, w, w, w[:, 0:NB - 384]], axis=1)
                y = bbuf[base * GR + x, g:g + 16, :] * w
                acc = y if acc is None else acc + y
            jp[2 * GR * s + x] = acc[0:8] + acc[8:16]

        for x in range(2):
            @pl.when(2 * s + NBUF + x < NG)
            def _():
                fetch(2 * s + NBUF + x).start()

    for t in range(NDEV - 1):
        a, o = peer(t)
        whole = arecv.at[a, :, pl.ds(o * NCH, NCH)]
        arrived = pltpu.make_async_remote_copy(whole, whole, ssem.at[name(t)], rsem.at[name(t)],
                                               device_id=at(t), device_id_type=MESH)
        arrived.wait_send()
        arrived.wait_recv()

    for t in range(NDEV - 1):
        pltpu.make_async_remote_copy(gsend, grecv.at[index(t)], gs_sem.at[name(t)], gr_sem.at[name(t)],
                                     device_id=at(t), device_id_type=MESH).wait()
    off = af[0:QB, 0:QB]
    gam = [sum(grecv[side[r] * NORB + o][0:1, 0:QB] for o in range(NORB)) for r in range(2)]
    fit0 = jnp.sum(md[...] * gam[0], axis=1, keepdims=True) + jnp.sum(off * gam[1], axis=1, keepdims=True)
    turn = jnp.broadcast_to(gam[0], (128, QB)).T
    fit1 = (jnp.sum(off * turn[:, 0:1], axis=0, keepdims=True)
            + jnp.sum(mx[...] * jnp.broadcast_to(gam[1], (128, QB)).T[:, 0:1], axis=0, keepdims=True))
    wcol = jnp.sum(off * fit1, axis=1, keepdims=True)
    wrow = jnp.sum(md[...] * fit0, axis=0, keepdims=True)
    wb[...] = jnp.broadcast_to(wrow, (128, QB)).T + wcol

    PAIRS = ((0, 0), (0, 1), (1, 0), (1, 1), (0, 2), (2, 0))

    @pl.loop(0, IV)
    def _(v):
        def decode(sd, r):
            y = arecv[side[sd], v, r // MC:r // MC + 2].astype(F32).reshape(2 * MC, QP)
            u = jnp.log(y) * (1.0 / LN2)
            return ((u + ROUND) - ROUND) * y[:, QB:QB + 1]

        for r in range(0, NORB * MP, 16):
            af[r:r + 16, :] = decode(0, r)
        af[pl.ds(pl.multiple_of(orb * MP, 8), MP), :] = own[v]
        for r in range(0, NORB * MP, 16):
            for j, x in enumerate(split3(af[r:r + 16, :])):
                bs[j, r:r + 16, :] = x
            for j, x in enumerate(split3(decode(1, r))[:2]):
                bs[3 + j, r:r + 16, :] = x
        t = None
        for sd in range(2):
            for i, j in PAIRS[:6 - sd]:
                x = jnp.dot(bs[3 * sd + i], ms[j, sd * QP:(sd + 1) * QP, :], preferred_element_type=F32)
                t = x if t is None else t + x
        for j, x in enumerate(split3(t)):
            bs[5 + j], bs[8 + j] = x[:, 0:QP], x[:, QP:2 * QP]
        coulomb(3 * v, 2 * lax.rem(v, 2))
        half = jnp.asarray(0.5, BF16)
        s1 = None
        for b in (5, 8):
            t1, t2, t3 = bs[b], bs[b + 1], bs[b + 2]
            for x, y in ((t1, t1 * half), (t1, t2), (t1, t3), (t2, t2 * half)):
                z = lax.dot_general(x, y, NT, preferred_element_type=F32)
                s1 = z if s1 is None else s1 + z
        kacc[...] += s1
        coulomb(3 * v + 1, 2 - 2 * lax.rem(v, 2))
        coulomb(3 * v + 2, 2 * lax.rem(v, 2))

    k = kacc[...]
    k = k + k.T
    for a in range(NAUX):
        cols = jnp.concatenate([k[:, o * MP:o * MP + MB] for o in (2 * a, 2 * a + 1)], axis=1)
        for o in range(NORB):
            kout[o % 2, 2 * a + o // 2, :, 0:OB] = -cols[o * MP:(o + 1) * MP]
    j = jnp.sum(jp[...], axis=1)
    for a in range(NAUX):
        kout[core, 2 * a + chip, :, 0:OB] += 2.0 * j[:, a * OB:(a + 1) * OB]

    pair = pltpu.make_async_remote_copy(kout.at[1 - core], kin.at[pl.ds(0, 4)], ks_sem.at[0], kr_sem.at[0],
                                        device_id=at(6), device_id_type=MESH)
    pair.start()
    pair.wait()
    for b in range(4):
        kout[core, b] = kout[core, b] + kin[b]

    def give(t):
        a, o = peer(t)
        return pltpu.make_async_remote_copy(kout.at[core, 2 * a + o // 2], kin.at[3 + name(t) // 2],
                                            ks_sem.at[name(t)], kr_sem.at[name(t)],
                                            device_id=at(t), device_id_type=MESH)

    for t in (0, 2, 4):
        give(t).start()
    total = kout[core, 2 * aux + chip]
    for t in (0, 2, 4):
        give(t).wait_recv()
        total = total + kin[3 + name(t) // 2]
    out_ref[...] = total[0:MB, 0:OB].reshape(MB, 1, OB)
    for t in (0, 2, 4):
        give(t).wait_send()


def fock(ints, ct, metric):
    vmem, hbm = pl.BlockSpec(memory_space=pltpu.VMEM), pl.BlockSpec(memory_space=pl.ANY)
    dma = pltpu.SemaphoreType.DMA
    return pl.pallas_call(
        kernel,
        name='fock',
        out_shape=jax.ShapeDtypeStruct((MB, 1, OB), F32),
        in_specs=[hbm, vmem, vmem],
        out_specs=vmem,
        scratch_shapes=[
            pltpu.VMEM((NBUF * GR, QB, NB), F32),
            pltpu.VMEM((6 * GR, NORB * MP, QP), BF16),
            pltpu.VMEM((NB, 128), BF16),
            pltpu.VMEM((4, NDEV * SP, 128), F32),
            pltpu.VMEM((NCH, NDEV, IV, MC, QP), BF16),
            pltpu.VMEM((NAUX, IV, NORB * NCH, MC, QP), BF16),
            pltpu.VMEM((IV, MP, QP), F32),
            pltpu.VMEM((MC, QP), F32),
            pltpu.VMEM((8, QP), F32),
            pltpu.VMEM((NDEV, 8, QP), F32),
            pltpu.VMEM((QB, QB), F32),
            pltpu.VMEM((QB, QB), F32),
            pltpu.VMEM((3, 2 * QP, 2 * QP), BF16),
            pltpu.VMEM((NORB * MP, QP), F32),
            pltpu.VMEM((QB, 128), F32),
            pltpu.VMEM((MP, 8, NB), F32),
            pltpu.VMEM((NORB * MP, NORB * MP), F32),
            pltpu.VMEM((2, 4, MP, 256), F32),
            pltpu.VMEM((7, MP, 256), F32),
            dma((NBUF,)), dma((NDEV,)), dma((NDEV,)), dma((NDEV,)), dma((NDEV,)),
            dma((2,)), dma((2,)), dma((NDEV,)), dma((NDEV,)),
            pltpu.VMEM((MP, 128), F32),
        ],
        compiler_params=pltpu.CompilerParams(collective_id=0, has_side_effects=True, vmem_limit_bytes=67043328),
    )(ints, ct, metric)


def solution(mesh):
    def local_fock(ints, metric, orbitals):
        return jnp.transpose(fock(jnp.transpose(ints, (1, 0, 2)), orbitals[0].T, metric), (1, 0, 2))

    return jax.shard_map(local_fock, mesh=mesh,
                         in_specs=(P(('sys', 'aux'), 'orb', None), P(('sys', 'aux'), None), P('sys', None, None)),
                         out_specs=P('sys', 'orb', 'aux'), check_vma=False)
```
